32 devices in a mesh: dp: 32 (over z, y, x, core).
Axes of the slice: x: 2, y: 2, z: 4, core: 2. Of those that a mesh axis runs over, the one named last changes fastest.
Arguments:
- images: bfloat16 [512, 14, 14, 512], P('dp'), may hold values from -6 to 6
- first_gain: bfloat16 [512], P('dp'), may hold values from 0.099609375 to 1.8984375
- first_shift: bfloat16 [512], P('dp'), may hold values from -1.75 to 1.75
- joint_weight: bfloat16 [512, 1536], P('dp'), may hold values from -0.25 to 0.25
- joint_bias: bfloat16 [2, 512], P(None, 'dp'), may hold values from -3 to 3
- output_weight: bfloat16 [512, 512], P('dp'), may hold values from -0.5 to 0.5
- output_bias: bfloat16 [512], P('dp'), may hold values from -1.75 to 1.75
- second_gain: bfloat16 [512], P('dp'), may hold values from 0.099609375 to 1.8984375
- second_shift: bfloat16 [512], P('dp'), may hold values from -1.75 to 1.75
- expand_weight: bfloat16 [512, 2048], P('dp'), may hold values from -0.25 to 0.25
- expand_bias: bfloat16 [2048], P('dp'), may hold values from -3 to 3
- reduce_weight: bfloat16 [2048, 512], P('dp'), may hold values from -0.125 to 0.125
- reduce_bias: bfloat16 [512], P('dp'), may hold values from -1.75 to 1.75
- bias_table: bfloat16 [169, 16], replicated, may hold values from -4 to 260
- regions: int32 [14, 14], replicated, may hold values from 0 to 8
- live_slots: int32 [512], P('dp'), may hold values from 0 to 1, as said below
- cotangent: bfloat16 [512, 14, 14, 512], P('dp'), may hold values from -6 to 6
Outputs:
- block_output: bfloat16 [512, 14, 14, 512], P('dp')
- input_grad: bfloat16 [512, 14, 14, 512], P('dp')
- first_gain_grad: float32 [512], P('dp')
- first_shift_grad: float32 [512], P('dp')
- joint_weight_grad: float32 [512, 1536], P('dp')
- joint_bias_grad: float32 [2, 512], P(None, 'dp')
- output_weight_grad: float32 [512, 512], P('dp')
- output_bias_grad: float32 [512], P('dp')
- second_gain_grad: float32 [512], P('dp')
- second_shift_grad: float32 [512], P('dp')
- expand_weight_grad: float32 [512, 2048], P('dp')
- expand_bias_grad: float32 [2048], P('dp')
- reduce_weight_grad: float32 [2048, 512], P('dp')
- reduce_bias_grad: float32 [512], P('dp')
- table_grad: float32 [169, 16], replicated
The draws below stay inside these ranges and needn't reach their ends.
Inputs may be any that keep to these rules, and one draw needn't show every extreme that they name: `live_slots`: on each device the live image slots come first: the first 1 to 16 of its 16 slots hold images, and some device holds 16.
All inputs are finite; a program needn't handle non-finite values.
Results may differ from the reference program's by a relative error of at most 0.011.
Values may be sent and summed in bfloat16 or wider, within the bound.
A program may use at most 320 MiB of HBM per device.

```python
import jax
import jax.numpy as jnp
from jax import lax

C = 512
HEADS = 16
HEAD_DIM = 32
EXPAND = 2048
WIN = 7
SIDE = 14
SHIFT = 3
REGIONS = 9
IMG_DEV = 16
PANES = 4
TABLE_ROWS = 169
IMAGES = 512
N_DP = 32


def draw_bias_table(key, part):
    noise_key = jax.random.fold_in(jax.random.fold_in(key, 11), 0)
    base = jnp.clip(jax.random.normal(noise_key, (TABLE_ROWS, HEADS), jnp.float32), -4.0, 4.0)
    return base.astype(jnp.bfloat16)


def draw_live_slots(key, part):
    count_key, full_key = jax.random.split(jax.random.fold_in(key, 23))
    devices = IMAGES // IMG_DEV
    counts = jax.random.randint(count_key, (devices,), 1, IMG_DEV + 1)
    busiest = jax.random.randint(full_key, (), 0, devices)
    counts = jnp.where(jnp.arange(devices) == busiest, IMG_DEV, counts)
    slots = jnp.arange(IMG_DEV)
    return (slots[None, :] < counts[:, None]).astype(jnp.int32).reshape(IMAGES)


def with_ends(entries, own_key, least, top_value):
    dims = entries.shape
    spot = [jax.random.randint(jax.random.fold_in(own_key, axis), (), 0, dims[axis]) for axis in range(len(dims))]
    entries = entries.at[tuple(spot)].set(least)
    longest = dims.index(max(dims))
    spot[longest] = (spot[longest] + 1) % dims[longest]
    return entries.at[tuple(spot)].set(top_value)


def with_spikes(array, own_key, source, target, parts, factor):
    def block_of(position):
        return (jnp.arange(array.shape[position]) // (array.shape[position] // parts)).reshape((-1,) + (1,) * (array.ndim - 1 - position))

    near = jax.random.permutation(own_key, parts)[block_of(target)]
    second = (block_of(target) + parts // 2) % parts
    return jnp.where((block_of(source) == near) | (block_of(source) == second), factor * array, array)


def level_of(key, shape, cuts, low, top_value):
    loudness, own = 1.0, jax.random.fold_in(key, 6)
    for dim, shards_of in cuts:
        heights = jnp.exp(jax.random.uniform(jax.random.fold_in(own, dim), (shards_of,), jnp.float32, low / len(cuts), top_value / len(cuts)))
        loudness = loudness * jnp.repeat(heights, shape[dim] // shards_of).reshape([-1 if axis == dim else 1 for axis in range(len(shape))])
    return loudness


def scatter_about(stream_key, extent, deviation, limit, shards=(), held_as=jnp.bfloat16):
    loudness = level_of(stream_key, extent, shards, -0.22, 0.18) if shards else 1.0
    array = jax.random.normal(stream_key, extent, jnp.float32) * deviation * loudness
    return jnp.minimum(jnp.maximum(array, -limit), limit).astype(held_as)


def heavy_noise(own_key, shape, deviation, bound, shards, heavy, kind=jnp.bfloat16):
    array = deviation * jax.random.normal(own_key, shape, jnp.float32)
    if shards:
        array = array * level_of(own_key, shape, shards, -0.22, 0.18)
    return jnp.clip(with_spikes(array, jax.random.fold_in(own_key, 3), *heavy), -bound, bound).astype(kind)


def setup_inputs(seed: int = 0) -> dict:
    streams_of = jax.random.split(jax.random.key(seed), 18)
    images = heavy_noise(streams_of[0], (IMAGES, SIDE, SIDE, C), 1.0, 6.0, ((0, 32),), (0, 3, 32, 2.75))
    first_gain = jnp.clip(1.0 + 0.18 * jax.random.normal(streams_of[1], (C,), jnp.float32), 0.099609375, 1.8984375).astype(jnp.bfloat16)
    first_shift = scatter_about(streams_of[2], (C,), 0.3, 1.75, ((0, 32),))
    joint_weight = scatter_about(streams_of[3], (C, 3 * C), C ** -0.5, 0.25, ((0, 32),))
    joint_bias = scatter_about(streams_of[4], (2, C), 0.5, 3.0, ((1, 32),))
    output_weight = scatter_about(streams_of[5], (C, C), (C // 4) ** -0.5, 0.5, ((0, 32),))
    output_bias = scatter_about(streams_of[6], (C,), 0.3, 1.75, ((0, 32),))
    second_gain = jnp.clip(1.0 + 0.18 * jax.random.normal(streams_of[7], (C,), jnp.float32), 0.099609375, 1.8984375).astype(jnp.bfloat16)
    second_shift = scatter_about(streams_of[8], (C,), 0.3, 1.75, ((0, 32),))
    expand_weight = scatter_about(streams_of[9], (C, EXPAND), C ** -0.5, 0.25, ((0, 32),))
    expand_bias = scatter_about(streams_of[10], (EXPAND,), 0.5, 3.0, ((0, 32),))
    reduce_weight = scatter_about(streams_of[11], (EXPAND, C), EXPAND ** -0.5, 0.125, ((0, 32),))
    reduce_bias = scatter_about(streams_of[12], (C,), 0.3, 1.75, ((0, 32),))
    bias_table = draw_bias_table(jax.random.fold_in(streams_of[17], 71), 0)
    regions = with_ends(jax.random.randint(streams_of[14], (SIDE, SIDE), 0, REGIONS), jax.random.fold_in(streams_of[14], 1), 0, REGIONS - 1).astype(jnp.int32)
    live_slots = draw_live_slots(jax.random.fold_in(streams_of[17], 71), 0)
    cotangent = scatter_about(streams_of[16], (IMAGES, SIDE, SIDE, C), 1.0, 6.0, ((0, 32),))
    return dict(images=images, first_gain=first_gain, first_shift=first_shift, joint_weight=joint_weight, joint_bias=joint_bias, output_weight=output_weight, output_bias=output_bias, second_gain=second_gain, second_shift=second_shift, expand_weight=expand_weight, expand_bias=expand_bias, reduce_weight=reduce_weight, reduce_bias=reduce_bias, bias_table=bias_table, regions=regions, live_slots=live_slots, cotangent=cotangent)


epsilon = 1e-05
exact_mode = lax.Precision.HIGHEST

@jax.custom_vjp
def low(v):
    return lax.optimization_barrier(v.astype(jnp.bfloat16)).astype(jnp.float32)

@jax.custom_vjp
def low_back(v):
    return v

def low_keep(v):
    return (low(v), None)

def low_pass(kept, grad):
    return (grad,)

def back_keep(v):
    return (v, None)

def back_low(kept, grad):
    return (low(grad),)
low.defvjp(low_keep, low_pass)
low_back.defvjp(back_keep, back_low)

def norm_rows(values, gains, offset):
    center = lax.optimization_barrier(jnp.mean(values, axis=-1, keepdims=True))
    centred = values - center
    spread = lax.optimization_barrier(jnp.mean(centred * centred, axis=-1, keepdims=True))
    return centred * lax.rsqrt(spread + epsilon) * gains + offset

def windows_of(field):
    count = field.shape[0]
    width = field.shape[-1]
    rolled = jnp.roll(field, (-SHIFT, -SHIFT), axis=(1, 2))
    parted = rolled.reshape(count, SIDE // WIN, WIN, SIDE // WIN, WIN, width)
    return parted.transpose(0, 1, 3, 2, 4, 5).reshape(count * PANES, WIN * WIN, width)

def images_of(panes):
    count = panes.shape[0] // PANES
    width = panes.shape[-1]
    parted = panes.reshape(count, SIDE // WIN, SIDE // WIN, WIN, WIN, width).transpose(0, 1, 3, 2, 4, 5)
    return jnp.roll(parted.reshape(count, SIDE, SIDE, width), (SHIFT, SHIFT), axis=(1, 2))

def relative_index():
    cells = jnp.arange(WIN * WIN, dtype=jnp.int32)
    down = cells // WIN
    across = cells % WIN
    return (down[:, None] - down[None, :] + WIN - 1) * (2 * WIN - 1) + (across[:, None] - across[None, :] + WIN - 1)

def pane_mask(regions):
    labels = windows_of(regions[None, :, :, None])[:, :, 0]
    return jnp.where(labels[:, :, None] == labels[:, None, :], 0.0, -100.0).astype(jnp.float32)

def block_forward(params, group, mask):
    first_gain, first_shift, joint_weight, joint_bias, output_weight, output_bias, second_gain, second_shift, expand_weight, expand_bias, reduce_weight, reduce_bias, bias_table = params
    count = group.shape[0]
    normed = low(norm_rows(group, first_gain, first_shift)).reshape(-1, C)
    joint_add = jnp.concatenate([joint_bias[0], jnp.zeros((C,), jnp.float32), joint_bias[1]])
    joint = jnp.dot(normed, joint_weight, precision=exact_mode, preferred_element_type=jnp.float32) + joint_add
    joint = low(low_back(joint))
    panes = windows_of(joint.reshape(count, SIDE, SIDE, 3 * C))
    split_heads = panes.reshape(-1, WIN * WIN, 3, HEADS, HEAD_DIM).transpose(2, 0, 3, 1, 4)
    queries, keys, values = (split_heads[0], split_heads[1], split_heads[2])
    pair_bias = bias_table[relative_index()].transpose(2, 0, 1)
    scores = jnp.einsum('nhid,nhjd->nhij', queries, keys, precision=exact_mode) * HEAD_DIM ** (-0.5)
    scores = scores.reshape(count, PANES, HEADS, WIN * WIN, WIN * WIN) + pair_bias[None, None] + mask[None, :, None]
    scores = low_back(scores)
    probs = low(jax.nn.softmax(scores, axis=-1))
    grouped = values.reshape(count, PANES, HEADS, WIN * WIN, HEAD_DIM)
    mixed = jnp.einsum('bphij,bphjd->bpihd', probs, grouped, precision=exact_mode)
    mixed = low(low_back(mixed.reshape(-1, C)))
    projected = jnp.dot(mixed, output_weight, precision=exact_mode, preferred_element_type=jnp.float32) + output_bias
    projected = low_back(projected)
    residual = group + images_of(projected.reshape(-1, WIN * WIN, C))
    second = low(norm_rows(residual, second_gain, second_shift)).reshape(-1, C)
    hidden = jnp.dot(second, expand_weight, precision=exact_mode, preferred_element_type=jnp.float32) + expand_bias
    hidden = low_back(hidden)
    active = low(jax.nn.gelu(hidden, approximate=False))
    reduced = jnp.dot(active, reduce_weight, precision=exact_mode, preferred_element_type=jnp.float32) + reduce_bias
    reduced = low_back(reduced)
    return residual + reduced.reshape(residual.shape)

def reference(images, first_gain, first_shift, joint_weight, joint_bias, output_weight, output_bias, second_gain, second_shift, expand_weight, expand_bias, reduce_weight, reduce_bias, bias_table, regions, live_slots, cotangent):
    params = tuple((value.astype(jnp.float32) for value in (first_gain, first_shift, joint_weight, joint_bias, output_weight, output_bias, second_gain, second_shift, expand_weight, expand_bias, reduce_weight, reduce_bias, bias_table)))
    groups = images.astype(jnp.float32).reshape(N_DP, IMG_DEV, SIDE, SIDE, C)
    mask = pane_mask(regions)

    def whole(params, groups):
        stepper = jax.checkpoint(lambda group: block_forward(params, group, mask))
        return lax.map(stepper, groups)
    outputs, pull = jax.vjp(whole, params, groups)
    upstream = cotangent.astype(jnp.float32) * live_slots.astype(jnp.float32)[:, None, None, None]
    param_grads, group_grads = pull(upstream.reshape(groups.shape))
    return (outputs.reshape(images.shape).astype(jnp.bfloat16), group_grads.reshape(images.shape).astype(jnp.bfloat16), param_grads[0], param_grads[1], param_grads[2], param_grads[3], param_grads[4], param_grads[5], param_grads[6], param_grads[7], param_grads[8], param_grads[9], param_grads[10], param_grads[11], param_grads[12])
```

```python
import functools

import jax
import jax.numpy as jnp
from jax import lax
from jax.experimental import pallas as pl
from jax.experimental.pallas import tpu as pltpu
from jax.sharding import PartitionSpec as P

C = 512
HEADS = 16
HEAD_DIM = 32
EXPAND = 2048
WIN = 7
SIDE = 14
SHIFT = 3
PANES = 4
RANKS = 32

epsilon = 1e-05
exact_mode = lax.Precision.HIGHEST


def norm_rows(values, gains, offset):
    center = jnp.mean(values, axis=-1, keepdims=True)
    centred = values - center
    spread = jnp.mean(centred * centred, axis=-1, keepdims=True)
    return centred * lax.rsqrt(spread + epsilon) * gains + offset


def exact_gelu(values):
    return jax.nn.gelu(values, approximate=False)


def windows_of(field):
    count = field.shape[0]
    width = field.shape[-1]
    rolled = jnp.roll(field, (-SHIFT, -SHIFT), axis=(1, 2))
    parted = rolled.reshape(count, SIDE // WIN, WIN, SIDE // WIN, WIN, width)
    return parted.transpose(0, 1, 3, 2, 4, 5).reshape(count * PANES, WIN * WIN, width)


def images_of(panes):
    count = panes.shape[0] // PANES
    width = panes.shape[-1]
    parted = panes.reshape(count, SIDE // WIN, SIDE // WIN, WIN, WIN, width).transpose(
        0, 1, 3, 2, 4, 5
    )
    return jnp.roll(parted.reshape(count, SIDE, SIDE, width), (SHIFT, SHIFT), axis=(1, 2))


def relative_index():
    cells = jnp.arange(WIN * WIN, dtype=jnp.int32)
    down = cells // WIN
    across = cells % WIN
    return (down[:, None] - down[None, :] + WIN - 1) * (2 * WIN - 1) + (
        across[:, None] - across[None, :] + WIN - 1
    )


def pane_mask(regions):
    labels = windows_of(regions[None, :, :, None])[:, :, 0]
    return jnp.where(labels[:, :, None] == labels[:, None, :], 0.0, -100.0).astype(jnp.float32)


def heads_of(panes):
    count = panes.shape[0]
    split_heads = panes.reshape(count, WIN * WIN, 3, HEADS, HEAD_DIM).transpose(2, 0, 3, 1, 4)
    return (split_heads[0], split_heads[1], split_heads[2])


def pane_scores(queries, keys, pair_bias, mask):
    count = queries.shape[0]
    raw = jnp.einsum(
        "nhid,nhjd->nhij", queries, keys, preferred_element_type=jnp.float32
    ) * HEAD_DIM ** (-0.5)
    raw = (
        raw.reshape(count // PANES, PANES, HEADS, WIN * WIN, WIN * WIN)
        + pair_bias[None, None]
        + mask[None, :, None]
    )
    return raw.reshape(count, HEADS, WIN * WIN, WIN * WIN)


def forward_pass(slab, full, pair_bias, mask):
    (
        first_gain,
        first_shift,
        joint_weight,
        joint_bias,
        output_weight,
        output_bias,
        second_gain,
        second_shift,
        expand_weight,
        expand_bias,
        reduce_weight,
        reduce_bias,
    ) = full
    count = slab.shape[0]
    source = slab.astype(jnp.float32)
    normed = norm_rows(source, first_gain.astype(jnp.float32), first_shift.astype(jnp.float32))
    normed = normed.astype(jnp.bfloat16).reshape(-1, C)
    joint_add = jnp.concatenate(
        [
            joint_bias[0].astype(jnp.float32),
            jnp.zeros((C,), jnp.float32),
            joint_bias[1].astype(jnp.float32),
        ]
    )
    joint = (jnp.dot(normed, joint_weight, preferred_element_type=jnp.float32) + joint_add).astype(
        jnp.bfloat16
    )
    panes = windows_of(joint.reshape(count, SIDE, SIDE, 3 * C))
    queries, keys, values = heads_of(panes)
    scores = pane_scores(queries, keys, pair_bias, mask)
    log_totals = jax.nn.logsumexp(scores, axis=-1, keepdims=True)
    probs = jnp.exp(scores - log_totals).astype(jnp.bfloat16)
    mixed = jnp.einsum("nhij,nhjd->nihd", probs, values, preferred_element_type=jnp.float32)
    mixed = mixed.astype(jnp.bfloat16).reshape(-1, C)
    projected = jnp.dot(
        mixed, output_weight, preferred_element_type=jnp.float32
    ) + output_bias.astype(jnp.float32)
    residual = source + images_of(projected.reshape(-1, WIN * WIN, C))
    second = norm_rows(residual, second_gain.astype(jnp.float32), second_shift.astype(jnp.float32))
    second = second.astype(jnp.bfloat16).reshape(-1, C)
    hidden = jnp.dot(
        second, expand_weight, preferred_element_type=jnp.float32
    ) + expand_bias.astype(jnp.float32)
    active = exact_gelu(hidden).astype(jnp.bfloat16)
    reduced = jnp.dot(
        active, reduce_weight, preferred_element_type=jnp.float32
    ) + reduce_bias.astype(jnp.float32)
    output = residual + reduced.reshape(residual.shape)
    kept = (normed, panes, log_totals, mixed, residual, second, hidden, active)
    return (output.astype(jnp.bfloat16), kept)


def backward_pass(slab, upstream, full, kept, pair_bias, mask, onehot):
    (
        first_gain,
        first_shift,
        joint_weight,
        joint_bias,
        output_weight,
        output_bias,
        second_gain,
        second_shift,
        expand_weight,
        expand_bias,
        reduce_weight,
        reduce_bias,
    ) = full
    normed, panes, log_totals, mixed, residual, second, hidden, active = kept
    upstream_low = upstream.reshape(-1, C).astype(jnp.bfloat16)
    reduce_weight_grad = jnp.einsum(
        "tc,tf->cf", active, upstream_low, preferred_element_type=jnp.float32
    )
    reduce_bias_grad = jnp.sum(upstream_low.astype(jnp.float32), axis=0)
    active_grad = jnp.einsum(
        "tf,cf->tc", upstream_low, reduce_weight, preferred_element_type=jnp.float32
    )
    hidden_grad = jax.vjp(exact_gelu, hidden)[1](active_grad)[0].astype(jnp.bfloat16)
    expand_weight_grad = jnp.einsum(
        "tc,tf->cf", second, hidden_grad, preferred_element_type=jnp.float32
    )
    expand_bias_grad = jnp.sum(hidden_grad.astype(jnp.float32), axis=0)
    second_grad = jnp.einsum(
        "tf,cf->tc", hidden_grad, expand_weight, preferred_element_type=jnp.float32
    )
    second_pull = jax.vjp(
        norm_rows, residual, second_gain.astype(jnp.float32), second_shift.astype(jnp.float32)
    )[1]
    residual_grad, second_gain_grad, second_shift_grad = second_pull(
        second_grad.reshape(residual.shape)
    )
    residual_grad = residual_grad + upstream
    projected_grad = windows_of(residual_grad).reshape(-1, C).astype(jnp.bfloat16)
    output_weight_grad = jnp.einsum(
        "tc,tf->cf", mixed, projected_grad, preferred_element_type=jnp.float32
    )
    output_bias_grad = jnp.sum(projected_grad.astype(jnp.float32), axis=0)
    mixed_grad = jnp.einsum(
        "tf,cf->tc", projected_grad, output_weight, preferred_element_type=jnp.float32
    )
    mixed_grad = mixed_grad.astype(jnp.bfloat16).reshape(-1, WIN * WIN, HEADS, HEAD_DIM)
    queries, keys, values = heads_of(panes)
    scores = pane_scores(queries, keys, pair_bias, mask)
    probs = jnp.exp(scores - log_totals)
    probs_low = probs.astype(jnp.bfloat16)
    values_grad = jnp.einsum(
        "nhij,nihd->njhd", probs_low, mixed_grad, preferred_element_type=jnp.float32
    )
    probs_grad = jnp.einsum(
        "nihd,nhjd->nhij", mixed_grad, values, preferred_element_type=jnp.float32
    )
    scores_grad = probs * (probs_grad - jnp.sum(probs_grad * probs, axis=-1, keepdims=True))
    scores_grad = scores_grad.astype(jnp.bfloat16)
    table_part = jnp.sum(scores_grad, axis=0, dtype=jnp.float32).reshape(
        HEADS, WIN * WIN * WIN * WIN
    )
    table_grad = jnp.dot(
        table_part, onehot, precision=exact_mode, preferred_element_type=jnp.float32
    ).T
    scale = HEAD_DIM ** (-0.5)
    queries_grad = (
        jnp.einsum("nhij,nhjd->nihd", scores_grad, keys, preferred_element_type=jnp.float32) * scale
    )
    keys_grad = (
        jnp.einsum("nhij,nhid->njhd", scores_grad, queries, preferred_element_type=jnp.float32)
        * scale
    )
    panes_grad = jnp.stack([queries_grad, keys_grad, values_grad], axis=2).reshape(
        -1, WIN * WIN, 3 * C
    )
    joint_grad = images_of(panes_grad).reshape(-1, 3 * C).astype(jnp.bfloat16)
    joint_weight_grad = jnp.einsum(
        "tc,tf->cf", normed, joint_grad, preferred_element_type=jnp.float32
    )
    column_sums = jnp.sum(joint_grad.astype(jnp.float32), axis=0)
    joint_bias_grad = jnp.stack([column_sums[:C], column_sums[2 * C :]])
    normed_grad = jnp.einsum(
        "tf,cf->tc", joint_grad, joint_weight, preferred_element_type=jnp.float32
    )
    first_pull = jax.vjp(
        norm_rows,
        slab.astype(jnp.float32),
        first_gain.astype(jnp.float32),
        first_shift.astype(jnp.float32),
    )[1]
    source_grad, first_gain_grad, first_shift_grad = first_pull(normed_grad.reshape(residual.shape))
    input_grad = (residual_grad + source_grad).astype(jnp.bfloat16)
    grads = (
        first_gain_grad,
        first_shift_grad,
        joint_weight_grad,
        joint_bias_grad,
        output_weight_grad,
        output_bias_grad,
        second_gain_grad,
        second_shift_grad,
        expand_weight_grad,
        expand_bias_grad,
        reduce_weight_grad,
        reduce_bias_grad,
    )
    return (input_grad, grads, table_grad)


MESH = pl.DeviceIdType.MESH


def place():
    me = lax.axis_index("dp")
    return me, me // 8, (me // 4) % 2, (me // 2) % 2, me % 2


def rank_of(z, y, x, c):
    return z * 8 + y * 4 + x * 2 + c


def greet(peers):
    barrier = pltpu.get_barrier_semaphore()
    for peer in peers:
        pl.semaphore_signal(barrier, inc=1, device_id=(peer,), device_id_type=MESH)
    pl.semaphore_wait(barrier, len(peers))


def flip(z, k):
    low, high = z % 2, z // 2
    if k % 2:
        low = 1 - low
    if k // 2:
        high = 1 - high
    return high * 2 + low


def gather_kernel(groups, *refs):
    shards = refs[:groups]
    fulls = refs[groups : 2 * groups]
    local, send, recv = refs[2 * groups :]
    me, z, y, x, c = place()
    peer_x = rank_of(z, y, 1 - x, c)
    peer_y = rank_of(z, 1 - y, x, c)
    mate = rank_of(z, y, x, 1 - c)
    peers_z = [rank_of(flip(z, k), y, x, c) for k in (1, 2, 3)]
    greet([mate, peer_x, peer_y] + peers_z)

    def copy(group, lane, source, owner, target):
        return pltpu.make_async_remote_copy(
            src_ref=source,
            dst_ref=fulls[group].at[owner],
            send_sem=send.at[group, lane],
            recv_sem=recv.at[group, lane],
            device_id=(target,),
            device_id_type=MESH,
        )

    def column(k, dy, dx):
        return rank_of(flip(z, k), 1 - y if dy else y, 1 - x if dx else x, c)

    def incoming(group, lane):
        return copy(group, lane, shards[group], me, mate)

    started = []
    keep = []

    def push(group, lane, source, owner, target):
        made = copy(group, lane, source, owner, target)
        made.start()
        started.append(made)

    for group in range(groups):
        own = shards[group]
        for k in (1, 2, 3):
            push(group, k - 1, own, me, peers_z[k - 1])
        push(group, 3, own, me, peer_x)
        push(group, 7, own, me, peer_y)
        push(group, 15, own, me, mate)
        made = pltpu.make_async_copy(own, fulls[group].at[me], local.at[group])
        made.start()
        keep.append(made)
    for group in range(groups):
        full = fulls[group]
        for k in (1, 2, 3):
            incoming(group, k - 1).wait_recv()
            owner = column(k, 0, 0)
            push(group, 3 + k, full.at[owner], owner, peer_x)
            push(group, 7 + k, full.at[owner], owner, peer_y)
            push(group, 15 + k, full.at[owner], owner, mate)
        for k in range(4):
            incoming(group, 3 + k).wait_recv()
            owner = column(k, 0, 1)
            if k % 2 == 0:
                push(group, 11 + k, full.at[owner], owner, peer_y)
            push(group, 15 + 4 + k, full.at[owner], owner, mate)
            incoming(group, 7 + k).wait_recv()
            owner = column(k, 1, 0)
            if k % 2 == 1:
                push(group, 11 + k, full.at[owner], owner, peer_x)
            push(group, 15 + 8 + k, full.at[owner], owner, mate)
        for k in range(4):
            incoming(group, 11 + k).wait_recv()
            owner = column(k, 1, 1)
            push(group, 15 + 12 + k, full.at[owner], owner, mate)
    for group in range(groups):
        for lane in range(15, 31):
            incoming(group, lane).wait_recv()
    for made in started:
        made.wait_send()
    for made in keep:
        made.wait()


def gather_all(*shards):
    count = len(shards)
    return pl.pallas_call(
        functools.partial(gather_kernel, count),
        out_shape=[jax.ShapeDtypeStruct((32,) + s.shape, s.dtype) for s in shards],
        in_specs=[pl.BlockSpec(memory_space=pl.ANY)] * count,
        out_specs=[pl.BlockSpec(memory_space=pl.ANY)] * count,
        scratch_shapes=[
            pltpu.SemaphoreType.DMA((count,)),
            pltpu.SemaphoreType.DMA((count, 31)),
            pltpu.SemaphoreType.DMA((count, 31)),
        ],
        compiler_params=pltpu.CompilerParams(collective_id=0, has_side_effects=True),
        name="gather_shards",
    )(*shards)


def reduce_kernel(groups, chunks, *refs):
    parts = refs[:groups]
    sums_in = refs[groups]
    outs = refs[groups + 1 : 2 * groups + 1]
    sums_out = refs[2 * groups + 1]
    rest = refs[2 * groups + 2 :]
    acc, rc, r1x, r1y, r2x, r2y, rz = (rest[i * groups : (i + 1) * groups] for i in range(7))
    vec, vecs, local, send, recv, vsend, vrecv = rest[7 * groups :]
    me, z, y, x, c = place()
    peer_x = rank_of(z, y, 1 - x, c)
    peer_y = rank_of(z, 1 - y, x, c)
    mate = rank_of(z, y, x, 1 - c)
    peers_z = [rank_of(flip(z, k), y, x, c) for k in (1, 2, 3)]
    greet([mate, peer_x, peer_y] + peers_z)
    started = []

    def copy(source, target_ref, sems, index, target):
        return pltpu.make_async_remote_copy(
            src_ref=source,
            dst_ref=target_ref,
            send_sem=sems[0].at[index],
            recv_sem=sems[1].at[index],
            device_id=(target,),
            device_id_type=MESH,
        )

    def push(*what):
        made = copy(*what)
        made.start()
        started.append(made)
        return made

    wide = (send, recv)
    slim = (vsend, vrecv)
    spans = []
    first = {}
    mine = {}
    for group, count in enumerate(chunks):
        rows = parts[group].shape[-2] // count
        for index in range(count):
            spans.append((group, index * rows, rows))
    for number, (group, start, rows) in enumerate(spans):
        cut = pl.ds(start, rows)
        first[number] = push(
            parts[group].at[:, :, :, 1 - c, cut], rc[group].at[:, :, :, cut], wide, (number, 0), mate
        )
        made = pltpu.make_async_copy(
            parts[group].at[:, :, :, c, cut], acc[group].at[:, :, :, cut], local.at[number]
        )
        made.start()
        mine[number] = made
    hop = push(sums_in, vecs.at[0], slim, 0, mate)
    hop.wait_recv()
    vec[0] = sums_in[...] + vecs[0]
    hop = push(vec.at[0], vecs.at[1], slim, 1, peer_x)

    def add(into, where, other):
        into[where] = (into[where].astype(jnp.float32) + other.astype(jnp.float32)).astype(jnp.bfloat16)

    second = {}
    for number, (group, start, rows) in enumerate(spans):
        cut = pl.ds(start, rows)
        mine[number].wait()
        first[number].wait_recv()
        a = acc[group]
        for zz in range(4):
            for yy in range(2):
                for xx in range(2):
                    add(a, (zz, yy, xx, cut), rc[group][zz, yy, xx, cut])
        second[number] = (
            push(a.at[0:2, :, 1 - x, cut], r1x[group].at[:, :, cut], wide, (number, 1), peer_x),
            push(a.at[2:4, 1 - y, :, cut], r1y[group].at[:, :, cut], wide, (number, 2), peer_y),
        )
    hop.wait_recv()
    vec[1] = vec[0] + vecs[1]
    hop = push(vec.at[1], vecs.at[2], slim, 2, peer_y)
    third = {}
    for number, (group, start, rows) in enumerate(spans):
        cut = pl.ds(start, rows)
        for made in second[number]:
            made.wait_recv()
        a = acc[group]
        for zz in range(2):
            for other in range(2):
                add(a, (zz, other, x, cut), r1x[group][zz, other, cut])
                add(a, (2 + zz, y, other, cut), r1y[group][zz, other, cut])
        third[number] = (
            push(a.at[0:2, 1 - y, x, cut], r2y[group].at[:, cut], wide, (number, 3), peer_y),
            push(a.at[2:4, y, 1 - x, cut], r2x[group].at[:, cut], wide, (number, 4), peer_x),
        )
    hop.wait_recv()
    vec[2] = vec[1] + vecs[2]
    hops = [push(vec.at[2], vecs.at[2 + k], slim, 2 + k, peers_z[k - 1]) for k in (1, 2, 3)]
    fourth = {}
    for number, (group, start, rows) in enumerate(spans):
        cut = pl.ds(start, rows)
        for made in third[number]:
            made.wait_recv()
        a = acc[group]
        for zz in range(2):
            add(a, (zz, y, x, cut), r2y[group][zz, cut])
            add(a, (2 + zz, y, x, cut), r2x[group][zz, cut])
        fourth[number] = [
            push(
                a.at[flip(z, k), y, x, cut],
                rz[group].at[k - 1, cut],
                wide,
                (number, 4 + k),
                peers_z[k - 1],
            )
            for k in (1, 2, 3)
        ]
    for number, (group, start, rows) in enumerate(spans):
        cut = pl.ds(start, rows)
        total = acc[group][z, y, x, cut].astype(jnp.float32)
        for k in (1, 2, 3):
            fourth[number][k - 1].wait_recv()
            total += rz[group][k - 1, cut].astype(jnp.float32)
        outs[group][cut, :] = total
    for made in hops:
        made.wait_recv()
    sums_out[...] = (vec[2] + vecs[3]) + (vecs[4] + vecs[5])
    for made in started:
        made.wait_send()


def reduce_all(parts, sums, chunks, collective_id):
    groups = len(parts)
    rows = [p.shape[1] for p in parts]
    number = sum(chunks)
    scratch = [pltpu.VMEM((4, 2, 2, r, C), jnp.bfloat16) for r in rows]
    scratch += [pltpu.VMEM((4, 2, 2, r, C), jnp.bfloat16) for r in rows]
    scratch += [pltpu.VMEM((2, 2, r, C), jnp.bfloat16) for r in rows]
    scratch += [pltpu.VMEM((2, 2, r, C), jnp.bfloat16) for r in rows]
    scratch += [pltpu.VMEM((2, r, C), jnp.bfloat16) for r in rows]
    scratch += [pltpu.VMEM((2, r, C), jnp.bfloat16) for r in rows]
    scratch += [pltpu.VMEM((3, r, C), jnp.bfloat16) for r in rows]
    scratch += [
        pltpu.VMEM((3,) + sums.shape, jnp.float32),
        pltpu.VMEM((6,) + sums.shape, jnp.float32),
        pltpu.SemaphoreType.DMA((number,)),
        pltpu.SemaphoreType.DMA((number, 8)),
        pltpu.SemaphoreType.DMA((number, 8)),
        pltpu.SemaphoreType.DMA((6,)),
        pltpu.SemaphoreType.DMA((6,)),
    ]
    return pl.pallas_call(
        functools.partial(reduce_kernel, groups, chunks),
        out_shape=[jax.ShapeDtypeStruct((r, C), jnp.float32) for r in rows]
        + [jax.ShapeDtypeStruct(sums.shape, jnp.float32)],
        in_specs=[pl.BlockSpec(memory_space=pl.ANY)] * groups
        + [pl.BlockSpec(memory_space=pltpu.VMEM)],
        out_specs=[pl.BlockSpec(memory_space=pltpu.VMEM)] * (groups + 1),
        scratch_shapes=scratch,
        compiler_params=pltpu.CompilerParams(
            collective_id=collective_id, has_side_effects=True, vmem_limit_bytes=60 << 20
        ),
        name="reduce_shards",
    )(*[p.reshape(4, 2, 2, 2, p.shape[1], C) for p in parts], sums)


def pack_shards(joint_weight, output_weight, expand_weight, reduce_weight, vectors):
    row = jnp.concatenate([v.reshape(-1) for v in vectors])
    tail = jnp.zeros((16 * C - row.shape[0],), row.dtype)
    near = jnp.concatenate(
        [joint_weight[:, i * C : (i + 1) * C] for i in range(3)]
        + [output_weight, jnp.concatenate([row, tail]).reshape(16, C)],
        axis=0,
    )
    far = jnp.concatenate(
        [expand_weight[:, i * C : (i + 1) * C] for i in range(4)] + [reduce_weight], axis=0
    )
    return near, far


def split_blocks(packed, width):
    return packed.reshape(RANKS, width, 16, C).transpose(0, 2, 1, 3).reshape(RANKS * 16, width * C)


def join_blocks(grad, width):
    return grad.reshape(RANKS, 16, width, C).transpose(0, 2, 1, 3).reshape(RANKS, width * 16, C)


def regroup(packed, blocks, rows):
    count = packed.shape[0]
    return (
        packed.reshape(RANKS, count // RANKS, blocks, rows, C)
        .transpose(0, 2, 1, 3, 4)
        .reshape(RANKS, blocks * rows * count // RANKS, C)
    )


def ungroup(parts, blocks, ranks):
    rows = parts.shape[1] // blocks
    return (
        parts.reshape(RANKS, blocks, ranks // RANKS, rows * RANKS // ranks, C)
        .transpose(0, 2, 1, 3, 4)
        .reshape(ranks, -1, C)
    )


def on_device(
    images,
    first_gain,
    first_shift,
    joint_weight,
    joint_bias,
    output_weight,
    output_bias,
    second_gain,
    second_shift,
    expand_weight,
    expand_bias,
    reduce_weight,
    reduce_bias,
    bias_table,
    regions,
    live_slots,
    cotangent,
):
    ranks = lax.axis_size("dp")
    me = lax.axis_index("dp")
    cells = relative_index().reshape(-1)
    offsets = jnp.arange((2 * WIN - 1) ** 2, dtype=jnp.int32)
    onehot = (cells[:, None] == offsets[None, :]).astype(jnp.float32)
    pair_bias = jnp.dot(
        onehot,
        bias_table.astype(jnp.float32),
        precision=exact_mode,
        preferred_element_type=jnp.float32,
    ).T.reshape(HEADS, WIN * WIN, WIN * WIN)
    mask = pane_mask(regions)
    upstream = cotangent.astype(jnp.float32) * live_slots.astype(jnp.float32)[:, None, None, None]
    small = (first_gain, first_shift, joint_bias[0], joint_bias[1], output_bias, second_gain, second_shift, reduce_bias, expand_bias)
    if ranks == RANKS:
        near, far = pack_shards(joint_weight, output_weight, expand_weight, reduce_weight, small)
        near, far = gather_all(near, far)
        vec = near[:, 64].reshape(RANKS, C)[:, : 12 * 16]
        vectors = [vec[:, 16 * i : 16 * i + 16].reshape(-1) for i in range(8)] + [vec[:, 128:].reshape(-1)]
        wj = split_blocks(near[:, :48], 3)
        wo = near[:, 48:64].reshape(C, C)
        we = split_blocks(far[:, :64], 4)
        wr = far[:, 64:].reshape(EXPAND, C)
    else:
        wj, wo, we, wr = (lax.all_gather(w, "dp", axis=0, tiled=True) for w in (joint_weight, output_weight, expand_weight, reduce_weight))
        vectors = [lax.all_gather(v, "dp", axis=0, tiled=True) for v in small]
    jb = jnp.stack([vectors[2], vectors[3]])
    full = (vectors[0], vectors[1], wj, jb, wo, vectors[4], vectors[5], vectors[6], we, vectors[8], wr, vectors[7])
    output, kept = forward_pass(images, full, pair_bias, mask)
    input_grad, grads, table_part = backward_pass(images, upstream, full, kept, pair_bias, mask, onehot)
    gsmall = [grads[0], grads[1], grads[3][0], grads[3][1], grads[5], grads[6], grads[7], grads[11], grads[9]]
    if ranks == RANKS:
        flat = jnp.concatenate(gsmall + [table_part.reshape(-1)])
        sums = jnp.concatenate([flat, jnp.zeros((72 * 128 - flat.shape[0],), jnp.float32)]).reshape(72, 128)
        ga = jnp.concatenate([join_blocks(grads[2], 3), grads[4].reshape(RANKS, 16, C)], axis=1).astype(jnp.bfloat16)
        gb = jnp.concatenate([join_blocks(grads[8], 4), grads[10].reshape(RANKS, 64, C)], axis=1).astype(jnp.bfloat16)
        gb, ga, sums = reduce_all([gb, ga], sums, (4, 2), 1)
        sums = sums.reshape(-1)
        own = [lax.dynamic_slice(sums, (C * i + 16 * me,), (16,)) for i in range(8)]
        own.append(lax.dynamic_slice(sums, (C * 8 + 64 * me,), (64,)))
        table = sums[C * 12 : C * 12 + 169 * HEADS].reshape(169, HEADS)
        gj = ga[:48].reshape(3, 16, C).transpose(1, 0, 2).reshape(16, 3 * C)
        go = ga[48:]
        ge = gb[:64].reshape(4, 16, C).transpose(1, 0, 2).reshape(16, 4 * C)
        gr = gb[64:]
    else:
        gj, go, ge, gr = (lax.psum_scatter(g, "dp", scatter_dimension=0, tiled=True) for g in (grads[2], grads[4], grads[8], grads[10]))
        own = [lax.psum_scatter(g, "dp", scatter_dimension=0, tiled=True) for g in gsmall]
        table = lax.psum(table_part, "dp")
    return (
        output,
        input_grad,
        own[0],
        own[1],
        gj,
        jnp.stack([own[2], own[3]]),
        go,
        own[4],
        own[5],
        own[6],
        ge,
        own[8],
        gr,
        own[7],
        table,
    )


def solution(mesh):
    in_specs = (
        P("dp", None, None, None),
        P("dp"),
        P("dp"),
        P("dp", None),
        P(None, "dp"),
        P("dp", None),
        P("dp"),
        P("dp"),
        P("dp"),
        P("dp", None),
        P("dp"),
        P("dp", None),
        P("dp"),
        P(),
        P(),
        P("dp"),
        P("dp", None, None, None),
    )
    out_specs = (
        P("dp", None, None, None),
        P("dp", None, None, None),
        P("dp"),
        P("dp"),
        P("dp", None),
        P(None, "dp"),
        P("dp", None),
        P("dp"),
        P("dp"),
        P("dp"),
        P("dp", None),
        P("dp"),
        P("dp", None),
        P("dp"),
        P(),
    )
    return jax.shard_map(
        on_device, mesh=mesh, in_specs=in_specs, out_specs=out_specs, check_vma=False
    )
```

```python
import functools

import jax
import jax.numpy as jnp
from jax import lax
from jax.experimental import pallas as pl
from jax.experimental.pallas import tpu as pltpu
from jax.sharding import PartitionSpec as P

C = 512
HEADS = 16
HEAD_DIM = 32
EXPAND = 2048
WIN = 7
SIDE = 14
SHIFT = 3
PANES = 4
RANKS = 32

epsilon = 1e-05
exact_mode = lax.Precision.HIGHEST

MESH = pl.DeviceIdType.MESH


def place():
    me = lax.axis_index("dp")
    return me, me // 8, (me // 4) % 2, (me // 2) % 2, me % 2


def rank_of(z, y, x, c):
    return z * 8 + y * 4 + x * 2 + c


def greet(peers):
    barrier = pltpu.get_barrier_semaphore()
    for peer in peers:
        pl.semaphore_signal(barrier, inc=1, device_id=(peer,), device_id_type=MESH)
    pl.semaphore_wait(barrier, len(peers))


def flip(z, k):
    low, high = z % 2, z // 2
    if k % 2:
        low = 1 - low
    if k // 2:
        high = 1 - high
    return high * 2 + low


def gather_kernel(groups, *refs):
    shards = refs[:groups]
    fulls = refs[groups : 2 * groups]
    local, send, recv = refs[2 * groups :]
    me, z, y, x, c = place()
    peer_x = rank_of(z, y, 1 - x, c)
    peer_y = rank_of(z, 1 - y, x, c)
    mate = rank_of(z, y, x, 1 - c)
    peers_z = [rank_of(flip(z, k), y, x, c) for k in (1, 2, 3)]
    greet([mate, peer_x, peer_y] + peers_z)

    def copy(group, lane, source, owner, target):
        return pltpu.make_async_remote_copy(
            src_ref=source,
            dst_ref=fulls[group].at[owner],
            send_sem=send.at[group, lane],
            recv_sem=recv.at[group, lane],
            device_id=(target,),
            device_id_type=MESH,
        )

    def column(k, dy, dx):
        return rank_of(flip(z, k), 1 - y if dy else y, 1 - x if dx else x, c)

    def incoming(group, lane):
        return copy(group, lane, shards[group], me, mate)

    started = []
    keep = []

    def push(group, lane, source, owner, target):
        made = copy(group, lane, source, owner, target)
        made.start()
        started.append(made)

    for group in range(groups):
        own = shards[group]
        for k in (1, 2, 3):
            push(group, k - 1, own, me, peers_z[k - 1])
        push(group, 3, own, me, peer_x)
        push(group, 7, own, me, peer_y)
        push(group, 15, own, me, mate)
        made = pltpu.make_async_copy(own, fulls[group].at[me], local.at[group])
        made.start()
        keep.append(made)
    for group in range(groups):
        full = fulls[group]
        for k in (1, 2, 3):
            incoming(group, k - 1).wait_recv()
            owner = column(k, 0, 0)
            push(group, 3 + k, full.at[owner], owner, peer_x)
            push(group, 7 + k, full.at[owner], owner, peer_y)
            push(group, 15 + k, full.at[owner], owner, mate)
        for k in range(4):
            incoming(group, 3 + k).wait_recv()
            owner = column(k, 0, 1)
            if k % 2 == 0:
                push(group, 11 + k, full.at[owner], owner, peer_y)
            push(group, 15 + 4 + k, full.at[owner], owner, mate)
            incoming(group, 7 + k).wait_recv()
            owner = column(k, 1, 0)
            if k % 2 == 1:
                push(group, 11 + k, full.at[owner], owner, peer_x)
            push(group, 15 + 8 + k, full.at[owner], owner, mate)
        for k in range(4):
            incoming(group, 11 + k).wait_recv()
            owner = column(k, 1, 1)
            push(group, 15 + 12 + k, full.at[owner], owner, mate)
    for group in range(groups):
        for lane in range(15, 31):
            incoming(group, lane).wait_recv()
    for made in started:
        made.wait_send()
    for made in keep:
        made.wait()


def gather_all(*shards):
    count = len(shards)
    return pl.pallas_call(
        functools.partial(gather_kernel, count),
        out_shape=[jax.ShapeDtypeStruct((32,) + s.shape, s.dtype) for s in shards],
        in_specs=[pl.BlockSpec(memory_space=pl.ANY)] * count,
        out_specs=[pl.BlockSpec(memory_space=pl.ANY)] * count,
        scratch_shapes=[
            pltpu.SemaphoreType.DMA((count,)),
            pltpu.SemaphoreType.DMA((count, 31)),
            pltpu.SemaphoreType.DMA((count, 31)),
        ],
        compiler_params=pltpu.CompilerParams(collective_id=0, has_side_effects=True),
        name="gather_shards",
    )(*shards)


def reduce_kernel(groups, chunks, *refs):
    parts = refs[:groups]
    sums_in = refs[groups]
    outs = refs[groups + 1 : 2 * groups + 1]
    sums_out = refs[2 * groups + 1]
    rest = refs[2 * groups + 2 :]
    acc, rc, r1x, r1y, r2x, r2y, rz = (rest[i * groups : (i + 1) * groups] for i in range(7))
    vec, vecs, local, send, recv, vsend, vrecv = rest[7 * groups :]
    me, z, y, x, c = place()
    peer_x = rank_of(z, y, 1 - x, c)
    peer_y = rank_of(z, 1 - y, x, c)
    mate = rank_of(z, y, x, 1 - c)
    peers_z = [rank_of(flip(z, k), y, x, c) for k in (1, 2, 3)]
    greet([mate, peer_x, peer_y] + peers_z)
    started = []

    def copy(source, target_ref, sems, index, target):
        return pltpu.make_async_remote_copy(
            src_ref=source,
            dst_ref=target_ref,
            send_sem=sems[0].at[index],
            recv_sem=sems[1].at[index],
            device_id=(target,),
            device_id_type=MESH,
        )

    def push(*what):
        made = copy(*what)
        made.start()
        started.append(made)
        return made

    wide = (send, recv)
    slim = (vsend, vrecv)
    spans = []
    first = {}
    mine = {}
    for group, count in enumerate(chunks):
        rows = parts[group].shape[-2] // count
        for index in range(count):
            spans.append((group, index * rows, rows))
    for number, (group, start, rows) in enumerate(spans):
        cut = pl.ds(start, rows)
        first[number] = push(
            parts[group].at[:, :, :, 1 - c, cut], rc[group].at[:, :, :, cut], wide, (number, 0), mate
        )
        made = pltpu.make_async_copy(
            parts[group].at[:, :, :, c, cut], acc[group].at[:, :, :, cut], local.at[number]
        )
        made.start()
        mine[number] = made
    hop = push(sums_in, vecs.at[0], slim, 0, mate)
    hop.wait_recv()
    vec[0] = sums_in[...] + vecs[0]
    hop = push(vec.at[0], vecs.at[1], slim, 1, peer_x)

    def add(into, where, other):
        into[where] = (into[where].astype(jnp.float32) + other.astype(jnp.float32)).astype(jnp.bfloat16)

    second = {}
    for number, (group, start, rows) in enumerate(spans):
        cut = pl.ds(start, rows)
        mine[number].wait()
        first[number].wait_recv()
        a = acc[group]
        for zz in range(4):
            for yy in range(2):
                for xx in range(2):
                    add(a, (zz, yy, xx, cut), rc[group][zz, yy, xx, cut])
        second[number] = (
            push(a.at[0:2, :, 1 - x, cut], r1x[group].at[:, :, cut], wide, (number, 1), peer_x),
            push(a.at[2:4, 1 - y, :, cut], r1y[group].at[:, :, cut], wide, (number, 2), peer_y),
        )
    hop.wait_recv()
    vec[1] = vec[0] + vecs[1]
    hop = push(vec.at[1], vecs.at[2], slim, 2, peer_y)
    third = {}
    for number, (group, start, rows) in enumerate(spans):
        cut = pl.ds(start, rows)
        for made in second[number]:
            made.wait_recv()
        a = acc[group]
        for zz in range(2):
            for other in range(2):
                add(a, (zz, other, x, cut), r1x[group][zz, other, cut])
                add(a, (2 + zz, y, other, cut), r1y[group][zz, other, cut])
        third[number] = (
            push(a.at[0:2, 1 - y, x, cut], r2y[group].at[:, cut], wide, (number, 3), peer_y),
            push(a.at[2:4, y, 1 - x, cut], r2x[group].at[:, cut], wide, (number, 4), peer_x),
        )
    hop.wait_recv()
    vec[2] = vec[1] + vecs[2]
    hops = [push(vec.at[2], vecs.at[2 + k], slim, 2 + k, peers_z[k - 1]) for k in (1, 2, 3)]
    fourth = {}
    for number, (group, start, rows) in enumerate(spans):
        cut = pl.ds(start, rows)
        for made in third[number]:
            made.wait_recv()
        a = acc[group]
        for zz in range(2):
            add(a, (zz, y, x, cut), r2y[group][zz, cut])
            add(a, (2 + zz, y, x, cut), r2x[group][zz, cut])
        fourth[number] = [
            push(
                a.at[flip(z, k), y, x, cut],
                rz[group].at[k - 1, cut],
                wide,
                (number, 4 + k),
                peers_z[k - 1],
            )
            for k in (1, 2, 3)
        ]
    for number, (group, start, rows) in enumerate(spans):
        cut = pl.ds(start, rows)
        total = acc[group][z, y, x, cut].astype(jnp.float32)
        for k in (1, 2, 3):
            fourth[number][k - 1].wait_recv()
            total += rz[group][k - 1, cut].astype(jnp.float32)
        outs[group][cut, :] = total
    for made in hops:
        made.wait_recv()
    sums_out[...] = (vec[2] + vecs[3]) + (vecs[4] + vecs[5])
    for made in started:
        made.wait_send()


def reduce_all(parts, sums, chunks, collective_id):
    groups = len(parts)
    rows = [p.shape[1] for p in parts]
    number = sum(chunks)
    scratch = [pltpu.VMEM((4, 2, 2, r, C), jnp.bfloat16) for r in rows]
    scratch += [pltpu.VMEM((4, 2, 2, r, C), jnp.bfloat16) for r in rows]
    scratch += [pltpu.VMEM((2, 2, r, C), jnp.bfloat16) for r in rows]
    scratch += [pltpu.VMEM((2, 2, r, C), jnp.bfloat16) for r in rows]
    scratch += [pltpu.VMEM((2, r, C), jnp.bfloat16) for r in rows]
    scratch += [pltpu.VMEM((2, r, C), jnp.bfloat16) for r in rows]
    scratch += [pltpu.VMEM((3, r, C), jnp.bfloat16) for r in rows]
    scratch += [
        pltpu.VMEM((3,) + sums.shape, jnp.float32),
        pltpu.VMEM((6,) + sums.shape, jnp.float32),
        pltpu.SemaphoreType.DMA((number,)),
        pltpu.SemaphoreType.DMA((number, 8)),
        pltpu.SemaphoreType.DMA((number, 8)),
        pltpu.SemaphoreType.DMA((6,)),
        pltpu.SemaphoreType.DMA((6,)),
    ]
    return pl.pallas_call(
        functools.partial(reduce_kernel, groups, chunks),
        out_shape=[jax.ShapeDtypeStruct((r, C), jnp.float32) for r in rows]
        + [jax.ShapeDtypeStruct(sums.shape, jnp.float32)],
        in_specs=[pl.BlockSpec(memory_space=pl.ANY)] * groups
        + [pl.BlockSpec(memory_space=pltpu.VMEM)],
        out_specs=[pl.BlockSpec(memory_space=pltpu.VMEM)] * (groups + 1),
        scratch_shapes=scratch,
        compiler_params=pltpu.CompilerParams(
            collective_id=collective_id, has_side_effects=True, vmem_limit_bytes=60 << 20
        ),
        name="reduce_shards",
    )(*[p.reshape(4, 2, 2, 2, p.shape[1], C) for p in parts], sums)


def pack_shards(joint_weight, output_weight, expand_weight, reduce_weight, vectors):
    row = jnp.concatenate([v.reshape(-1) for v in vectors])
    tail = jnp.zeros((16 * C - row.shape[0],), row.dtype)
    near = jnp.concatenate(
        [joint_weight[:, i * C : (i + 1) * C] for i in range(3)]
        + [output_weight, jnp.concatenate([row, tail]).reshape(16, C)],
        axis=0,
    )
    far = jnp.concatenate(
        [expand_weight[:, i * C : (i + 1) * C] for i in range(4)] + [reduce_weight], axis=0
    )
    return near, far

ERFC_SLOPE = 0.4
ERFC_TERMS = (
    0.23192538182549352,
    0.16180412136440986,
    0.4683198256010739,
    -0.3709611648908394,
    0.7091781371622337,
    -0.20026632849062864,
)


def gelu_pair(v):
    bell = jnp.exp(v * v * -0.5)
    t = 1.0 / (1.0 + jnp.abs(v) * (ERFC_SLOPE * 0.5**0.5))
    tail = ERFC_TERMS[5] * 0.5
    for term in ERFC_TERMS[4::-1]:
        tail = tail * t + term * 0.5
    tail = tail * t * bell
    below = jnp.where(v < 0, tail, 1.0 - tail)
    return v * below, below + v * (bell * 0.3989422804014327)


def norm_parts(v):
    center = jnp.mean(v, axis=-1, keepdims=True)
    centred = v - center
    spread = jnp.mean(centred * centred, axis=-1, keepdims=True)
    rate = lax.rsqrt(spread + epsilon)
    return centred * rate, rate


def norm_pull(grad, gain, xhat, rate):
    scaled = grad * gain
    first = jnp.mean(scaled, axis=-1, keepdims=True)
    second = jnp.mean(scaled * xhat, axis=-1, keepdims=True)
    return rate * (scaled - first - xhat * second)


def dot_nn(a, b):
    return lax.dot_general(a, b, (((1,), (0,)), ((), ())), preferred_element_type=jnp.float32)


def dot_nt(a, b):
    return lax.dot_general(a, b, (((1,), (1,)), ((), ())), preferred_element_type=jnp.float32)


def dot_tn(a, b):
    return lax.dot_general(a, b, (((0,), (0,)), ((), ())), preferred_element_type=jnp.float32)


def column_sum(v):
    return jnp.sum(v, axis=0, keepdims=True)


def mlp_kernel(
    res_ref, cot_ref, live_ref, far_ref, gain_ref, shift_ref, ebias_ref, rbias_ref,
    out_ref, rgrad_ref, part_ref, vec_ref, ebg_ref, we_acc, wr_acc,
):
    step = pl.program_id(0)
    rows = res_ref.shape[0]

    @pl.when(step == 0)
    def _():
        we_acc[...] = jnp.zeros_like(we_acc)
        wr_acc[...] = jnp.zeros_like(wr_acc)
        vec_ref[...] = jnp.zeros_like(vec_ref)
        ebg_ref[...] = jnp.zeros_like(ebg_ref)

    res = res_ref[...]
    gain = gain_ref[...]
    xhat, rate = norm_parts(res)
    second = (xhat * gain + shift_ref[...]).astype(jnp.bfloat16)
    upstream = (
        cot_ref[...].astype(jnp.float32).reshape(rows // 16, 16, C) * live_ref[...][None, :, :1]
    ).reshape(rows, C)
    low = upstream.astype(jnp.bfloat16)
    second_t = second.T
    low_t = low.T
    reduced = jnp.zeros((rows, C), jnp.float32)
    pulled = jnp.zeros((rows, C), jnp.float32)
    for b in range(4):
        we = far_ref[:, b * 16 : (b + 1) * 16, :].reshape(C, C)
        wr = far_ref[b * 8 : (b + 1) * 8, 64:128, :].reshape(C, C)
        hidden = dot_nn(second, we) + ebias_ref[:, b * C : (b + 1) * C]
        active, slope = gelu_pair(hidden)
        active = active.astype(jnp.bfloat16)
        reduced += dot_nn(active, wr)
        hgrad = (dot_nt(low, wr) * slope).astype(jnp.bfloat16)
        pulled += dot_nt(hgrad, we)
        wr_acc[b] += dot_nn(low_t, active)
        we_acc[b] += dot_nn(second_t, hgrad)
        ebg_ref[:, b * C : (b + 1) * C] += column_sum(hgrad.astype(jnp.float32))
    out_ref[...] = (res + reduced + rbias_ref[...]).astype(jnp.bfloat16)
    rgrad_ref[...] = upstream + norm_pull(pulled, gain, xhat, rate)
    vec_ref[0:1] += column_sum(pulled * xhat)
    vec_ref[1:2] += column_sum(pulled)
    vec_ref[2:3] += column_sum(low.astype(jnp.float32))

    @pl.when(step == pl.num_programs(0) - 1)
    def _():
        for b in range(4):
            part_ref[:, b * 16 : (b + 1) * 16, :] = we_acc[b].reshape(RANKS, 16, C).astype(jnp.bfloat16)
            part_ref[b * 8 : (b + 1) * 8, 64:128, :] = (
                wr_acc[b].T.reshape(8, 64, C).astype(jnp.bfloat16)
            )


def mlp_block(res, cot, live, far, gain, shift, ebias, rbias, rows=448):
    tokens = res.shape[0]
    fixed = lambda shape: pl.BlockSpec(shape, lambda i: (0,) * len(shape), pipeline_mode=pl.Buffered(1))
    moving = pl.BlockSpec((rows, C), lambda i: (i, 0))
    return pl.pallas_call(
        mlp_kernel,
        grid=(tokens // rows,),
        in_specs=[moving, moving, fixed((16, 128)), fixed((RANKS, 128, C)), fixed((1, C)), fixed((1, C)),
                  fixed((1, EXPAND)), fixed((1, C))],
        out_specs=[moving, moving, fixed((RANKS, 128, C)), fixed((8, C)), fixed((1, EXPAND))],
        out_shape=[
            jax.ShapeDtypeStruct((tokens, C), jnp.bfloat16),
            jax.ShapeDtypeStruct((tokens, C), jnp.float32),
            jax.ShapeDtypeStruct((RANKS, 128, C), jnp.bfloat16),
            jax.ShapeDtypeStruct((8, C), jnp.float32),
            jax.ShapeDtypeStruct((1, EXPAND), jnp.float32),
        ],
        scratch_shapes=[pltpu.VMEM((4, C, C), jnp.float32), pltpu.VMEM((4, C, C), jnp.float32)],
        compiler_params=pltpu.CompilerParams(vmem_limit_bytes=60 << 20, dimension_semantics=("arbitrary",)),
        name="mlp_block",
    )(res, cot, live, far, gain, shift, ebias, rbias)

SPOTS = WIN * WIN
ROWS = SPOTS * 16
QUERY_ROWS = 56
KEY_ROWS = 64
QUAD = 4 * HEAD_DIM
SPAN = 4 * KEY_ROWS
SCALE = HEAD_DIM**-0.5


def spot_of(pane, spot):
    y = lax.rem((pane // 2) * WIN + spot // WIN + SHIFT, SIDE)
    x = lax.rem((pane % 2) * WIN + spot % WIN + SHIFT, SIDE)
    return y, x


def take_pane(pane, source, target):
    for spot in range(SPOTS):
        y, x = spot_of(pane, spot)
        target[spot * 16 : (spot + 1) * 16, :] = source[y, x]


def give_pane(pane, value, target):
    for spot in range(SPOTS):
        y, x = spot_of(pane, spot)
        target[y, x] = value[spot * 16 : (spot + 1) * 16, :]


def put_tiles(target, first, value):
    for tile in range(4):
        target[first + tile, 0:ROWS, :] = value[:, tile * QUAD : (tile + 1) * QUAD]


def get_tiles(source, first):
    return jnp.concatenate([source[first + tile, 0:ROWS, :] for tile in range(4)], axis=1)


def low_half(rows):
    return lax.broadcasted_iota(jnp.int32, (rows, 128), 1) < KEY_ROWS


def by_segment(value, op, neutral):
    low = low_half(value.shape[0])
    tiles = []
    for tile in range(2):
        part = value[:, tile * 128 : (tile + 1) * 128]
        first = op(jnp.where(low, part, neutral), axis=-1, keepdims=True)
        second = op(jnp.where(low, neutral, part), axis=-1, keepdims=True)
        tiles.append(jnp.where(low, first, second))
    return jnp.concatenate(tiles, axis=1)


def head_lanes(rows):
    return lax.broadcasted_iota(jnp.int32, (rows, QUAD), 1) // HEAD_DIM


def spread_heads(tile):
    lanes = head_lanes(KEY_ROWS)
    return jnp.concatenate(
        [jnp.where(lanes == h, tile, jnp.zeros_like(tile)) for h in range(4)], axis=0
    )


def merge_heads(value):
    lanes = head_lanes(KEY_ROWS)
    parts = [value[h * KEY_ROWS : (h + 1) * KEY_ROWS] for h in range(4)]
    return jnp.where(
        lanes < 2, jnp.where(lanes == 0, parts[0], parts[1]), jnp.where(lanes == 2, parts[2], parts[3])
    )


def attend_kernel(
    x_ref, near_ref, bias_ref, mask_ref, gain_ref, shift_ref, jbias_ref, obias_ref,
    joint_ref, probs_ref, mixed_ref, res_ref, window, wide, blend,
):
    pane = pl.program_id(0)

    @pl.when(pane == 0)
    def _():
        wide[...] = jnp.zeros_like(wide)

    take_pane(pane, x_ref, window)
    source = window[...].astype(jnp.float32)
    xhat, _ = norm_parts(source)
    normed = (xhat * gain_ref[...] + shift_ref[...]).astype(jnp.bfloat16)
    for b in range(3):
        weight = near_ref[:, b * 16 : (b + 1) * 16, :].reshape(C, C)
        block = (dot_nn(normed, weight) + jbias_ref[:, b * C : (b + 1) * C]).astype(jnp.bfloat16)
        joint_ref[0, :, b * C : (b + 1) * C] = block
        put_tiles(wide, b * 4, block.astype(jnp.float32))
    mask = mask_ref[0]

    def per_image(m, carry):
        for quad in range(4):
            few, many = pl.ds(m, QUERY_ROWS, stride=16), pl.ds(m, KEY_ROWS, stride=16)
            q = wide[quad, few, :].astype(jnp.bfloat16)
            k = wide[4 + quad, many, :].astype(jnp.bfloat16)
            v = wide[8 + quad, many, :].astype(jnp.bfloat16)
            scores = dot_nt(q, spread_heads(k)) * SCALE + bias_ref[quad] + mask
            peak = by_segment(scores, jnp.max, -jnp.inf)
            powers = jnp.exp(scores - peak)
            total = by_segment(powers, jnp.sum, 0.0)
            probs = (powers * (1.0 / total)).astype(jnp.bfloat16)
            probs_ref[0, m, quad] = probs
            blend[quad, few, :] = dot_nn(probs, spread_heads(v))
        return carry

    lax.fori_loop(0, 16, per_image, 0)
    mixed = get_tiles(blend, 0).astype(jnp.bfloat16)
    mixed_ref[0] = mixed
    projected = dot_nn(mixed, near_ref[:, 48:64, :].reshape(C, C)) + obias_ref[...]
    give_pane(pane, window[...].astype(jnp.float32) + projected, res_ref)


def fixed(shape):
    return pl.BlockSpec(shape, lambda i: (0,) * len(shape), pipeline_mode=pl.Buffered(1))


def attend(x, near, bias, mask, gain, shift, jbias, obias):
    step = lambda shape: pl.BlockSpec((1,) + shape, lambda i: (i,) + (0,) * len(shape))
    return pl.pallas_call(
        attend_kernel,
        grid=(PANES,),
        in_specs=[fixed((SIDE, SIDE, 16, C)), fixed((RANKS, 80, C)), fixed((4, QUERY_ROWS, SPAN)),
                  step((QUERY_ROWS, SPAN)), fixed((1, C)), fixed((1, C)), fixed((1, 3 * C)), fixed((1, C))],
        out_specs=[step((ROWS, 3 * C)), step((16, 4, QUERY_ROWS, SPAN)), step((ROWS, C)),
                   fixed((SIDE, SIDE, 16, C))],
        out_shape=[
            jax.ShapeDtypeStruct((PANES, ROWS, 3 * C), jnp.bfloat16),
            jax.ShapeDtypeStruct((PANES, 16, 4, QUERY_ROWS, SPAN), jnp.bfloat16),
            jax.ShapeDtypeStruct((PANES, ROWS, C), jnp.bfloat16),
            jax.ShapeDtypeStruct((SIDE, SIDE, 16, C), jnp.float32),
        ],
        scratch_shapes=[
            pltpu.VMEM((ROWS, C), jnp.bfloat16),
            pltpu.VMEM((12, KEY_ROWS * 16, QUAD), jnp.float32),
            pltpu.VMEM((4, KEY_ROWS * 16, QUAD), jnp.float32),
        ],
        compiler_params=pltpu.CompilerParams(vmem_limit_bytes=62 << 20, dimension_semantics=("arbitrary",)),
        name="attend",
    )(x, near, bias, mask, gain, shift, jbias, obias)


def attend_back_kernel(
    x_ref, near_ref, joint_ref, probs_ref, mixed_ref, rgrad_ref, gain_ref, shift_ref,
    dx_ref, part_ref, vec_ref, pairs_ref, window, rwindow, wide, blend, turned, wj_acc, wo_acc,
):
    pane = pl.program_id(0)

    @pl.when(pane == 0)
    def _():
        wide[...] = jnp.zeros_like(wide)
        blend[...] = jnp.zeros_like(blend)
        wj_acc[...] = jnp.zeros_like(wj_acc)
        wo_acc[...] = jnp.zeros_like(wo_acc)
        vec_ref[...] = jnp.zeros_like(vec_ref)
        pairs_ref[...] = jnp.zeros_like(pairs_ref)

    take_pane(pane, x_ref, window)
    take_pane(pane, rgrad_ref, rwindow)
    pulled = rwindow[...].astype(jnp.bfloat16)
    wo = near_ref[:, 48:64, :].reshape(C, C)
    wo_acc[...] += dot_tn(mixed_ref[0], pulled)
    vec_ref[0:1] += column_sum(pulled.astype(jnp.float32))
    put_tiles(blend, 0, dot_nt(pulled, wo).astype(jnp.bfloat16).astype(jnp.float32))
    for b in range(3):
        put_tiles(wide, b * 4, joint_ref[0, :, b * C : (b + 1) * C].astype(jnp.float32))

    def per_image(m, carry):
        for quad in range(4):
            few, many = pl.ds(m, QUERY_ROWS, stride=16), pl.ds(m, KEY_ROWS, stride=16)
            q = wide[quad, few, :].astype(jnp.bfloat16)
            k = spread_heads(wide[4 + quad, many, :].astype(jnp.bfloat16))
            v = spread_heads(wide[8 + quad, many, :].astype(jnp.bfloat16))
            pull = blend[quad, few, :].astype(jnp.bfloat16)
            probs = probs_ref[0, m, quad]
            wider = probs.astype(jnp.float32)
            weighted = dot_nt(pull, v) * wider
            sgrad = (weighted - wider * by_segment(weighted, jnp.sum, 0.0)).astype(jnp.bfloat16)
            pairs_ref[quad] += sgrad.astype(jnp.float32)
            turned[quad, few, :] = dot_nn(sgrad, k) * SCALE
            turned[4 + quad, many, :] = merge_heads(dot_tn(sgrad, q)) * SCALE
            turned[8 + quad, many, :] = merge_heads(dot_tn(probs, pull))
        return carry

    lax.fori_loop(0, 16, per_image, 0)
    gain = gain_ref[...]
    xhat, rate = norm_parts(window[...].astype(jnp.float32))
    normed = (xhat * gain + shift_ref[...]).astype(jnp.bfloat16)
    normed_t = normed.T
    total = jnp.zeros((ROWS, C), jnp.float32)
    for b in range(3):
        weight = near_ref[:, b * 16 : (b + 1) * 16, :].reshape(C, C)
        block = get_tiles(turned, b * 4).astype(jnp.bfloat16)
        wj_acc[b] += dot_nn(normed_t, block)
        total += dot_nt(block, weight)
        if b != 1:
            vec_ref[1 + b // 2 : 2 + b // 2] += column_sum(block.astype(jnp.float32))
    vec_ref[3:4] += column_sum(total * xhat)
    vec_ref[4:5] += column_sum(total)
    dx = rwindow[...] + norm_pull(total, gain, xhat, rate)
    give_pane(pane, dx.astype(jnp.bfloat16), dx_ref)

    @pl.when(pane == PANES - 1)
    def _():
        for b in range(3):
            part_ref[:, b * 16 : (b + 1) * 16, :] = wj_acc[b].reshape(RANKS, 16, C).astype(jnp.bfloat16)
        part_ref[:, 48:64, :] = wo_acc[...].reshape(RANKS, 16, C).astype(jnp.bfloat16)


def attend_back(x, near, joint, probs, mixed, rgrad, gain, shift):
    step = lambda shape: pl.BlockSpec((1,) + shape, lambda i: (i,) + (0,) * len(shape))
    return pl.pallas_call(
        attend_back_kernel,
        grid=(PANES,),
        in_specs=[fixed((SIDE, SIDE, 16, C)), fixed((RANKS, 80, C)), step((ROWS, 3 * C)),
                  step((16, 4, QUERY_ROWS, SPAN)), step((ROWS, C)), fixed((SIDE, SIDE, 16, C)),
                  fixed((1, C)), fixed((1, C))],
        out_specs=[fixed((SIDE, SIDE, 16, C)), fixed((RANKS, 64, C)), fixed((8, C)),
                   fixed((4, QUERY_ROWS, SPAN))],
        out_shape=[
            jax.ShapeDtypeStruct((SIDE, SIDE, 16, C), jnp.bfloat16),
            jax.ShapeDtypeStruct((RANKS, 64, C), jnp.bfloat16),
            jax.ShapeDtypeStruct((8, C), jnp.float32),
            jax.ShapeDtypeStruct((4, QUERY_ROWS, SPAN), jnp.float32),
        ],
        scratch_shapes=[
            pltpu.VMEM((ROWS, C), jnp.bfloat16),
            pltpu.VMEM((ROWS, C), jnp.float32),
            pltpu.VMEM((12, KEY_ROWS * 16, QUAD), jnp.float32),
            pltpu.VMEM((4, KEY_ROWS * 16, QUAD), jnp.float32),
            pltpu.VMEM((12, KEY_ROWS * 16, QUAD), jnp.float32),
            pltpu.VMEM((3, C, C), jnp.float32),
            pltpu.VMEM((C, C), jnp.float32),
        ],
        compiler_params=pltpu.CompilerParams(vmem_limit_bytes=62 << 20, dimension_semantics=("arbitrary",)),
        name="attend_back",
    )(x, near, joint, probs, mixed, rgrad, gain, shift)


def pair_tables(bias_table, regions):
    rows, cols = jnp.arange(QUERY_ROWS), jnp.arange(KEY_ROWS)
    real = (rows < SPOTS)[:, None] & (cols < SPOTS)[None, :]
    cells = (
        (rows[:, None] // WIN - cols[None, :] // WIN + WIN - 1) * (2 * WIN - 1)
        + rows[:, None] % WIN - cols[None, :] % WIN + WIN - 1
    )
    cells = jnp.where(real, cells, -1).reshape(-1)
    onehot = (cells[None, :] == jnp.arange((2 * WIN - 1) ** 2)[:, None]).astype(jnp.bfloat16)
    bias = dot_tn(bias_table, onehot).reshape(4, 4, QUERY_ROWS, KEY_ROWS)
    bias = jnp.where((cols < SPOTS)[None, None, None, :], bias, -1e30)
    bias = bias.transpose(0, 2, 1, 3).reshape(4, QUERY_ROWS, SPAN)
    labels = jnp.roll(regions, (-SHIFT, -SHIFT), axis=(0, 1)).reshape(2, WIN, 2, WIN)
    labels = labels.transpose(0, 2, 1, 3).reshape(PANES, SPOTS)
    across = jnp.pad(labels, ((0, 0), (0, QUERY_ROWS - SPOTS)))
    along = jnp.pad(labels, ((0, 0), (0, KEY_ROWS - SPOTS)))
    along = jnp.tile(along, (1, 4))
    mask = jnp.where(across[:, :, None] == along[:, None, :], 0.0, -100.0).astype(jnp.float32)
    return bias, mask, onehot


def table_sums(pairs, onehot):
    heads = pairs.reshape(4, QUERY_ROWS, 4, KEY_ROWS).transpose(0, 2, 1, 3).reshape(HEADS, QUERY_ROWS * KEY_ROWS)
    return lax.dot_general(
        onehot.astype(jnp.float32), heads, (((1,), (1,)), ((), ())),
        precision=exact_mode, preferred_element_type=jnp.float32,
    )

def regroup(packed, blocks, rows):
    count = packed.shape[0] // RANKS
    return (
        packed.reshape(RANKS, count, blocks, rows, C)
        .transpose(0, 2, 1, 3, 4)
        .reshape(RANKS, blocks * rows * count, C)
    )


def ungroup(parts, blocks, ranks):
    rows = parts.shape[1] // blocks
    flat = parts.reshape(RANKS, blocks, rows, C).transpose(1, 0, 2, 3).reshape(blocks, RANKS * rows, C)
    return flat.reshape(blocks, ranks, RANKS * rows // ranks, C).transpose(1, 0, 2, 3)


def on_device(
    images,
    first_gain,
    first_shift,
    joint_weight,
    joint_bias,
    output_weight,
    output_bias,
    second_gain,
    second_shift,
    expand_weight,
    expand_bias,
    reduce_weight,
    reduce_bias,
    bias_table,
    regions,
    live_slots,
    cotangent,
):
    ranks = lax.axis_size("dp")
    me = lax.axis_index("dp")
    count = images.shape[0]
    small = (
        first_gain,
        first_shift,
        joint_bias[0],
        joint_bias[1],
        output_bias,
        second_gain,
        second_shift,
        reduce_bias,
        expand_bias,
    )
    x = images.transpose(1, 2, 0, 3)
    cot = cotangent.transpose(1, 2, 0, 3).reshape(-1, C)
    live = jnp.broadcast_to(live_slots.astype(jnp.float32)[:, None], (count, 128))
    bias, mask, onehot = pair_tables(bias_table, regions)
    if ranks == RANKS:
        near, far = pack_shards(joint_weight, output_weight, expand_weight, reduce_weight, small)
        near, far = gather_all(near, far)
        row = near[:, 64, : 12 * 16].astype(jnp.float32)
        vectors = [row[:, 16 * i : 16 * i + 16].reshape(1, C) for i in range(8)]
        vectors.append(row[:, 128:].reshape(1, EXPAND))
    else:
        wide = lambda w: lax.all_gather(w, "dp", axis=0)
        rows = C // ranks
        near = jnp.concatenate(
            [wide(joint_weight[:, i * C : (i + 1) * C]) for i in range(3)] + [wide(output_weight)], axis=1
        )
        near = regroup(near, 4, rows)
        near = jnp.concatenate([near, jnp.zeros((RANKS, 16, C), near.dtype)], axis=1)
        far = jnp.concatenate([wide(expand_weight[:, i * C : (i + 1) * C]) for i in range(4)], axis=1)
        far = jnp.concatenate([regroup(far, 4, rows), wide(reduce_weight).reshape(RANKS, 64, C)], axis=1)
        vectors = [
            lax.all_gather(v, "dp", axis=0, tiled=True).astype(jnp.float32).reshape(1, -1) for v in small
        ]
    gain1, shift1, qbias, vbias, obias, gain2, shift2, rbias, ebias = vectors
    jbias = jnp.concatenate([qbias, jnp.zeros((1, C), jnp.float32), vbias], axis=1)
    joint, probs, mixed, res = attend(x, near, bias, mask, gain1, shift1, jbias, obias)
    out, rgrad, far_part, far_vec, ebias_grad = mlp_block(
        res.reshape(-1, C), cot, live, far, gain2, shift2, ebias, rbias
    )
    rgrad = rgrad.reshape(SIDE, SIDE, count, C)
    dx, near_part, near_vec, pairs = attend_back(x, near, joint, probs, mixed, rgrad, gain1, shift1)
    table = table_sums(pairs, onehot)
    small_sums = [near_vec[i] for i in (3, 4, 1, 2, 0)] + [far_vec[i] for i in (0, 1, 2)] + [ebias_grad[0]]
    if ranks == RANKS:
        flat = jnp.concatenate(small_sums + [table.reshape(-1)])
        sums = jnp.concatenate([flat, jnp.zeros((72 * 128 - flat.shape[0],), jnp.float32)]).reshape(72, 128)
        gfar, gnear, sums = reduce_all([far_part, near_part], sums, (4, 2), 1)
        sums = sums.reshape(-1)
        own = [lax.dynamic_slice(sums, (C * i + 16 * me,), (16,)) for i in range(8)]
        own.append(lax.dynamic_slice(sums, (C * 8 + 64 * me,), (64,)))
        table = sums[C * 12 : C * 12 + 169 * HEADS].reshape(169, HEADS)
        pick = lambda part, start, blocks: jnp.concatenate(
            [part[start + 16 * i : start + 16 * i + 16] for i in range(blocks)], axis=1
        )
        gj, go, ge, gr = pick(gnear, 0, 3), gnear[48:], pick(gfar, 0, 4), gfar[64:]
    else:
        rows = C // ranks
        scatter = lambda g: lax.psum_scatter(g.astype(jnp.float32), "dp", scatter_dimension=0, tiled=True)
        cut = lambda part, blocks: scatter(
            ungroup(part, blocks, ranks).transpose(0, 2, 1, 3).reshape(C, blocks * C)
        )
        gj, go = cut(near_part[:, :48], 3), cut(near_part[:, 48:], 1)
        ge, gr = cut(far_part[:, :64], 4), scatter(far_part[:, 64:].reshape(EXPAND, C))
        own = [scatter(g) for g in small_sums]
        table = lax.psum(table, "dp")
    image_order = lambda v: v.reshape(SIDE, SIDE, count, C).transpose(2, 0, 1, 3)
    return (
        image_order(out),
        image_order(dx),
        own[0],
        own[1],
        gj,
        jnp.stack([own[2], own[3]]),
        go,
        own[4],
        own[5],
        own[6],
        ge,
        own[8],
        gr,
        own[7],
        table,
    )


def solution(mesh):
    in_specs = (
        P("dp", None, None, None),
        P("dp"),
        P("dp"),
        P("dp", None),
        P(None, "dp"),
        P("dp", None),
        P("dp"),
        P("dp"),
        P("dp"),
        P("dp", None),
        P("dp"),
        P("dp", None),
        P("dp"),
        P(),
        P(),
        P("dp"),
        P("dp", None, None, None),
    )
    out_specs = (
        P("dp", None, None, None),
        P("dp", None, None, None),
        P("dp"),
        P("dp"),
        P("dp", None),
        P(None, "dp"),
        P("dp", None),
        P("dp"),
        P("dp"),
        P("dp"),
        P("dp", None),
        P("dp"),
        P("dp", None),
        P("dp"),
        P(),
    )
    return jax.shard_map(
        on_device, mesh=mesh, in_specs=in_specs, out_specs=out_specs, check_vma=False
    )
```

```python
import functools

import jax
import jax.numpy as jnp
from jax import lax
from jax.experimental import pallas as pl
from jax.experimental.pallas import tpu as pltpu
from jax.sharding import PartitionSpec as P

C = 512
HEADS = 16
HEAD_DIM = 32
EXPAND = 2048
WIN = 7
SIDE = 14
SHIFT = 3
PANES = 4
RANKS = 32

epsilon = 1e-05
exact_mode = lax.Precision.HIGHEST

MESH = pl.DeviceIdType.MESH
NEAR = 80
FAR = 128


def rank_of(z, y, x, c):
    return z * 8 + y * 4 + x * 2 + c


def flip(z, k):
    low, high = lax.rem(z, 2), z // 2
    if k % 2:
        low = 1 - low
    if k // 2:
        high = 1 - high
    return high * 2 + low


class Place:
    def __init__(self):
        self.me = lax.axis_index("dp")
        self.z, self.y = self.me // 8, lax.rem(self.me // 4, 2)
        self.x, self.c = lax.rem(self.me // 2, 2), lax.rem(self.me, 2)
        self.peer_x = rank_of(self.z, self.y, 1 - self.x, self.c)
        self.peer_y = rank_of(self.z, 1 - self.y, self.x, self.c)
        self.mate = rank_of(self.z, self.y, self.x, 1 - self.c)
        self.peers_z = [rank_of(flip(self.z, k), self.y, self.x, self.c) for k in (1, 2, 3)]

    def column(self, k, dy, dx):
        y = 1 - self.y if dy else self.y
        x = 1 - self.x if dx else self.x
        return rank_of(flip(self.z, k), y, x, self.c)

    def greet(self):
        barrier = pltpu.get_barrier_semaphore()
        peers = [self.mate, self.peer_x, self.peer_y] + self.peers_z
        for peer in peers:
            pl.semaphore_signal(barrier, inc=1, device_id=(peer,), device_id_type=MESH)
        pl.semaphore_wait(barrier, len(peers))


def remote(source, target, send, recv, rank):
    return pltpu.make_async_remote_copy(
        src_ref=source, dst_ref=target, send_sem=send, recv_sem=recv, device_id=(rank,), device_id_type=MESH
    )


class Gather:
    def __init__(self, place, own, full, send, recv):
        self.place, self.own, self.full, self.send, self.recv = place, own, full, send, recv

    def push(self, lane, owner, rank, source=None):
        source = self.full.at[owner] if source is None else source
        remote(source, self.full.at[owner], self.send.at[lane], self.recv.at[lane], rank).start()

    def some(self, lane):
        place = self.place
        return remote(
            self.own, self.full.at[place.me], self.send.at[lane], self.recv.at[lane], place.mate
        )

    def start(self):
        place = self.place
        for k in (1, 2, 3):
            self.push(k - 1, place.me, place.peers_z[k - 1], self.own)
        self.push(3, place.me, place.peer_x, self.own)
        self.push(7, place.me, place.peer_y, self.own)
        self.push(15, place.me, place.mate, self.own)

    def relay_columns(self):
        place = self.place
        for k in (1, 2, 3):
            self.some(k - 1).wait_recv()
            owner = place.column(k, 0, 0)
            self.push(3 + k, owner, place.peer_x)
            self.push(7 + k, owner, place.peer_y)
            self.push(15 + k, owner, place.mate)

    def relay_sides(self):
        place = self.place
        for k in range(4):
            self.some(3 + k).wait_recv()
            owner = place.column(k, 0, 1)
            if k % 2 == 0:
                self.push(11 + k, owner, place.peer_y)
            self.push(19 + k, owner, place.mate)
            self.some(7 + k).wait_recv()
            owner = place.column(k, 1, 0)
            if k % 2 == 1:
                self.push(11 + k, owner, place.peer_x)
            self.push(23 + k, owner, place.mate)

    def relay_corners(self):
        place = self.place
        for k in range(4):
            self.some(11 + k).wait_recv()
            self.push(27 + k, place.column(k, 1, 1), place.mate)

    def finish(self):
        for lane in range(15, 31):
            self.some(lane).wait_recv()

    def drain(self):
        for lane in range(31):
            self.some(lane).wait_send()


class Reduce:
    def __init__(self, place, parts, scratch):
        self.place, self.parts = place, parts
        self.acc, self.rc, self.r1x, self.r1y, self.r2x, self.r2y, self.rz = scratch[:7]
        self.local, self.send, self.recv = scratch[7:]

    @staticmethod
    def scratch(rows):
        shapes = [(4, 2, 2), (4, 2, 2), (2, 2), (2, 2), (2,), (2,), (3,)]
        return [pltpu.VMEM(s + (rows, C), jnp.bfloat16) for s in shapes] + [
            pltpu.SemaphoreType.DMA(()),
            pltpu.SemaphoreType.DMA((8,)),
            pltpu.SemaphoreType.DMA((8,)),
        ]

    def copies(self, lane):
        p, a = self.place, self.acc
        source, target, rank = {
            0: lambda: (self.parts.at[:, :, :, 1 - p.c], self.rc, p.mate),
            1: lambda: (a.at[0:2, :, 1 - p.x], self.r1x, p.peer_x),
            2: lambda: (a.at[2:4, 1 - p.y, :], self.r1y, p.peer_y),
            3: lambda: (a.at[0:2, 1 - p.y, p.x], self.r2y, p.peer_y),
            4: lambda: (a.at[2:4, p.y, 1 - p.x], self.r2x, p.peer_x),
            5: lambda: (a.at[flip(p.z, 1), p.y, p.x], self.rz.at[0], p.peers_z[0]),
            6: lambda: (a.at[flip(p.z, 2), p.y, p.x], self.rz.at[1], p.peers_z[1]),
            7: lambda: (a.at[flip(p.z, 3), p.y, p.x], self.rz.at[2], p.peers_z[2]),
        }[lane]()
        return remote(source, target, self.send.at[lane], self.recv.at[lane], rank)

    def mine(self):
        return pltpu.make_async_copy(self.parts.at[:, :, :, self.place.c], self.acc, self.local)

    def add(self, where, other):
        total = self.acc[where].astype(jnp.float32) + other.astype(jnp.float32)
        self.acc[where] = total.astype(jnp.bfloat16)

    def start(self):
        self.copies(0).start()
        self.mine().start()

    def cores(self):
        self.mine().wait()
        self.copies(0).wait_recv()

        def body(zz, carry):
            for yy in range(2):
                for xx in range(2):
                    self.add((zz, yy, xx), self.rc[zz, yy, xx])
            return carry

        lax.fori_loop(0, 4, body, 0)
        self.copies(1).start()
        self.copies(2).start()

    def sides(self):
        p = self.place
        self.copies(1).wait_recv()
        self.copies(2).wait_recv()
        for zz in range(2):
            for other in range(2):
                self.add((zz, other, p.x), self.r1x[zz, other])
                self.add((2 + zz, p.y, other), self.r1y[zz, other])
        self.copies(3).start()
        self.copies(4).start()

    def corners(self):
        p = self.place
        self.copies(3).wait_recv()
        self.copies(4).wait_recv()
        for zz in range(2):
            self.add((zz, p.y, p.x), self.r2y[zz])
            self.add((2 + zz, p.y, p.x), self.r2x[zz])
        for lane in (5, 6, 7):
            self.copies(lane).start()

    def finish(self):
        p = self.place
        total = self.acc[p.z, p.y, p.x].astype(jnp.float32)
        for lane in (5, 6, 7):
            self.copies(lane).wait_recv()
            total += self.rz[lane - 5].astype(jnp.float32)
        return total

    def drain(self):
        for lane in range(8):
            self.copies(lane).wait_send()


class Swap:
    def __init__(self, place, scratch):
        self.place = place
        self.own, self.got, self.send, self.recv = scratch

    @staticmethod
    def scratch(shape):
        return [
            pltpu.VMEM((4,) + shape, jnp.float32),
            pltpu.VMEM((6,) + shape, jnp.float32),
            pltpu.SemaphoreType.DMA((6,)),
            pltpu.SemaphoreType.DMA((6,)),
        ]

    def copies(self, lane):
        p = self.place
        rank = ([p.mate, p.peer_x, p.peer_y] + p.peers_z)[lane]
        return remote(
            self.own.at[min(lane, 3)], self.got.at[lane], self.send.at[lane], self.recv.at[lane], rank
        )

    def hop(self, lane):
        self.copies(lane).wait_recv()
        self.own[lane + 1] = self.own[lane] + self.got[lane]
        if lane < 2:
            self.copies(lane + 1).start()
        else:
            for last in (3, 4, 5):
                self.copies(last).start()

    def finish(self):
        for lane in (3, 4, 5):
            self.copies(lane).wait_recv()
        return (self.own[3] + self.got[3]) + (self.got[4] + self.got[5])

    def drain(self):
        for lane in range(6):
            self.copies(lane).wait_send()


def reduce_near_kernel(
    parts, near_vec, far_vec, table_ref,
    gj_ref, go_ref, table_out, jb_ref, eb_ref, *rest,
):
    owns = rest[:7]
    spread = rest[7]
    reduce_scratch, vec_scratch, table_scratch = rest[8:18], rest[18:22], rest[22:26]
    place = Place()
    place.greet()
    big = Reduce(place, parts, reduce_scratch)
    vec = Swap(place, vec_scratch)
    tab = Swap(place, table_scratch)
    big.start()
    vec.own[0, 0:8] = near_vec[...]
    vec.own[0, 8:16] = far_vec[...]
    tab.own[0] = table_ref[...]
    vec.copies(0).start()
    tab.copies(0).start()
    big.cores()
    vec.hop(0)
    tab.hop(0)
    big.sides()
    vec.hop(1)
    tab.hop(1)
    big.corners()
    vec.hop(2)
    tab.hop(2)
    total = big.finish()
    for b in range(3):
        gj_ref[:, b * C : (b + 1) * C] = total[b * 16 : (b + 1) * 16]
    go_ref[...] = total[48:64]
    sums = vec.finish()
    table_out[...] = tab.finish()
    for tile in range(4):
        spread[tile] = sums[:, tile * 128 : (tile + 1) * 128]
    me = place.me
    turn = lax.rem(128 - 16 * lax.rem(me, 8), 128)
    mine = pltpu.roll(spread[me // 8], turn, 1)[:, 0:16]
    jb_ref[...] = mine[1:3]
    for own, row in zip(owns, (0, 3, 4, 8, 9, 10)):
        own[...] = mine[row : row + 1]
    wide = pltpu.roll(spread[lax.rem(me, 8) // 2], 64 * lax.rem(me, 2), 1)[:, 0:64]
    owns[6][...] = wide[8:16]
    eb_ref[...] = owns[6][pl.ds(3 + me // 8, 1), :]
    big.drain()
    vec.drain()
    tab.drain()


def reduce_near(parts, near_vec, far_vec, table):
    one = jax.ShapeDtypeStruct((1, 16), jnp.float32)
    outs = pl.pallas_call(
        reduce_near_kernel,
        out_shape=[
            jax.ShapeDtypeStruct((16, 3 * C), jnp.float32),
            jax.ShapeDtypeStruct((16, C), jnp.float32),
            jax.ShapeDtypeStruct(table.shape, jnp.float32),
            jax.ShapeDtypeStruct((2, 16), jnp.float32),
            jax.ShapeDtypeStruct((1, 64), jnp.float32),
        ]
        + [one] * 6,
        in_specs=[pl.BlockSpec(memory_space=pl.ANY)] + [pl.BlockSpec(memory_space=pltpu.VMEM)] * 3,
        out_specs=[pl.BlockSpec(memory_space=pltpu.VMEM)] * 11,
        scratch_shapes=[pltpu.VMEM((8, 64), jnp.float32), pltpu.VMEM((4, 16, 128), jnp.float32)]
        + Reduce.scratch(64)
        + Swap.scratch((16, C))
        + Swap.scratch(table.shape),
        compiler_params=pltpu.CompilerParams(
            collective_id=2, has_side_effects=True, vmem_limit_bytes=40 << 20
        ),
        name="reduce_near",
    )(parts.reshape(4, 2, 2, 2, 64, C), near_vec, far_vec, table)
    return outs

ERFC_SLOPE = 0.4
ERFC_TERMS = (
    0.23192538182549352,
    0.16180412136440986,
    0.4683198256010739,
    -0.3709611648908394,
    0.7091781371622337,
    -0.20026632849062864,
)


def gelu_pair(v):
    bell = jnp.exp(v * v * -0.5)
    t = 1.0 / (1.0 + jnp.abs(v) * (ERFC_SLOPE * 0.5**0.5))
    tail = ERFC_TERMS[5] * 0.5
    for term in ERFC_TERMS[4::-1]:
        tail = tail * t + term * 0.5
    tail = tail * t * bell
    below = jnp.where(v < 0, tail, 1.0 - tail)
    return v * below, below + v * (bell * 0.3989422804014327)


def norm_parts(v):
    center = jnp.mean(v, axis=-1, keepdims=True)
    centred = v - center
    spread = jnp.mean(centred * centred, axis=-1, keepdims=True)
    rate = lax.rsqrt(spread + epsilon)
    return centred * rate, rate


def norm_pull(grad, gain, xhat, rate):
    scaled = grad * gain
    first = jnp.mean(scaled, axis=-1, keepdims=True)
    second = jnp.mean(scaled * xhat, axis=-1, keepdims=True)
    return rate * (scaled - first - xhat * second)


def dot_nn(a, b):
    return lax.dot_general(a, b, (((1,), (0,)), ((), ())), preferred_element_type=jnp.float32)


def dot_nt(a, b):
    return lax.dot_general(a, b, (((1,), (1,)), ((), ())), preferred_element_type=jnp.float32)


def dot_tn(a, b):
    return lax.dot_general(a, b, (((0,), (0,)), ((), ())), preferred_element_type=jnp.float32)


def column_sum(v):
    return jnp.sum(v, axis=0, keepdims=True)


def mlp_kernel(
    res_ref, cot_ref, live_ref, far_ref, bias_ref, ebias_ref,
    out_ref, rgrad_ref, part_ref, vec_ref, we_acc, wr_acc,
):
    step = pl.program_id(0)
    rows = res_ref.shape[0]

    @pl.when(step == 0)
    def _():
        we_acc[...] = jnp.zeros_like(we_acc)
        wr_acc[...] = jnp.zeros_like(wr_acc)
        vec_ref[...] = jnp.zeros_like(vec_ref)

    res = res_ref[...]
    gain = bias_ref[5:6]
    xhat, rate = norm_parts(res)
    second = (xhat * gain + bias_ref[6:7]).astype(jnp.bfloat16)
    upstream = (
        cot_ref[...].astype(jnp.float32).reshape(rows // 16, 16, C) * live_ref[...].astype(jnp.float32)[None]
    ).reshape(rows, C)
    low = upstream.astype(jnp.bfloat16)
    second_t = second.T
    low_t = low.T
    reduced = jnp.zeros((rows, C), jnp.float32)
    pulled = jnp.zeros((rows, C), jnp.float32)
    for b in range(4):
        we = far_ref[:, b * 16 : (b + 1) * 16, :].reshape(C, C)
        wr = far_ref[b * 8 : (b + 1) * 8, 64:128, :].reshape(C, C)
        hidden = dot_nn(second, we) + ebias_ref[:, b * C : (b + 1) * C]
        active, slope = gelu_pair(hidden)
        active = active.astype(jnp.bfloat16)
        reduced += dot_nn(active, wr)
        hgrad = (dot_nt(low, wr) * slope).astype(jnp.bfloat16)
        pulled += dot_nt(hgrad, we)
        wr_acc[b] += dot_nn(low_t, active)
        we_acc[b] += dot_nn(second_t, hgrad)
        vec_ref[3 + b : 4 + b] += column_sum(hgrad.astype(jnp.float32))
    out_ref[...] = (res + reduced + bias_ref[7:8]).astype(jnp.bfloat16)
    rgrad_ref[...] = upstream + norm_pull(pulled, gain, xhat, rate)
    vec_ref[0:1] += column_sum(pulled * xhat)
    vec_ref[1:2] += column_sum(pulled)
    vec_ref[2:3] += column_sum(low.astype(jnp.float32))

    @pl.when(step == pl.num_programs(0) - 1)
    def _():
        for b in range(4):
            part_ref[:, b * 16 : (b + 1) * 16, :] = we_acc[b].reshape(RANKS, 16, C).astype(jnp.bfloat16)
            part_ref[b * 8 : (b + 1) * 8, 64:128, :] = (
                wr_acc[b].T.reshape(8, 64, C).astype(jnp.bfloat16)
            )


def mlp_block(res, cot, live, far, vectors, ebias, rows=448):
    tokens = res.shape[0]
    moving = pl.BlockSpec((rows, C), lambda i: (i, 0))
    return pl.pallas_call(
        mlp_kernel,
        grid=(tokens // rows,),
        in_specs=[moving, moving, fixed((16, 1)), fixed((RANKS, FAR, C)), fixed((8, C)), fixed((1, EXPAND))],
        out_specs=[moving, moving, fixed((RANKS, FAR, C)), fixed((8, C))],
        out_shape=[
            jax.ShapeDtypeStruct((tokens, C), jnp.bfloat16),
            jax.ShapeDtypeStruct((tokens, C), jnp.float32),
            jax.ShapeDtypeStruct((RANKS, 128, C), jnp.bfloat16),
            jax.ShapeDtypeStruct((8, C), jnp.float32),
        ],
        scratch_shapes=[pltpu.VMEM((4, C, C), jnp.float32), pltpu.VMEM((4, C, C), jnp.float32)],
        compiler_params=pltpu.CompilerParams(vmem_limit_bytes=60 << 20, dimension_semantics=("arbitrary",)),
        name="mlp_block",
    )(res, cot, live, far, vectors, ebias)

SPOTS = WIN * WIN
ROWS = SPOTS * 16
QUERY_ROWS = 64
KEY_ROWS = 56
QUAD = 4 * HEAD_DIM
PAIR_SHAPE = (4 * KEY_ROWS, 2 * QUERY_ROWS)
SCALE = HEAD_DIM**-0.5


def spot_of(pane, spot):
    y = lax.rem((pane // 2) * WIN + spot // WIN + SHIFT, SIDE)
    x = lax.rem((pane % 2) * WIN + spot % WIN + SHIFT, SIDE)
    return y, x


def take_pane(pane, source, target):
    for spot in range(SPOTS):
        y, x = spot_of(pane, spot)
        target[spot * 16 : (spot + 1) * 16, :] = source[y, x]


def give_pane(pane, value, target):
    for spot in range(SPOTS):
        y, x = spot_of(pane, spot)
        target[y, x] = value[spot * 16 : (spot + 1) * 16, :]


def put_tiles(target, first, value):
    for tile in range(4):
        target[first + tile, 0:ROWS, :] = value[:, tile * QUAD : (tile + 1) * QUAD]


def get_tiles(source, first):
    return jnp.concatenate([source[first + tile, 0:ROWS, :] for tile in range(4)], axis=1)


def heads_mask(rows):
    return lax.rem(lax.broadcasted_iota(jnp.int32, (rows, 2 * QUAD), 1), QUAD) // HEAD_DIM


def load_pair(source, first, rows):
    return jnp.concatenate([source[first, rows, :], source[first + 1, rows, :]], axis=1)


def spread_heads(pair):
    lanes = heads_mask(KEY_ROWS)
    zero = jnp.zeros_like(pair)
    return jnp.concatenate([jnp.where(lanes == h, pair, zero) for h in range(4)], axis=0).astype(jnp.bfloat16)


def merge_heads(value):
    lanes = heads_mask(KEY_ROWS)
    parts = [value[h * KEY_ROWS : (h + 1) * KEY_ROWS] for h in range(4)]
    return jnp.where(
        lanes < 2, jnp.where(lanes == 0, parts[0], parts[1]), jnp.where(lanes == 2, parts[2], parts[3])
    )


def two_blocks(source, first, rows):
    upper = source[first, rows, :].astype(jnp.bfloat16)
    lower = source[first + 1, rows, :].astype(jnp.bfloat16)
    zero = jnp.zeros_like(upper)
    return jnp.concatenate(
        [jnp.concatenate([upper, zero], axis=1), jnp.concatenate([zero, lower], axis=1)], axis=0
    )


def over_keys(op, value):
    parts = value.reshape(4, KEY_ROWS, 2 * QUERY_ROWS)
    return jnp.broadcast_to(op(parts, axis=1, keepdims=True), parts.shape).reshape(value.shape)


def bias_rows(near, vec_ref, ebias_ref):
    rows = jnp.sum(near[:, 64:80, 0:256].astype(jnp.float32), axis=1)
    lane = lax.broadcasted_iota(jnp.int32, (RANKS, 256), 1)
    parts = [jnp.where(lane // 16 == i, rows, 0.0) for i in range(8)]
    parts = jnp.concatenate(parts, axis=0).astype(jnp.bfloat16)

    def taken(lhs, width):
        source = lax.broadcasted_iota(jnp.int32, (256, RANKS * width), 0)
        target = lax.broadcasted_iota(jnp.int32, (256, RANKS * width), 1)
        onehot = jnp.where(lax.rem(source, width) == lax.rem(target, width), 1.0, 0.0).astype(jnp.bfloat16)
        count = lhs.shape[0]
        shard = lax.rem(lax.broadcasted_iota(jnp.int32, (count, RANKS * width), 0), RANKS)
        place = lax.broadcasted_iota(jnp.int32, (count, RANKS * width), 1) // width
        return jnp.where(shard == place, dot_nn(lhs, onehot), 0.0)

    vec_ref[...] = jnp.sum(taken(parts, 16).reshape(8, RANKS, C), axis=1)
    tail = jnp.where(lane // 64 == 2, rows, 0.0).astype(jnp.bfloat16)
    ebias_ref[...] = jnp.sum(taken(tail, 64), axis=0, keepdims=True)


def attend_kernel(linked, *refs):
    x_ref, bias_ref, mask_ref, *refs = refs
    if linked:
        shards, refs = refs[:5], refs[5:]
    else:
        near_ref, *refs = refs
    joint_ref, probs_ref, mixed_ref, res_ref, vec_ref, ebias_ref, *refs = refs
    if linked:
        near_out, far_out, *refs = refs
    window, wide, blend, both, *refs = refs
    pane = pl.program_id(0)
    last = pl.num_programs(0) - 1
    if linked:
        near, far_own, local, near_send, near_recv, far_send, far_recv = refs
        place = Place()
        close = Gather(place, near.at[place.me], near, near_send, near_recv)
        distant = Gather(place, far_own, far_out, far_send, far_recv)
        joint_w, output_w, expand_w, reduce_w, row_w = shards
        own = near.at[place.me]
        pieces = [(joint_w.at[:, b * C : (b + 1) * C], own.at[b * 16 : (b + 1) * 16]) for b in range(3)]
        pieces += [(output_w, own.at[48:64]), (row_w, own.at[64:80])]
        pieces += [
            (expand_w.at[:, b * C : (b + 1) * C], far_own.at[b * 16 : (b + 1) * 16]) for b in range(4)
        ]
        pieces += [(reduce_w, far_own.at[64:128])]
        pieces = [pltpu.make_async_copy(a, b, local.at[i]) for i, (a, b) in enumerate(pieces)]
        keep_near = pltpu.make_async_copy(near, near_out, local.at[10])
        keep_far = pltpu.make_async_copy(far_own, far_out.at[place.me], local.at[11])
    else:
        near = near_ref

    @pl.when(pane == 0)
    def _():
        if linked:
            for piece in pieces:
                piece.start()
            place.greet()
            for piece in pieces[:5]:
                piece.wait()
            close.start()
            for piece in pieces[5:]:
                piece.wait()
        wide[...] = jnp.zeros_like(wide)
        if linked:
            close.relay_columns()
            close.relay_sides()
            close.relay_corners()
            distant.start()
            keep_far.start()
            close.finish()
            keep_near.start()
        bias_rows(near, vec_ref, ebias_ref)

    if linked:
        @pl.when(pane == 1)
        def _():
            distant.relay_columns()

        @pl.when(pane == 2)
        def _():
            distant.relay_sides()

        @pl.when(pane == 3)
        def _():
            distant.relay_corners()

    take_pane(pane, x_ref, window)
    source = window[...].astype(jnp.float32)
    xhat, _ = norm_parts(source)
    normed = (xhat * vec_ref[0:1] + vec_ref[1:2]).astype(jnp.bfloat16)
    for b in range(3):
        weight = near[:, b * 16 : (b + 1) * 16, :].reshape(C, C)
        block = dot_nn(normed, weight)
        if b != 1:
            block += vec_ref[2 + b // 2 : 3 + b // 2]
        block = block.astype(jnp.bfloat16)
        joint_ref[0, :, b * C : (b + 1) * C] = block
        put_tiles(wide, b * 4, block.astype(jnp.float32))
    for pair in range(2):
        both[pair] = bias_ref[pair] + mask_ref[0]

    def per_image(m, carry):
        few, many = pl.ds(m, QUERY_ROWS, stride=16), pl.ds(m, KEY_ROWS, stride=16)
        for pair in range(2):
            q = two_blocks(wide, 2 * pair, few)
            k = spread_heads(load_pair(wide, 4 + 2 * pair, many))
            v = spread_heads(load_pair(wide, 8 + 2 * pair, many))
            scores = dot_nt(k, q) * SCALE + both[pair]
            powers = jnp.exp(scores - over_keys(jnp.max, scores))
            probs = (powers * (1.0 / over_keys(jnp.sum, powers))).astype(jnp.bfloat16)
            probs_ref[0, m, pair] = probs
            blended = dot_tn(probs, v)
            blend[2 * pair, many, :] = blended[0:KEY_ROWS, 0:QUAD]
            blend[2 * pair + 1, many, :] = blended[QUERY_ROWS : QUERY_ROWS + KEY_ROWS, QUAD:]
        return carry

    lax.fori_loop(0, 16, per_image, 0, unroll=2)
    mixed = get_tiles(blend, 0).astype(jnp.bfloat16)
    mixed_ref[0] = mixed
    projected = dot_nn(mixed, near[:, 48:64, :].reshape(C, C)) + vec_ref[4:5]
    give_pane(pane, window[...].astype(jnp.float32) + projected, res_ref)

    if linked:
        @pl.when(pane == last)
        def _():
            distant.finish()
            close.drain()
            distant.drain()
            keep_near.wait()
            keep_far.wait()


def fixed(shape):
    return pl.BlockSpec(shape, lambda i: (0,) * len(shape), pipeline_mode=pl.Buffered(1))


def stepped(shape):
    return pl.BlockSpec((1,) + shape, lambda i: (i,) + (0,) * len(shape))


def attend(x, bias, mask, weights, linked):
    anywhere = pl.BlockSpec(memory_space=pl.ANY)
    out_specs = [stepped((ROWS, 3 * C)), stepped((16, 2) + PAIR_SHAPE), stepped((ROWS, C)),
                 fixed((SIDE, SIDE, 16, C)), fixed((8, C)), fixed((1, EXPAND))]
    out_shape = [
        jax.ShapeDtypeStruct((PANES, ROWS, 3 * C), jnp.bfloat16),
        jax.ShapeDtypeStruct((PANES, 16, 2) + PAIR_SHAPE, jnp.bfloat16),
        jax.ShapeDtypeStruct((PANES, ROWS, C), jnp.bfloat16),
        jax.ShapeDtypeStruct((SIDE, SIDE, 16, C), jnp.float32),
        jax.ShapeDtypeStruct((8, C), jnp.float32),
        jax.ShapeDtypeStruct((1, EXPAND), jnp.float32),
    ]
    scratch = [
        pltpu.VMEM((ROWS, C), jnp.bfloat16),
        pltpu.VMEM((12, QUERY_ROWS * 16, QUAD), jnp.float32),
        pltpu.VMEM((4, QUERY_ROWS * 16, QUAD), jnp.float32),
        pltpu.VMEM((2,) + PAIR_SHAPE, jnp.float32),
    ]
    in_specs = [fixed((SIDE, SIDE, 16, C)), fixed((2,) + PAIR_SHAPE), stepped(PAIR_SHAPE)]
    if linked:
        in_specs += [anywhere] * 5
        out_specs += [anywhere] * 2
        out_shape += [
            jax.ShapeDtypeStruct((RANKS, NEAR, C), jnp.bfloat16),
            jax.ShapeDtypeStruct((RANKS, FAR, C), jnp.bfloat16),
        ]
        scratch += [
            pltpu.VMEM((RANKS, NEAR, C), jnp.bfloat16),
            pltpu.VMEM((FAR, C), jnp.bfloat16),
            pltpu.SemaphoreType.DMA((12,)),
        ] + [pltpu.SemaphoreType.DMA((31,))] * 4
        extra = dict(collective_id=0, has_side_effects=True)
    else:
        in_specs += [fixed((RANKS, NEAR, C))]
        extra = {}
    return pl.pallas_call(
        functools.partial(attend_kernel, linked),
        grid=(PANES,),
        in_specs=in_specs,
        out_specs=out_specs,
        out_shape=out_shape,
        scratch_shapes=scratch,
        compiler_params=pltpu.CompilerParams(
            vmem_limit_bytes=62 << 20, dimension_semantics=("arbitrary",), **extra
        ),
        name="attend",
    )(x, bias, mask, *weights)


def attend_back_kernel(linked, *refs):
    x_ref, near_ref, joint_ref, probs_ref, mixed_ref, rgrad_ref, bias_ref, *refs = refs
    if linked:
        far_parts, *refs = refs
    dx_ref, part_ref, vec_ref, pairs_ref, *refs = refs
    if linked:
        ge_ref, gr_ref, *refs = refs
    window, rwindow, wide, blend, turned, wj_acc, wo_acc, *refs = refs
    pane = pl.program_id(0)
    if linked:
        place = Place()
        distant = Reduce(place, far_parts, refs)

    @pl.when(pane == 0)
    def _():
        if linked:
            place.greet()
            distant.start()
        wide[...] = jnp.zeros_like(wide)
        blend[...] = jnp.zeros_like(blend)
        wj_acc[...] = jnp.zeros_like(wj_acc)
        wo_acc[...] = jnp.zeros_like(wo_acc)
        vec_ref[...] = jnp.zeros_like(vec_ref)
        pairs_ref[...] = jnp.zeros_like(pairs_ref)

    if linked:
        @pl.when(pane == 1)
        def _():
            distant.cores()

        @pl.when(pane == 2)
        def _():
            distant.sides()

        @pl.when(pane == 3)
        def _():
            distant.corners()

    take_pane(pane, x_ref, window)
    take_pane(pane, rgrad_ref, rwindow)
    pulled = rwindow[...].astype(jnp.bfloat16)
    wo = near_ref[:, 48:64, :].reshape(C, C)
    wo_acc[...] += dot_tn(mixed_ref[0], pulled)
    vec_ref[0:1] += column_sum(pulled.astype(jnp.float32))
    put_tiles(blend, 0, dot_nt(pulled, wo).astype(jnp.bfloat16).astype(jnp.float32))
    for b in range(3):
        put_tiles(wide, b * 4, joint_ref[0, :, b * C : (b + 1) * C].astype(jnp.float32))

    def per_image(m, carry):
        few, many = pl.ds(m, QUERY_ROWS, stride=16), pl.ds(m, KEY_ROWS, stride=16)
        for pair in range(2):
            q = two_blocks(wide, 2 * pair, few)
            k = spread_heads(load_pair(wide, 4 + 2 * pair, many))
            v = spread_heads(load_pair(wide, 8 + 2 * pair, many))
            pull = two_blocks(blend, 2 * pair, few)
            probs = probs_ref[0, m, pair]
            wider = probs.astype(jnp.float32)
            weighted = dot_nt(v, pull) * wider
            sgrad = (weighted - wider * over_keys(jnp.sum, weighted)).astype(jnp.bfloat16)
            pairs_ref[pair] += sgrad.astype(jnp.float32)
            qgrad = dot_tn(sgrad, k) * SCALE
            turned[2 * pair, many, :] = qgrad[0:KEY_ROWS, 0:QUAD]
            turned[2 * pair + 1, many, :] = qgrad[QUERY_ROWS : QUERY_ROWS + KEY_ROWS, QUAD:]
            kgrad = merge_heads(dot_nn(sgrad, q)) * SCALE
            turned[4 + 2 * pair, many, :] = kgrad[:, 0:QUAD]
            turned[5 + 2 * pair, many, :] = kgrad[:, QUAD:]
            vgrad = merge_heads(dot_nn(probs, pull))
            turned[8 + 2 * pair, many, :] = vgrad[:, 0:QUAD]
            turned[9 + 2 * pair, many, :] = vgrad[:, QUAD:]
        return carry

    lax.fori_loop(0, 16, per_image, 0, unroll=2)
    gain = bias_ref[0:1]
    xhat, rate = norm_parts(window[...].astype(jnp.float32))
    normed = (xhat * gain + bias_ref[1:2]).astype(jnp.bfloat16)
    normed_t = normed.T
    total = jnp.zeros((ROWS, C), jnp.float32)
    for b in range(3):
        weight = near_ref[:, b * 16 : (b + 1) * 16, :].reshape(C, C)
        block = get_tiles(turned, b * 4).astype(jnp.bfloat16)
        wj_acc[b] += dot_nn(normed_t, block)
        total += dot_nt(block, weight)
        if b != 1:
            vec_ref[1 + b // 2 : 2 + b // 2] += column_sum(block.astype(jnp.float32))
    vec_ref[3:4] += column_sum(total * xhat)
    vec_ref[4:5] += column_sum(total)
    dx = rwindow[...] + norm_pull(total, gain, xhat, rate)
    give_pane(pane, dx.astype(jnp.bfloat16), dx_ref)

    @pl.when(pane == PANES - 1)
    def _():
        for b in range(3):
            part_ref[:, b * 16 : (b + 1) * 16, :] = wj_acc[b].reshape(RANKS, 16, C).astype(jnp.bfloat16)
        part_ref[:, 48:64, :] = wo_acc[...].reshape(RANKS, 16, C).astype(jnp.bfloat16)
        if linked:
            total = distant.finish()
            for b in range(4):
                ge_ref[:, b * C : (b + 1) * C] = total[b * 16 : (b + 1) * 16]
            gr_ref[...] = total[64:128]
            distant.drain()


def attend_back(x, near, joint, probs, mixed, rgrad, vectors, far_parts, linked):
    in_specs = [fixed((SIDE, SIDE, 16, C)), fixed((RANKS, NEAR, C)), stepped((ROWS, 3 * C)),
                stepped((16, 2) + PAIR_SHAPE), stepped((ROWS, C)), fixed((SIDE, SIDE, 16, C)), fixed((8, C))]
    out_specs = [fixed((SIDE, SIDE, 16, C)), fixed((RANKS, 64, C)), fixed((8, C)), fixed((2,) + PAIR_SHAPE)]
    out_shape = [
        jax.ShapeDtypeStruct((SIDE, SIDE, 16, C), jnp.bfloat16),
        jax.ShapeDtypeStruct((RANKS, 64, C), jnp.bfloat16),
        jax.ShapeDtypeStruct((8, C), jnp.float32),
        jax.ShapeDtypeStruct((2,) + PAIR_SHAPE, jnp.float32),
    ]
    scratch = [
        pltpu.VMEM((ROWS, C), jnp.bfloat16),
        pltpu.VMEM((ROWS, C), jnp.float32),
        pltpu.VMEM((12, QUERY_ROWS * 16, QUAD), jnp.float32),
        pltpu.VMEM((4, QUERY_ROWS * 16, QUAD), jnp.float32),
        pltpu.VMEM((12, QUERY_ROWS * 16, QUAD), jnp.float32),
        pltpu.VMEM((3, C, C), jnp.float32),
        pltpu.VMEM((C, C), jnp.float32),
    ]
    operands = [x, near, joint, probs, mixed, rgrad, vectors]
    extra = {}
    if linked:
        in_specs.append(pl.BlockSpec(memory_space=pl.ANY))
        out_specs += [fixed((16, EXPAND)), fixed((64, C))]
        out_shape += [
            jax.ShapeDtypeStruct((16, EXPAND), jnp.float32),
            jax.ShapeDtypeStruct((64, C), jnp.float32),
        ]
        scratch += Reduce.scratch(FAR)
        operands.append(far_parts.reshape(4, 2, 2, 2, FAR, C))
        extra = dict(collective_id=1, has_side_effects=True)
    return pl.pallas_call(
        functools.partial(attend_back_kernel, linked),
        grid=(PANES,),
        in_specs=in_specs,
        out_specs=out_specs,
        out_shape=out_shape,
        scratch_shapes=scratch,
        compiler_params=pltpu.CompilerParams(
            vmem_limit_bytes=(1 << 26) - (64 << 10), dimension_semantics=("arbitrary",), **extra
        ),
        name="attend_back",
    )(*operands)


def pair_tables(bias_table, regions):
    keys, queries = jnp.arange(KEY_ROWS), jnp.arange(QUERY_ROWS)
    real = (keys < SPOTS)[:, None] & (queries < SPOTS)[None, :]
    cells = (
        (queries[None, :] // WIN - keys[:, None] // WIN + WIN - 1) * (2 * WIN - 1)
        + queries[None, :] % WIN - keys[:, None] % WIN + WIN - 1
    )
    cells = jnp.where(real, cells, -1).reshape(-1)
    onehot = (cells[None, :] == jnp.arange((2 * WIN - 1) ** 2)[:, None]).astype(jnp.bfloat16)
    bias = dot_tn(bias_table, onehot).reshape(2, 2, 4, KEY_ROWS, QUERY_ROWS)
    bias = jnp.where((keys < SPOTS)[:, None], bias, -1e30)
    bias = bias.transpose(0, 2, 3, 1, 4).reshape((2,) + PAIR_SHAPE)
    labels = jnp.roll(regions, (-SHIFT, -SHIFT), axis=(0, 1)).reshape(2, WIN, 2, WIN)
    labels = labels.transpose(0, 2, 1, 3).reshape(PANES, SPOTS)
    along = jnp.tile(jnp.pad(labels, ((0, 0), (0, KEY_ROWS - SPOTS))), (1, 4))
    across = jnp.tile(jnp.pad(labels, ((0, 0), (0, QUERY_ROWS - SPOTS))), (1, 2))
    mask = jnp.where(along[:, :, None] == across[:, None, :], 0.0, -100.0).astype(jnp.float32)
    return bias, mask, onehot


def table_sums(pairs, onehot):
    heads = pairs.reshape(2, 4, KEY_ROWS, 2, QUERY_ROWS).transpose(0, 3, 1, 2, 4)
    return lax.dot_general(
        heads.reshape(HEADS, KEY_ROWS * QUERY_ROWS), onehot.astype(jnp.float32), (((1,), (1,)), ((), ())),
        precision=exact_mode, preferred_element_type=jnp.float32,
    )

def regroup(packed, blocks, rows):
    count = packed.shape[0] // RANKS
    return (
        packed.reshape(RANKS, count, blocks, rows, C)
        .transpose(0, 2, 1, 3, 4)
        .reshape(RANKS, blocks * rows * count, C)
    )


def ungroup(parts, blocks, ranks):
    rows = parts.shape[1] // blocks
    flat = parts.reshape(RANKS, blocks, rows, C).transpose(1, 0, 2, 3).reshape(blocks, RANKS * rows, C)
    return flat.reshape(blocks, ranks, RANKS * rows // ranks, C).transpose(1, 0, 2, 3)


def on_device(
    images,
    first_gain,
    first_shift,
    joint_weight,
    joint_bias,
    output_weight,
    output_bias,
    second_gain,
    second_shift,
    expand_weight,
    expand_bias,
    reduce_weight,
    reduce_bias,
    bias_table,
    regions,
    live_slots,
    cotangent,
):
    ranks = lax.axis_size("dp")
    count = images.shape[0]
    linked = ranks == RANKS
    small = (
        first_gain,
        first_shift,
        joint_bias[0],
        joint_bias[1],
        output_bias,
        second_gain,
        second_shift,
        reduce_bias,
        expand_bias,
    )
    x = images.transpose(1, 2, 0, 3)
    cot = cotangent.transpose(1, 2, 0, 3).reshape(-1, C)
    bias, mask, onehot = pair_tables(bias_table, regions)
    if linked:
        start, row = 0, jnp.zeros((C,), jnp.float32)
        for vector in small:
            size = vector.shape[0]
            row += jnp.pad(vector.astype(jnp.float32), (start, C - start - size))
            start += size
        row = jnp.pad(row.astype(jnp.bfloat16)[None], ((0, 15), (0, 0)))
        weights = (joint_weight, output_weight, expand_weight, reduce_weight, row)
        joint, probs, mixed, res, vectors, ebias, near, far = attend(x, bias, mask, weights, True)
    else:
        rows = C // ranks
        wide = lambda w: lax.all_gather(w, "dp", axis=0)
        near = jnp.concatenate(
            [wide(joint_weight[:, i * C : (i + 1) * C]) for i in range(3)] + [wide(output_weight)], axis=1
        )
        row = jnp.concatenate(
            [lax.all_gather(v, "dp", axis=0, tiled=True).reshape(RANKS, -1) for v in small], axis=1
        )
        row = jnp.pad(row[:, None], ((0, 0), (0, 15), (0, C - row.shape[1])))
        near = jnp.concatenate([regroup(near, 4, rows), row], axis=1)
        far = jnp.concatenate([wide(expand_weight[:, i * C : (i + 1) * C]) for i in range(4)], axis=1)
        far = jnp.concatenate([regroup(far, 4, rows), wide(reduce_weight).reshape(RANKS, 64, C)], axis=1)
        joint, probs, mixed, res, vectors, ebias = attend(x, bias, mask, (near,), False)
    out, rgrad, far_part, far_vec = mlp_block(
        res.reshape(-1, C), cot, live_slots[:, None], far, vectors, ebias
    )
    rgrad = rgrad.reshape(SIDE, SIDE, count, C)
    dx, near_part, near_vec, pairs, *far_grads = attend_back(
        x, near, joint, probs, mixed, rgrad, vectors, far_part, linked
    )
    table = table_sums(pairs, onehot)
    if linked:
        ge, gr = far_grads
        gj, go, table, jb, eb, *own = reduce_near(near_part, near_vec, far_vec, table)
        own = [v.reshape(-1) for v in own]
        ob, gain1, shift1, gain2, shift2, rb = own
        eb = eb.reshape(-1)
    else:
        scatter = lambda g: lax.psum_scatter(g.astype(jnp.float32), "dp", scatter_dimension=0, tiled=True)
        cut = lambda part, blocks: scatter(
            ungroup(part, blocks, ranks).transpose(0, 2, 1, 3).reshape(C, blocks * C)
        )
        gj, go = cut(near_part[:, :48], 3), cut(near_part[:, 48:], 1)
        ge, gr = cut(far_part[:, :64], 4), scatter(far_part[:, 64:].reshape(EXPAND, C))
        ob, qb, vb, gain1, shift1 = [scatter(near_vec[i]) for i in range(5)]
        gain2, shift2, rb = [scatter(far_vec[i]) for i in range(3)]
        eb, jb = scatter(far_vec[3:7].reshape(-1)), jnp.stack([qb, vb])
        table = lax.psum(table, "dp")
    image_order = lambda v: v.reshape(SIDE, SIDE, count, C).transpose(2, 0, 1, 3)
    return (
        image_order(out),
        image_order(dx),
        gain1,
        shift1,
        gj,
        jb,
        go,
        ob,
        gain2,
        shift2,
        ge,
        eb,
        gr,
        rb,
        table.T,
    )


def solution(mesh):
    in_specs = (
        P("dp", None, None, None),
        P("dp"),
        P("dp"),
        P("dp", None),
        P(None, "dp"),
        P("dp", None),
        P("dp"),
        P("dp"),
        P("dp"),
        P("dp", None),
        P("dp"),
        P("dp", None),
        P("dp"),
        P(),
        P(),
        P("dp"),
        P("dp", None, None, None),
    )
    out_specs = (
        P("dp", None, None, None),
        P("dp", None, None, None),
        P("dp"),
        P("dp"),
        P("dp", None),
        P(None, "dp"),
        P("dp", None),
        P("dp"),
        P("dp"),
        P("dp"),
        P("dp", None),
        P("dp"),
        P("dp", None),
        P("dp"),
        P(),
    )
    return jax.shard_map(
        on_device, mesh=mesh, in_specs=in_specs, out_specs=out_specs, check_vma=False
    )
```

```python
import functools

import jax
import jax.numpy as jnp
from jax import lax
from jax.experimental import pallas as pl
from jax.experimental.pallas import tpu as pltpu
from jax.sharding import PartitionSpec as P

C = 512
HEADS = 16
HEAD_DIM = 32
EXPAND = 2048
WIN = 7
SIDE = 14
SHIFT = 3
PANES = 4
RANKS = 32

epsilon = 1e-05
exact_mode = lax.Precision.HIGHEST

MESH = pl.DeviceIdType.MESH
NEAR = 48
FAR = 128


def rank_of(z, y, x, c):
    return z * 8 + y * 4 + x * 2 + c


def flip(z, k):
    low, high = lax.rem(z, 2), z // 2
    if k % 2:
        low = 1 - low
    if k // 2:
        high = 1 - high
    return high * 2 + low


class Place:
    def __init__(self):
        self.me = lax.axis_index("dp")
        self.z, self.y = self.me // 8, lax.rem(self.me // 4, 2)
        self.x, self.c = lax.rem(self.me // 2, 2), lax.rem(self.me, 2)
        self.peer_x = rank_of(self.z, self.y, 1 - self.x, self.c)
        self.peer_y = rank_of(self.z, 1 - self.y, self.x, self.c)
        self.mate = rank_of(self.z, self.y, self.x, 1 - self.c)
        self.peers_z = [rank_of(flip(self.z, k), self.y, self.x, self.c) for k in (1, 2, 3)]

    def column(self, k, dy, dx):
        y = 1 - self.y if dy else self.y
        x = 1 - self.x if dx else self.x
        return rank_of(flip(self.z, k), y, x, self.c)

    def greet(self):
        barrier = pltpu.get_barrier_semaphore()
        peers = [self.mate, self.peer_x, self.peer_y] + self.peers_z
        for peer in peers:
            pl.semaphore_signal(barrier, inc=1, device_id=(peer,), device_id_type=MESH)
        pl.semaphore_wait(barrier, len(peers))


def remote(source, target, send, recv, rank):
    return pltpu.make_async_remote_copy(
        src_ref=source, dst_ref=target, send_sem=send, recv_sem=recv, device_id=(rank,), device_id_type=MESH
    )


class Gather:
    def __init__(self, place, own, full, send, recv):
        self.place, self.own, self.full, self.send, self.recv = place, own, full, send, recv

    def push(self, lane, owner, rank, source=None):
        source = self.full.at[owner] if source is None else source
        remote(source, self.full.at[owner], self.send.at[lane], self.recv.at[lane], rank).start()

    def some(self, lane):
        place = self.place
        return remote(
            self.own, self.full.at[place.me], self.send.at[lane], self.recv.at[lane], place.mate
        )

    def start(self):
        place = self.place
        for k in (1, 2, 3):
            self.push(k - 1, place.me, place.peers_z[k - 1], self.own)
        self.push(3, place.me, place.peer_x, self.own)
        self.push(7, place.me, place.peer_y, self.own)
        self.push(15, place.me, place.mate, self.own)

    def relay_columns(self):
        place = self.place
        for k in (1, 2, 3):
            self.some(k - 1).wait_recv()
            owner = place.column(k, 0, 0)
            self.push(3 + k, owner, place.peer_x)
            self.push(7 + k, owner, place.peer_y)
            self.push(15 + k, owner, place.mate)

    def relay_sides(self):
        place = self.place
        for k in range(4):
            self.some(3 + k).wait_recv()
            owner = place.column(k, 0, 1)
            if k % 2 == 0:
                self.push(11 + k, owner, place.peer_y)
            self.push(19 + k, owner, place.mate)
            self.some(7 + k).wait_recv()
            owner = place.column(k, 1, 0)
            if k % 2 == 1:
                self.push(11 + k, owner, place.peer_x)
            self.push(23 + k, owner, place.mate)

    def relay_corners(self):
        place = self.place
        for k in range(4):
            self.some(11 + k).wait_recv()
            self.push(27 + k, place.column(k, 1, 1), place.mate)

    def finish(self):
        for lane in range(15, 31):
            self.some(lane).wait_recv()

    def drain(self):
        for lane in range(31):
            self.some(lane).wait_send()


class Reduce:
    def __init__(self, place, parts, scratch, start=0):
        self.place = place
        self.acc = scratch[0]
        self.cut = pl.ds(start, self.acc.shape[3])
        self.parts = parts
        self.acc, self.rc, self.r1x, self.r1y, self.r2x, self.r2y, self.rz = scratch[:7]
        self.local, self.send, self.recv = scratch[7:]

    @staticmethod
    def scratch(rows):
        shapes = [(4, 2, 2), (4, 2, 2), (2, 2), (2, 2), (2,), (2,), (3,)]
        return [pltpu.VMEM(s + (rows, C), jnp.bfloat16) for s in shapes] + [
            pltpu.SemaphoreType.DMA(()),
            pltpu.SemaphoreType.DMA((8,)),
            pltpu.SemaphoreType.DMA((8,)),
        ]

    def copies(self, lane):
        p, a = self.place, self.acc
        source, target, rank = {
            0: lambda: (self.parts.at[:, :, :, 1 - p.c, self.cut], self.rc, p.mate),
            1: lambda: (a.at[0:2, :, 1 - p.x], self.r1x, p.peer_x),
            2: lambda: (a.at[2:4, 1 - p.y, :], self.r1y, p.peer_y),
            3: lambda: (a.at[0:2, 1 - p.y, p.x], self.r2y, p.peer_y),
            4: lambda: (a.at[2:4, p.y, 1 - p.x], self.r2x, p.peer_x),
            5: lambda: (a.at[flip(p.z, 1), p.y, p.x], self.rz.at[0], p.peers_z[0]),
            6: lambda: (a.at[flip(p.z, 2), p.y, p.x], self.rz.at[1], p.peers_z[1]),
            7: lambda: (a.at[flip(p.z, 3), p.y, p.x], self.rz.at[2], p.peers_z[2]),
        }[lane]()
        return remote(source, target, self.send.at[lane], self.recv.at[lane], rank)

    def mine(self):
        return pltpu.make_async_copy(self.parts.at[:, :, :, self.place.c, self.cut], self.acc, self.local)

    def add(self, where, other):
        total = self.acc[where].astype(jnp.float32) + other.astype(jnp.float32)
        self.acc[where] = total.astype(jnp.bfloat16)

    def start(self):
        self.copies(0).start()
        self.mine().start()

    def cores(self):
        self.mine().wait()
        self.copies(0).wait_recv()

        def body(zz, carry):
            for yy in range(2):
                for xx in range(2):
                    self.add((zz, yy, xx), self.rc[zz, yy, xx])
            return carry

        lax.fori_loop(0, 4, body, 0)
        self.copies(1).start()
        self.copies(2).start()

    def sides(self):
        p = self.place
        self.copies(1).wait_recv()
        self.copies(2).wait_recv()
        for zz in range(2):
            for other in range(2):
                self.add((zz, other, p.x), self.r1x[zz, other])
                self.add((2 + zz, p.y, other), self.r1y[zz, other])
        self.copies(3).start()
        self.copies(4).start()

    def corners(self):
        p = self.place
        self.copies(3).wait_recv()
        self.copies(4).wait_recv()
        for zz in range(2):
            self.add((zz, p.y, p.x), self.r2y[zz])
            self.add((2 + zz, p.y, p.x), self.r2x[zz])
        for lane in (5, 6, 7):
            self.copies(lane).start()

    def finish(self):
        p = self.place
        total = self.acc[p.z, p.y, p.x].astype(jnp.float32)
        for lane in (5, 6, 7):
            self.copies(lane).wait_recv()
            total += self.rz[lane - 5].astype(jnp.float32)
        return total

    def drain(self):
        for lane in range(8):
            self.copies(lane).wait_send()


class Swap:
    def __init__(self, place, scratch):
        self.place = place
        self.own, self.got, self.send, self.recv = scratch

    @staticmethod
    def scratch(shape):
        return [
            pltpu.VMEM((4,) + shape, jnp.float32),
            pltpu.VMEM((6,) + shape, jnp.float32),
            pltpu.SemaphoreType.DMA((6,)),
            pltpu.SemaphoreType.DMA((6,)),
        ]

    def copies(self, lane):
        p = self.place
        rank = ([p.mate, p.peer_x, p.peer_y] + p.peers_z)[lane]
        return remote(
            self.own.at[min(lane, 3)], self.got.at[lane], self.send.at[lane], self.recv.at[lane], rank
        )

    def hop(self, lane):
        self.copies(lane).wait_recv()
        self.own[lane + 1] = self.own[lane] + self.got[lane]
        if lane < 2:
            self.copies(lane + 1).start()
        else:
            for last in (3, 4, 5):
                self.copies(last).start()

    def finish(self):
        for lane in (3, 4, 5):
            self.copies(lane).wait_recv()
        return (self.own[3] + self.got[3]) + (self.got[4] + self.got[5])

    def drain(self):
        for lane in range(6):
            self.copies(lane).wait_send()


HALVES = 2
HALF = 64 // HALVES


def reduce_near_kernel(
    parts, near_vec, far_vec, table_ref,
    gj_ref, go_ref, table_out, jb_ref, eb_ref, *rest,
):
    owns, rest = rest[:6], rest[6:]
    bias_scratch, spread, rest = rest[0], rest[1], rest[2:]
    bigs, rest = [rest[i * 10 : i * 10 + 10] for i in range(HALVES)], rest[10 * HALVES :]
    place = Place()
    place.greet()
    bigs = [Reduce(place, parts, scratch, i * HALF) for i, scratch in enumerate(bigs)]
    vec = Swap(place, rest[0:4])
    tab = Swap(place, rest[4:8])
    for big in bigs:
        big.start()
    vec.own[0, 0:8] = near_vec[...]
    vec.own[0, 8:16] = far_vec[...]
    tab.own[0] = table_ref[...]
    vec.copies(0).start()
    tab.copies(0).start()
    for big in bigs:
        big.cores()
    vec.hop(0)
    tab.hop(0)
    for big in bigs:
        big.sides()
    vec.hop(1)
    tab.hop(1)
    for big in bigs:
        big.corners()
    vec.hop(2)
    tab.hop(2)
    for i, big in enumerate(bigs):
        total = big.finish()
        for block in range(HALF // 16):
            b = i * (HALF // 16) + block
            rows = total[block * 16 : (block + 1) * 16]
            if b < 3:
                gj_ref[:, b * C : (b + 1) * C] = rows
            else:
                go_ref[...] = rows
    sums = vec.finish()
    table_out[...] = tab.finish()
    for tile in range(4):
        spread[tile] = sums[:, tile * 128 : (tile + 1) * 128]
    me = place.me
    turn = lax.rem(128 - 16 * lax.rem(me, 8), 128)
    mine = pltpu.roll(spread[me // 8], turn, 1)[:, 0:16]
    jb_ref[...] = mine[1:3]
    for own, row in zip(owns, (0, 3, 4, 8, 9, 10)):
        own[...] = mine[row : row + 1]
    wide = pltpu.roll(spread[lax.rem(me, 8) // 2], 64 * lax.rem(me, 2), 1)[:, 0:64]
    bias_scratch[...] = wide[8:16]
    eb_ref[...] = bias_scratch[pl.ds(3 + me // 8, 1), :]
    for big in bigs:
        big.drain()
    vec.drain()
    tab.drain()


def reduce_near(parts, near_vec, far_vec, table):
    one = jax.ShapeDtypeStruct((1, 16), jnp.float32)
    scratch = [pltpu.VMEM((8, 64), jnp.float32), pltpu.VMEM((4, 16, 128), jnp.float32)]
    for _ in range(HALVES):
        scratch += Reduce.scratch(HALF)
    return pl.pallas_call(
        reduce_near_kernel,
        out_shape=[
            jax.ShapeDtypeStruct((16, 3 * C), jnp.float32),
            jax.ShapeDtypeStruct((16, C), jnp.float32),
            jax.ShapeDtypeStruct(table.shape, jnp.float32),
            jax.ShapeDtypeStruct((2, 16), jnp.float32),
            jax.ShapeDtypeStruct((1, 64), jnp.float32),
        ]
        + [one] * 6,
        in_specs=[pl.BlockSpec(memory_space=pl.ANY)] + [pl.BlockSpec(memory_space=pltpu.VMEM)] * 3,
        out_specs=[pl.BlockSpec(memory_space=pltpu.VMEM)] * 11,
        scratch_shapes=scratch + Swap.scratch((16, C)) + Swap.scratch(table.shape),
        compiler_params=pltpu.CompilerParams(
            collective_id=2, has_side_effects=True, vmem_limit_bytes=40 << 20
        ),
        name="reduce_near",
    )(parts.reshape(4, 2, 2, 2, 64, C), near_vec, far_vec, table)


def settle_kernel(count, *refs):
    for source, target in zip(refs[:count], refs[count:]):
        target[...] = source[...]


def settle(dx, others):
    steps = SIDE // 2
    block = pl.BlockSpec((2, SIDE, 16, C), lambda i: (i, 0, 0, 0))
    whole = [pl.BlockSpec(v.shape, lambda i: (0, 0), pipeline_mode=pl.Buffered(1)) for v in others]
    return pl.pallas_call(
        functools.partial(settle_kernel, 1 + len(others)),
        grid=(steps,),
        in_specs=[block] + whole,
        out_specs=[block] + whole,
        out_shape=[jax.ShapeDtypeStruct(v.shape, v.dtype) for v in (dx, *others)],
        compiler_params=pltpu.CompilerParams(dimension_semantics=("arbitrary",)),
        name="settle",
    )(dx, *others)

ERFC_SLOPE = 0.4
ERFC_TERMS = (
    0.23192538182549352,
    0.16180412136440986,
    0.4683198256010739,
    -0.3709611648908394,
    0.7091781371622337,
    -0.20026632849062864,
)


def gelu_pair(v):
    bell = jnp.exp(v * v * -0.5)
    t = 1.0 / (1.0 + jnp.abs(v) * (ERFC_SLOPE * 0.5**0.5))
    tail = ERFC_TERMS[5] * 0.5
    for term in ERFC_TERMS[4::-1]:
        tail = tail * t + term * 0.5
    tail = tail * t * bell
    below = jnp.where(v < 0, tail, 1.0 - tail)
    return v * below, below + v * (bell * 0.3989422804014327)


def norm_parts(v):
    center = jnp.mean(v, axis=-1, keepdims=True)
    centred = v - center
    spread = jnp.mean(centred * centred, axis=-1, keepdims=True)
    rate = lax.rsqrt(spread + epsilon)
    return centred * rate, rate


def norm_pull(grad, gain, xhat, rate):
    scaled = grad * gain
    first = jnp.mean(scaled, axis=-1, keepdims=True)
    second = jnp.mean(scaled * xhat, axis=-1, keepdims=True)
    return rate * (scaled - first - xhat * second)


def dot_nn(a, b):
    return lax.dot_general(a, b, (((1,), (0,)), ((), ())), preferred_element_type=jnp.float32)


def dot_nt(a, b):
    return lax.dot_general(a, b, (((1,), (1,)), ((), ())), preferred_element_type=jnp.float32)


def dot_tn(a, b):
    return lax.dot_general(a, b, (((0,), (0,)), ((), ())), preferred_element_type=jnp.float32)


def column_sum(v):
    return jnp.sum(v, axis=0, keepdims=True)


def mlp_kernel(
    res_ref, cot_ref, live_ref, far_ref, bias_ref, ebias_ref,
    out_ref, rgrad_ref, part_ref, vec_ref, we_acc, wr_acc, act, hg,
):
    step = pl.program_id(0)
    rows = res_ref.shape[0]

    @pl.when(step == 0)
    def _():
        we_acc[...] = jnp.zeros_like(we_acc)
        wr_acc[...] = jnp.zeros_like(wr_acc)
        vec_ref[...] = jnp.zeros_like(vec_ref)

    res = res_ref[...]
    gain = bias_ref[5:6]
    xhat, rate = norm_parts(res)
    second = (xhat * gain + bias_ref[6:7]).astype(jnp.bfloat16)
    slot = lax.broadcasted_iota(jnp.int32, (16, 1), 0)
    live = jnp.zeros((16, 1), jnp.float32)
    for i in range(16):
        live = jnp.where(slot == i, live_ref[i].astype(jnp.float32), live)
    upstream = (
        cot_ref[...].astype(jnp.float32).reshape(rows // 16, 16, C) * live[None]
    ).reshape(rows, C)
    low = upstream.astype(jnp.bfloat16)
    second_t = second.T
    low_t = low.T
    for b in range(4):
        cut = slice(b * C, (b + 1) * C)
        we = far_ref[:, b * 16 : (b + 1) * 16, :].reshape(C, C)
        hidden = dot_nn(second, we) + ebias_ref[:, cut]
        active, slope = gelu_pair(hidden)
        act[:, cut] = active.astype(jnp.bfloat16)
        wr = far_ref[b * 8 : (b + 1) * 8, 64:128, :].reshape(C, C)
        hg[:, cut] = (dot_nt(low, wr) * slope).astype(jnp.bfloat16)
    reduced = dot_nn(act[...], far_ref[:, 64:128, :].reshape(EXPAND, C))
    pulled = dot_nt(hg[...], jnp.concatenate([far_ref[:, b * 16 : (b + 1) * 16, :].reshape(C, C) for b in range(4)], axis=1))
    for b in range(4):
        cut = slice(b * C, (b + 1) * C)
        wr_acc[b] += dot_nn(low_t, act[:, cut])
        we_acc[b] += dot_nn(second_t, hg[:, cut])
        vec_ref[3 + b : 4 + b] += column_sum(hg[:, cut].astype(jnp.float32))
    out_ref[...] = (res + reduced + bias_ref[7:8]).astype(jnp.bfloat16)
    rgrad_ref[...] = upstream + norm_pull(pulled, gain, xhat, rate)
    vec_ref[0:1] += column_sum(pulled * xhat)
    vec_ref[1:2] += column_sum(pulled)
    vec_ref[2:3] += column_sum(low.astype(jnp.float32))

    @pl.when(step == pl.num_programs(0) - 1)
    def _():
        for b in range(4):
            part_ref[:, b * 16 : (b + 1) * 16, :] = we_acc[b].reshape(RANKS, 16, C).astype(jnp.bfloat16)
            part_ref[b * 8 : (b + 1) * 8, 64:128, :] = (
                wr_acc[b].T.reshape(8, 64, C).astype(jnp.bfloat16)
            )


def mlp_block(res, cot, live, far, vectors, ebias, rows=448):
    tokens = res.shape[0]
    moving = pl.BlockSpec((rows, C), lambda i: (i, 0))
    return pl.pallas_call(
        mlp_kernel,
        grid=(tokens // rows,),
        in_specs=[moving, moving, pl.BlockSpec(memory_space=pltpu.SMEM), fixed((RANKS, FAR, C)), fixed((8, C)), fixed((1, EXPAND))],
        out_specs=[moving, moving, fixed((RANKS, FAR, C)), fixed((8, C))],
        out_shape=[
            jax.ShapeDtypeStruct((tokens, C), jnp.bfloat16),
            jax.ShapeDtypeStruct((tokens, C), jnp.float32),
            jax.ShapeDtypeStruct((RANKS, 128, C), jnp.bfloat16),
            jax.ShapeDtypeStruct((8, C), jnp.float32),
        ],
        scratch_shapes=[pltpu.VMEM((4, C, C), jnp.float32), pltpu.VMEM((4, C, C), jnp.float32), pltpu.VMEM((rows, EXPAND), jnp.bfloat16), pltpu.VMEM((rows, EXPAND), jnp.bfloat16)],
        compiler_params=pltpu.CompilerParams(vmem_limit_bytes=60 << 20, dimension_semantics=("arbitrary",)),
        name="mlp_block",
    )(res, cot, live, far, vectors, ebias)

SPOTS = WIN * WIN
ROWS = SPOTS * 16
QUERY_ROWS = 64
KEY_ROWS = 56
QUAD = 4 * HEAD_DIM
PAIR_SHAPE = (4 * KEY_ROWS, 2 * QUERY_ROWS)
SCALE = HEAD_DIM**-0.5


def spot_of(pane, spot):
    y = lax.rem((pane // 2) * WIN + spot // WIN + SHIFT, SIDE)
    x = lax.rem((pane % 2) * WIN + spot % WIN + SHIFT, SIDE)
    return y, x


def take_pane(pane, source, target):
    for spot in range(SPOTS):
        y, x = spot_of(pane, spot)
        target[spot * 16 : (spot + 1) * 16, :] = source[y, x]


def give_pane(pane, value, target):
    for spot in range(SPOTS):
        y, x = spot_of(pane, spot)
        target[y, x] = value[spot * 16 : (spot + 1) * 16, :]


def put_tiles(target, first, value):
    for tile in range(4):
        target[first + tile, 0:ROWS, :] = value[:, tile * QUAD : (tile + 1) * QUAD]


def get_tiles(source, first):
    return jnp.concatenate([source[first + tile, 0:ROWS, :] for tile in range(4)], axis=1)


def heads_mask(rows):
    return lax.rem(lax.broadcasted_iota(jnp.int32, (rows, 2 * QUAD), 1), QUAD) // HEAD_DIM


def load_pair(source, first, rows):
    return jnp.concatenate([source[first, rows, :], source[first + 1, rows, :]], axis=1)


def spread_heads(pair):
    lanes = heads_mask(KEY_ROWS)
    zero = jnp.zeros_like(pair)
    return jnp.concatenate([jnp.where(lanes == h, pair, zero) for h in range(4)], axis=0).astype(jnp.bfloat16)


def merge_heads(value):
    lanes = heads_mask(KEY_ROWS)
    parts = [value[h * KEY_ROWS : (h + 1) * KEY_ROWS] for h in range(4)]
    return jnp.where(
        lanes < 2, jnp.where(lanes == 0, parts[0], parts[1]), jnp.where(lanes == 2, parts[2], parts[3])
    )


def two_blocks(source, first, rows):
    upper = source[first, rows, :].astype(jnp.bfloat16)
    lower = source[first + 1, rows, :].astype(jnp.bfloat16)
    zero = jnp.zeros_like(upper)
    return jnp.concatenate(
        [jnp.concatenate([upper, zero], axis=1), jnp.concatenate([zero, lower], axis=1)], axis=0
    )


def over_keys(op, value):
    parts = value.reshape(4, KEY_ROWS, 2 * QUERY_ROWS)
    return jnp.broadcast_to(op(parts, axis=1, keepdims=True), parts.shape).reshape(value.shape)


def bias_rows(rows, vec_ref, ebias_ref):
    values = rows[...].astype(jnp.float32)

    def taken(lhs, width):
        source = lax.broadcasted_iota(jnp.int32, (128, RANKS * width), 0)
        target = lax.broadcasted_iota(jnp.int32, (128, RANKS * width), 1)
        onehot = jnp.where(source == lax.rem(target, width), 1.0, 0.0).astype(jnp.bfloat16)
        spread = dot_nn(lhs.reshape(-1, 128).astype(jnp.bfloat16), onehot).reshape(RANKS, -1, RANKS * width)
        shard = lax.broadcasted_iota(jnp.int32, spread.shape, 0)
        place = lax.broadcasted_iota(jnp.int32, spread.shape, 2) // width
        return jnp.sum(jnp.where(shard == place, spread, 0.0), axis=0)

    vec_ref[...] = taken(values[:, 0:8], 16)
    ebias_ref[...] = taken(values[:, 8:16], 64)[0:1]


def attend_kernel(linked, *refs):
    x_ref, bias_ref, mask_ref, *refs = refs
    if linked:
        shards, refs = refs[:5], refs[5:]
    else:
        near, output, rows, *refs = refs
    joint_ref, probs_ref, mixed_ref, res_ref, vec_ref, ebias_ref, *refs = refs
    if linked:
        near_out, output_out, far_out, *refs = refs
    window, wide, blend, both, score_a, score_b, probs_a, probs_b, *refs = refs
    pane = pl.program_id(0)
    last = pl.num_programs(0) - 1
    if linked:
        near, rows, output, far_own, local, *sems = refs
        place = Place()
        close = Gather(place, near.at[place.me], near, *sems[0:2])
        little = Gather(place, rows.at[place.me], rows, *sems[2:4])
        middle = Gather(place, output.at[place.me], output, *sems[4:6])
        distant = Gather(place, far_own, far_out, *sems[6:8])
        joint_w, output_w, expand_w, reduce_w, row_w = shards
        pieces = [
            (joint_w.at[:, b * C : (b + 1) * C], near.at[place.me].at[b * 16 : (b + 1) * 16]) for b in range(3)
        ]
        pieces += [(row_w, rows.at[place.me]), (output_w, output.at[place.me])]
        pieces += [
            (expand_w.at[:, b * C : (b + 1) * C], far_own.at[b * 16 : (b + 1) * 16]) for b in range(4)
        ]
        pieces += [(reduce_w, far_own.at[64:128])]
        pieces = [pltpu.make_async_copy(a, b, local.at[i]) for i, (a, b) in enumerate(pieces)]
        keep = [(near, near_out), (output, output_out), (far_own, far_out.at[place.me])]
        keep = [pltpu.make_async_copy(a, b, local.at[10 + i]) for i, (a, b) in enumerate(keep)]

    @pl.when(pane == 0)
    def _():
        if linked:
            for piece in pieces:
                piece.start()
            place.greet()
            for piece in pieces[:4]:
                piece.wait()
            close.start()
            little.start()
            for piece in pieces[4:]:
                piece.wait()
            middle.start()
            keep[2].start()
        wide[:, ROWS:, :] = jnp.zeros((12, QUERY_ROWS * 16 - ROWS, QUAD), jnp.float32)
        probs_b[...] = jnp.zeros_like(probs_b)
        if linked:
            close.relay_columns()
            little.relay_columns()
            close.relay_sides()
            little.relay_sides()
            middle.relay_columns()
            distant.start()
            close.relay_corners()
            little.relay_corners()
            little.finish()
        bias_rows(rows, vec_ref, ebias_ref)
        if linked:
            close.finish()
            keep[0].start()
            middle.relay_sides()

    if linked:
        @pl.when(pane == 1)
        def _():
            keep[1].start()
            distant.relay_columns()

        @pl.when(pane == 2)
        def _():
            distant.relay_sides()

        @pl.when(pane == 3)
        def _():
            distant.relay_corners()

    take_pane(pane, x_ref, window)
    source = window[...].astype(jnp.float32)
    xhat, _ = norm_parts(source)
    normed = (xhat * vec_ref[0:1] + vec_ref[1:2]).astype(jnp.bfloat16)
    for b in range(3):
        weight = near[:, b * 16 : (b + 1) * 16, :].reshape(C, C)
        block = dot_nn(normed, weight)
        if b != 1:
            block += vec_ref[2 + b // 2 : 3 + b // 2]
        block = block.astype(jnp.bfloat16)
        joint_ref[0, :, b * C : (b + 1) * C] = block
        put_tiles(wide, b * 4, block.astype(jnp.float32))
    for pair in range(2):
        both[pair] = bias_ref[pair] + mask_ref[0]

    def rows_of(m):
        return pl.ds(m, QUERY_ROWS, stride=16), pl.ds(m, KEY_ROWS, stride=16)

    def score(m, target):
        few, many = rows_of(m)
        for pair in range(2):
            k = spread_heads(load_pair(wide, 4 + 2 * pair, many))
            target[pair] = dot_nt(k, two_blocks(wide, 2 * pair, few))

    def soften(m, source, target):
        for pair in range(2):
            scores = source[pair] * SCALE + both[pair]
            powers = jnp.exp(scores - over_keys(jnp.max, scores))
            probs = (powers * (1.0 / over_keys(jnp.sum, powers))).astype(jnp.bfloat16)
            target[pair] = probs
            probs_ref[0, m, pair] = probs

    def mix(m, source):
        few, many = rows_of(m)
        for pair in range(2):
            v = spread_heads(load_pair(wide, 8 + 2 * pair, many))
            blended = dot_tn(source[pair], v)
            blend[2 * pair, many, :] = blended[0:KEY_ROWS, 0:QUAD]
            blend[2 * pair + 1, many, :] = blended[QUERY_ROWS : QUERY_ROWS + KEY_ROWS, QUAD:]

    def two_images(step, carry):
        m = 2 * step
        if linked:
            @pl.when((pane == 0) & (step == 2))
            def _():
                middle.relay_corners()

        mix(jnp.maximum(m - 1, 0), probs_b)
        soften(m, score_a, probs_a)
        score(m + 1, score_b)
        mix(m, probs_a)
        soften(m + 1, score_b, probs_b)
        score(jnp.minimum(m + 2, 15), score_a)
        return carry

    score(0, score_a)
    lax.fori_loop(0, 8, two_images, 0)
    mix(15, probs_b)
    if linked:
        @pl.when(pane == 0)
        def _():
            middle.finish()

    mixed = get_tiles(blend, 0).astype(jnp.bfloat16)
    mixed_ref[0] = mixed
    projected = dot_nn(mixed, output[...].reshape(C, C)) + vec_ref[4:5]
    give_pane(pane, window[...].astype(jnp.float32) + projected, res_ref)

    if linked:
        @pl.when(pane == last)
        def _():
            distant.finish()
            for group in (close, little, middle, distant):
                group.drain()
            for kept in keep:
                kept.wait()


def fixed(shape):
    return pl.BlockSpec(shape, lambda i: (0,) * len(shape), pipeline_mode=pl.Buffered(1))


def stepped(shape):
    return pl.BlockSpec((1,) + shape, lambda i: (i,) + (0,) * len(shape))


def attend(x, bias, mask, weights, linked):
    anywhere = pl.BlockSpec(memory_space=pl.ANY)
    out_specs = [stepped((ROWS, 3 * C)), stepped((16, 2) + PAIR_SHAPE), stepped((ROWS, C)),
                 fixed((SIDE, SIDE, 16, C)), fixed((8, C)), fixed((1, EXPAND))]
    out_shape = [
        jax.ShapeDtypeStruct((PANES, ROWS, 3 * C), jnp.bfloat16),
        jax.ShapeDtypeStruct((PANES, 16, 2) + PAIR_SHAPE, jnp.bfloat16),
        jax.ShapeDtypeStruct((PANES, ROWS, C), jnp.bfloat16),
        jax.ShapeDtypeStruct((SIDE, SIDE, 16, C), jnp.float32),
        jax.ShapeDtypeStruct((8, C), jnp.float32),
        jax.ShapeDtypeStruct((1, EXPAND), jnp.float32),
    ]
    scratch = [
        pltpu.VMEM((ROWS, C), jnp.bfloat16),
        pltpu.VMEM((12, QUERY_ROWS * 16, QUAD), jnp.float32),
        pltpu.VMEM((4, QUERY_ROWS * 16, QUAD), jnp.float32),
        pltpu.VMEM((2,) + PAIR_SHAPE, jnp.float32),
        pltpu.VMEM((2,) + PAIR_SHAPE, jnp.float32),
        pltpu.VMEM((2,) + PAIR_SHAPE, jnp.float32),
        pltpu.VMEM((2,) + PAIR_SHAPE, jnp.bfloat16),
        pltpu.VMEM((2,) + PAIR_SHAPE, jnp.bfloat16),
    ]
    in_specs = [fixed((SIDE, SIDE, 16, C)), fixed((2,) + PAIR_SHAPE), stepped(PAIR_SHAPE)]
    if linked:
        in_specs += [anywhere] * 5
        out_specs += [anywhere] * 3
        out_shape += [
            jax.ShapeDtypeStruct((RANKS, NEAR, C), jnp.bfloat16),
            jax.ShapeDtypeStruct((RANKS, 16, C), jnp.bfloat16),
            jax.ShapeDtypeStruct((RANKS, FAR, C), jnp.bfloat16),
        ]
        scratch += [
            pltpu.VMEM((RANKS, NEAR, C), jnp.bfloat16),
            pltpu.VMEM((RANKS, 16, 128), jnp.bfloat16),
            pltpu.VMEM((RANKS, 16, C), jnp.bfloat16),
            pltpu.VMEM((FAR, C), jnp.bfloat16),
            pltpu.SemaphoreType.DMA((13,)),
        ] + [pltpu.SemaphoreType.DMA((31,))] * 8
        extra = dict(collective_id=0, has_side_effects=True)
    else:
        in_specs += [fixed((RANKS, NEAR, C)), fixed((RANKS, 16, C)), fixed((RANKS, 16, 128))]
        extra = {}
    return pl.pallas_call(
        functools.partial(attend_kernel, linked),
        grid=(PANES,),
        in_specs=in_specs,
        out_specs=out_specs,
        out_shape=out_shape,
        scratch_shapes=scratch,
        compiler_params=pltpu.CompilerParams(
            vmem_limit_bytes=62 << 20, dimension_semantics=("arbitrary",), **extra
        ),
        name="attend",
    )(x, bias, mask, *weights)


def attend_back_kernel(linked, *refs):
    x_ref, near_ref, output_ref, joint_ref, probs_ref, mixed_ref, rgrad_ref, bias_ref, *refs = refs
    if linked:
        far_parts, *refs = refs
    dx_ref, part_ref, vec_ref, pairs_ref, *refs = refs
    if linked:
        ge_ref, gr_ref, *refs = refs
    window, rwindow, wide, blend, turned, wj_acc, wo_acc, pgrad_a, pgrad_b, sgrad_a, sgrad_b, *refs = refs
    pane = pl.program_id(0)
    if linked:
        place = Place()
        distant = Reduce(place, far_parts, refs)

    @pl.when(pane == 0)
    def _():
        if linked:
            place.greet()
            distant.start()
        pads = QUERY_ROWS * 16 - ROWS
        wide[:, ROWS:, :] = jnp.zeros((12, pads, QUAD), jnp.float32)
        blend[:, ROWS:, :] = jnp.zeros((4, pads, QUAD), jnp.float32)
        sgrad_b[...] = jnp.zeros_like(sgrad_b)
        wj_acc[...] = jnp.zeros_like(wj_acc)
        wo_acc[...] = jnp.zeros_like(wo_acc)
        vec_ref[...] = jnp.zeros_like(vec_ref)
        pairs_ref[...] = jnp.zeros_like(pairs_ref)

    if linked:
        @pl.when(pane == 1)
        def _():
            distant.cores()

        @pl.when(pane == 2)
        def _():
            distant.sides()

        @pl.when(pane == 3)
        def _():
            distant.corners()

    take_pane(pane, x_ref, window)
    take_pane(pane, rgrad_ref, rwindow)
    pulled = rwindow[...].astype(jnp.bfloat16)
    wo = output_ref[...].reshape(C, C)
    wo_acc[...] += dot_tn(mixed_ref[0], pulled)
    vec_ref[0:1] += column_sum(pulled.astype(jnp.float32))
    put_tiles(blend, 0, dot_nt(pulled, wo).astype(jnp.bfloat16).astype(jnp.float32))
    for b in range(3):
        put_tiles(wide, b * 4, joint_ref[0, :, b * C : (b + 1) * C].astype(jnp.float32))

    def rows_of(m):
        return pl.ds(m, QUERY_ROWS, stride=16), pl.ds(m, KEY_ROWS, stride=16)

    def pull_probs(m, target):
        few, many = rows_of(m)
        for pair in range(2):
            v = spread_heads(load_pair(wide, 8 + 2 * pair, many))
            target[pair] = dot_nt(v, two_blocks(blend, 2 * pair, few))

    def pull_scores(m, source, target):
        for pair in range(2):
            probs = probs_ref[0, m, pair].astype(jnp.float32)
            weighted = source[pair] * probs
            sgrad = (weighted - probs * over_keys(jnp.sum, weighted)).astype(jnp.bfloat16)
            target[pair] = sgrad
            pairs_ref[pair] += sgrad.astype(jnp.float32)

    def pull_rest(m, source):
        few, many = rows_of(m)
        for pair in range(2):
            sgrad = source[pair]
            k = spread_heads(load_pair(wide, 4 + 2 * pair, many))
            qgrad = dot_tn(sgrad, k) * SCALE
            turned[2 * pair, many, :] = qgrad[0:KEY_ROWS, 0:QUAD]
            turned[2 * pair + 1, many, :] = qgrad[QUERY_ROWS : QUERY_ROWS + KEY_ROWS, QUAD:]
            kgrad = merge_heads(dot_nn(sgrad, two_blocks(wide, 2 * pair, few))) * SCALE
            turned[4 + 2 * pair, many, :] = kgrad[:, 0:QUAD]
            turned[5 + 2 * pair, many, :] = kgrad[:, QUAD:]
            vgrad = merge_heads(dot_nn(probs_ref[0, m, pair], two_blocks(blend, 2 * pair, few)))
            turned[8 + 2 * pair, many, :] = vgrad[:, 0:QUAD]
            turned[9 + 2 * pair, many, :] = vgrad[:, QUAD:]

    def two_images(step, carry):
        m = 2 * step
        pull_rest(jnp.maximum(m - 1, 0), sgrad_b)
        pull_scores(m, pgrad_a, sgrad_a)
        pull_probs(m + 1, pgrad_b)
        pull_rest(m, sgrad_a)
        pull_scores(m + 1, pgrad_b, sgrad_b)
        pull_probs(jnp.minimum(m + 2, 15), pgrad_a)
        return carry

    pull_probs(0, pgrad_a)
    lax.fori_loop(0, 8, two_images, 0)
    pull_rest(15, sgrad_b)
    gain = bias_ref[0:1]
    xhat, rate = norm_parts(window[...].astype(jnp.float32))
    normed = (xhat * gain + bias_ref[1:2]).astype(jnp.bfloat16)
    normed_t = normed.T
    total = jnp.zeros((ROWS, C), jnp.float32)
    for b in range(3):
        weight = near_ref[:, b * 16 : (b + 1) * 16, :].reshape(C, C)
        block = get_tiles(turned, b * 4).astype(jnp.bfloat16)
        wj_acc[b] += dot_nn(normed_t, block)
        total += dot_nt(block, weight)
        if b != 1:
            vec_ref[1 + b // 2 : 2 + b // 2] += column_sum(block.astype(jnp.float32))
    vec_ref[3:4] += column_sum(total * xhat)
    vec_ref[4:5] += column_sum(total)
    dx = rwindow[...] + norm_pull(total, gain, xhat, rate)
    give_pane(pane, dx.astype(jnp.bfloat16), dx_ref)

    @pl.when(pane == PANES - 1)
    def _():
        for b in range(3):
            part_ref[:, b * 16 : (b + 1) * 16, :] = wj_acc[b].reshape(RANKS, 16, C).astype(jnp.bfloat16)
        part_ref[:, 48:64, :] = wo_acc[...].reshape(RANKS, 16, C).astype(jnp.bfloat16)
        if linked:
            total = distant.finish()
            for b in range(4):
                ge_ref[:, b * C : (b + 1) * C] = total[b * 16 : (b + 1) * 16]
            gr_ref[...] = total[64:128]
            distant.drain()


def attend_back(x, near, output, joint, probs, mixed, rgrad, vectors, far_parts, linked):
    in_specs = [fixed((SIDE, SIDE, 16, C)), fixed((RANKS, NEAR, C)), fixed((RANKS, 16, C)), stepped((ROWS, 3 * C)),
                stepped((16, 2) + PAIR_SHAPE), stepped((ROWS, C)), fixed((SIDE, SIDE, 16, C)), fixed((8, C))]
    out_specs = [fixed((SIDE, SIDE, 16, C)), fixed((RANKS, 64, C)), fixed((8, C)), fixed((2,) + PAIR_SHAPE)]
    out_shape = [
        jax.ShapeDtypeStruct((SIDE, SIDE, 16, C), jnp.bfloat16),
        jax.ShapeDtypeStruct((RANKS, 64, C), jnp.bfloat16),
        jax.ShapeDtypeStruct((8, C), jnp.float32),
        jax.ShapeDtypeStruct((2,) + PAIR_SHAPE, jnp.float32),
    ]
    scratch = [
        pltpu.VMEM((ROWS, C), jnp.bfloat16),
        pltpu.VMEM((ROWS, C), jnp.float32),
        pltpu.VMEM((12, QUERY_ROWS * 16, QUAD), jnp.float32),
        pltpu.VMEM((4, QUERY_ROWS * 16, QUAD), jnp.float32),
        pltpu.VMEM((12, QUERY_ROWS * 16, QUAD), jnp.float32),
        pltpu.VMEM((3, C, C), jnp.float32),
        pltpu.VMEM((C, C), jnp.float32),
        pltpu.VMEM((2,) + PAIR_SHAPE, jnp.float32),
        pltpu.VMEM((2,) + PAIR_SHAPE, jnp.float32),
        pltpu.VMEM((2,) + PAIR_SHAPE, jnp.bfloat16),
        pltpu.VMEM((2,) + PAIR_SHAPE, jnp.bfloat16),
    ]
    operands = [x, near, output, joint, probs, mixed, rgrad, vectors]
    extra = {}
    if linked:
        in_specs.append(pl.BlockSpec(memory_space=pl.ANY))
        out_specs += [fixed((16, EXPAND)), fixed((64, C))]
        out_shape += [
            jax.ShapeDtypeStruct((16, EXPAND), jnp.float32),
            jax.ShapeDtypeStruct((64, C), jnp.float32),
        ]
        scratch += Reduce.scratch(FAR)
        operands.append(far_parts.reshape(4, 2, 2, 2, FAR, C))
        extra = dict(collective_id=1, has_side_effects=True)
    return pl.pallas_call(
        functools.partial(attend_back_kernel, linked),
        grid=(PANES,),
        in_specs=in_specs,
        out_specs=out_specs,
        out_shape=out_shape,
        scratch_shapes=scratch,
        compiler_params=pltpu.CompilerParams(
            vmem_limit_bytes=(1 << 26) - (64 << 10), dimension_semantics=("arbitrary",), **extra
        ),
        name="attend_back",
    )(*operands)


def pair_tables(bias_table, regions):
    keys, queries = jnp.arange(KEY_ROWS), jnp.arange(QUERY_ROWS)
    real = (keys < SPOTS)[:, None] & (queries < SPOTS)[None, :]
    cells = (
        (queries[None, :] // WIN - keys[:, None] // WIN + WIN - 1) * (2 * WIN - 1)
        + queries[None, :] % WIN - keys[:, None] % WIN + WIN - 1
    )
    cells = jnp.where(real, cells, -1).reshape(-1)
    onehot = (cells[None, :] == jnp.arange((2 * WIN - 1) ** 2)[:, None]).astype(jnp.bfloat16)
    bias = dot_tn(bias_table, onehot).reshape(2, 2, 4, KEY_ROWS, QUERY_ROWS)
    bias = jnp.where((keys < SPOTS)[:, None], bias, -1e30)
    bias = bias.transpose(0, 2, 3, 1, 4).reshape((2,) + PAIR_SHAPE)
    labels = jnp.roll(regions, (-SHIFT, -SHIFT), axis=(0, 1)).reshape(2, WIN, 2, WIN)
    labels = labels.transpose(0, 2, 1, 3).reshape(PANES, SPOTS)
    along = jnp.tile(jnp.pad(labels, ((0, 0), (0, KEY_ROWS - SPOTS))), (1, 4))
    across = jnp.tile(jnp.pad(labels, ((0, 0), (0, QUERY_ROWS - SPOTS))), (1, 2))
    mask = jnp.where(along[:, :, None] == across[:, None, :], 0.0, -100.0).astype(jnp.float32)
    return bias, mask, onehot


def table_sums(pairs, onehot):
    heads = pairs.reshape(2, 4, KEY_ROWS, 2, QUERY_ROWS).transpose(0, 3, 1, 2, 4)
    return lax.dot_general(
        heads.reshape(HEADS, KEY_ROWS * QUERY_ROWS), onehot.astype(jnp.float32), (((1,), (1,)), ((), ())),
        precision=exact_mode, preferred_element_type=jnp.float32,
    )

def regroup(packed, blocks, rows):
    count = packed.shape[0] // RANKS
    return (
        packed.reshape(RANKS, count, blocks, rows, C)
        .transpose(0, 2, 1, 3, 4)
        .reshape(RANKS, blocks * rows * count, C)
    )


def ungroup(parts, blocks, ranks):
    rows = parts.shape[1] // blocks
    flat = parts.reshape(RANKS, blocks, rows, C).transpose(1, 0, 2, 3).reshape(blocks, RANKS * rows, C)
    return flat.reshape(blocks, ranks, RANKS * rows // ranks, C).transpose(1, 0, 2, 3)


def on_device(
    images,
    first_gain,
    first_shift,
    joint_weight,
    joint_bias,
    output_weight,
    output_bias,
    second_gain,
    second_shift,
    expand_weight,
    expand_bias,
    reduce_weight,
    reduce_bias,
    bias_table,
    regions,
    live_slots,
    cotangent,
):
    ranks = lax.axis_size("dp")
    count = images.shape[0]
    linked = ranks == RANKS
    small = (
        first_gain,
        first_shift,
        joint_bias[0],
        joint_bias[1],
        output_bias,
        second_gain,
        second_shift,
        reduce_bias,
        expand_bias,
    )
    x = images.transpose(1, 2, 0, 3)
    cot = cotangent.transpose(1, 2, 0, 3).reshape(-1, C)
    bias, mask, onehot = pair_tables(bias_table, regions)
    if linked:
        row = jnp.zeros((16, 128), jnp.bfloat16)
        for first, vector in (
            (0, first_gain), (1, first_shift), (2, joint_bias), (4, output_bias), (5, second_gain),
            (6, second_shift), (7, reduce_bias), (8, expand_bias),
        ):
            vector = jnp.atleast_2d(vector)
            height, width = vector.shape
            row += jnp.pad(vector, ((first, 16 - first - height), (0, 128 - width)))
        weights = (joint_weight, output_weight, expand_weight, reduce_weight, row)
        joint, probs, mixed, res, vectors, ebias, near, output, far = attend(x, bias, mask, weights, True)
    else:
        rows = C // ranks
        wide = lambda w: lax.all_gather(w, "dp", axis=0)
        near = jnp.concatenate([wide(joint_weight[:, i * C : (i + 1) * C]) for i in range(3)], axis=1)
        near, output = regroup(near, 3, rows), regroup(wide(output_weight), 1, rows)
        pieces = [
            lax.all_gather(v, "dp", axis=0, tiled=True).reshape(RANKS, 1, -1) for v in small
        ]
        row = jnp.concatenate([jnp.pad(v, ((0, 0), (0, 0), (0, 128 - v.shape[2]))) for v in pieces], axis=1)
        row = jnp.pad(row, ((0, 0), (0, 7), (0, 0)))
        far = jnp.concatenate([wide(expand_weight[:, i * C : (i + 1) * C]) for i in range(4)], axis=1)
        far = jnp.concatenate([regroup(far, 4, rows), wide(reduce_weight).reshape(RANKS, 64, C)], axis=1)
        joint, probs, mixed, res, vectors, ebias = attend(x, bias, mask, (near, output, row), False)
    out, rgrad, far_part, far_vec = mlp_block(
        res.reshape(-1, C), cot, live_slots, far, vectors, ebias
    )
    rgrad = rgrad.reshape(SIDE, SIDE, count, C)
    dx, near_part, near_vec, pairs, *far_grads = attend_back(
        x, near, output, joint, probs, mixed, rgrad, vectors, far_part, linked
    )
    table = table_sums(pairs, onehot)
    if linked:
        ge, gr = far_grads
        reduced = reduce_near(near_part, near_vec, far_vec, table)
        dx, ge, gr, gj, go, table, jb, eb, *own = settle(dx, (ge, gr, *reduced))
        own = [v.reshape(-1) for v in own]
        ob, gain1, shift1, gain2, shift2, rb = own
        eb = eb.reshape(-1)
    else:
        scatter = lambda g: lax.psum_scatter(g.astype(jnp.float32), "dp", scatter_dimension=0, tiled=True)
        cut = lambda part, blocks: scatter(
            ungroup(part, blocks, ranks).transpose(0, 2, 1, 3).reshape(C, blocks * C)
        )
        gj, go = cut(near_part[:, :48], 3), cut(near_part[:, 48:], 1)
        ge, gr = cut(far_part[:, :64], 4), scatter(far_part[:, 64:].reshape(EXPAND, C))
        ob, qb, vb, gain1, shift1 = [scatter(near_vec[i]) for i in range(5)]
        gain2, shift2, rb = [scatter(far_vec[i]) for i in range(3)]
        eb, jb = scatter(far_vec[3:7].reshape(-1)), jnp.stack([qb, vb])
        table = lax.psum(table, "dp")
    image_order = lambda v: v.reshape(SIDE, SIDE, count, C).transpose(2, 0, 1, 3)
    return (
        image_order(out),
        image_order(dx),
        gain1,
        shift1,
        gj,
        jb,
        go,
        ob,
        gain2,
        shift2,
        ge,
        eb,
        gr,
        rb,
        table.T,
    )


def solution(mesh):
    in_specs = (
        P("dp", None, None, None),
        P("dp"),
        P("dp"),
        P("dp", None),
        P(None, "dp"),
        P("dp", None),
        P("dp"),
        P("dp"),
        P("dp"),
        P("dp", None),
        P("dp"),
        P("dp", None),
        P("dp"),
        P(),
        P(),
        P("dp"),
        P("dp", None, None, None),
    )
    out_specs = (
        P("dp", None, None, None),
        P("dp", None, None, None),
        P("dp"),
        P("dp"),
        P("dp", None),
        P(None, "dp"),
        P("dp", None),
        P("dp"),
        P("dp"),
        P("dp"),
        P("dp", None),
        P("dp"),
        P("dp", None),
        P("dp"),
        P(),
    )
    return jax.shard_map(
        on_device, mesh=mesh, in_specs=in_specs, out_specs=out_specs, check_vma=False
    )
```

```python
import functools

import jax
import jax.numpy as jnp
from jax import lax
from jax.experimental import pallas as pl
from jax.experimental.pallas import tpu as pltpu
from jax.sharding import PartitionSpec as P

C = 512
HEADS = 16
HEAD_DIM = 32
EXPAND = 2048
WIN = 7
SIDE = 14
SHIFT = 3
PANES = 4
RANKS = 32

epsilon = 1e-05
exact_mode = lax.Precision.HIGHEST

MESH = pl.DeviceIdType.MESH
NEAR = 48
FAR = 128


def rank_of(z, y, x, c):
    return z * 8 + y * 4 + x * 2 + c


def flip(z, k):
    low, high = lax.rem(z, 2), z // 2
    if k % 2:
        low = 1 - low
    if k // 2:
        high = 1 - high
    return high * 2 + low


class Place:
    def __init__(self):
        self.me = lax.axis_index("dp")
        self.z, self.y = self.me // 8, lax.rem(self.me // 4, 2)
        self.x, self.c = lax.rem(self.me // 2, 2), lax.rem(self.me, 2)
        self.peer_x = rank_of(self.z, self.y, 1 - self.x, self.c)
        self.peer_y = rank_of(self.z, 1 - self.y, self.x, self.c)
        self.mate = rank_of(self.z, self.y, self.x, 1 - self.c)
        self.peers_z = [rank_of(flip(self.z, k), self.y, self.x, self.c) for k in (1, 2, 3)]

    def column(self, k, dy, dx):
        y = 1 - self.y if dy else self.y
        x = 1 - self.x if dx else self.x
        return rank_of(flip(self.z, k), y, x, self.c)

    def greet(self):
        barrier = pltpu.get_barrier_semaphore()
        peers = [self.mate, self.peer_x, self.peer_y] + self.peers_z
        for peer in peers:
            pl.semaphore_signal(barrier, inc=1, device_id=(peer,), device_id_type=MESH)
        pl.semaphore_wait(barrier, len(peers))


def remote(source, target, send, recv, rank):
    return pltpu.make_async_remote_copy(
        src_ref=source, dst_ref=target, send_sem=send, recv_sem=recv, device_id=(rank,), device_id_type=MESH
    )


class Gather:
    def __init__(self, place, own, full, send, recv, start=0, rows=None):
        self.place, self.own, self.full, self.send, self.recv = place, own, full, send, recv
        self.cut = pl.ds(start, full.shape[1] if rows is None else rows)

    def at(self, owner):
        return self.full.at[owner, self.cut]

    def push(self, lane, owner, rank, source=None):
        source = self.at(owner) if source is None else source
        remote(source, self.at(owner), self.send.at[lane], self.recv.at[lane], rank).start()

    def some(self, lane):
        place = self.place
        return remote(
            self.own, self.at(place.me), self.send.at[lane], self.recv.at[lane], place.mate
        )

    def start(self):
        place = self.place
        for k in (1, 2, 3):
            self.push(k - 1, place.me, place.peers_z[k - 1], self.own)
        self.push(3, place.me, place.peer_x, self.own)
        self.push(7, place.me, place.peer_y, self.own)
        self.push(15, place.me, place.mate, self.own)

    def relay_columns(self):
        place = self.place
        for k in (1, 2, 3):
            self.some(k - 1).wait_recv()
            owner = place.column(k, 0, 0)
            self.push(3 + k, owner, place.peer_x)
            self.push(7 + k, owner, place.peer_y)
            self.push(15 + k, owner, place.mate)

    def relay_sides(self):
        place = self.place
        for k in range(4):
            self.some(3 + k).wait_recv()
            owner = place.column(k, 0, 1)
            if k % 2 == 0:
                self.push(11 + k, owner, place.peer_y)
            self.push(19 + k, owner, place.mate)
            self.some(7 + k).wait_recv()
            owner = place.column(k, 1, 0)
            if k % 2 == 1:
                self.push(11 + k, owner, place.peer_x)
            self.push(23 + k, owner, place.mate)

    def relay_corners(self):
        place = self.place
        for k in range(4):
            self.some(11 + k).wait_recv()
            self.push(27 + k, place.column(k, 1, 1), place.mate)

    def finish(self):
        for lane in range(15, 31):
            self.some(lane).wait_recv()

    def drain(self):
        for lane in range(31):
            self.some(lane).wait_send()


class Reduce:
    def __init__(self, place, parts, scratch, start=0):
        self.place = place
        self.acc = scratch[0]
        self.cut = pl.ds(start, self.acc.shape[3])
        self.parts = parts
        self.acc, self.rc, self.r1x, self.r1y, self.r2x, self.r2y, self.rz = scratch[:7]
        self.local, self.send, self.recv = scratch[7:]

    @staticmethod
    def scratch(rows):
        shapes = [(4, 2, 2), (4, 2, 2), (2, 2), (2, 2), (2,), (2,), (3,)]
        return [pltpu.VMEM(s + (rows, C), jnp.bfloat16) for s in shapes] + [
            pltpu.SemaphoreType.DMA(()),
            pltpu.SemaphoreType.DMA((8,)),
            pltpu.SemaphoreType.DMA((8,)),
        ]

    def copies(self, lane):
        p, a = self.place, self.acc
        source, target, rank = {
            0: lambda: (self.parts.at[:, :, :, 1 - p.c, self.cut], self.rc, p.mate),
            1: lambda: (a.at[0:2, :, 1 - p.x], self.r1x, p.peer_x),
            2: lambda: (a.at[2:4, 1 - p.y, :], self.r1y, p.peer_y),
            3: lambda: (a.at[0:2, 1 - p.y, p.x], self.r2y, p.peer_y),
            4: lambda: (a.at[2:4, p.y, 1 - p.x], self.r2x, p.peer_x),
            5: lambda: (a.at[flip(p.z, 1), p.y, p.x], self.rz.at[0], p.peers_z[0]),
            6: lambda: (a.at[flip(p.z, 2), p.y, p.x], self.rz.at[1], p.peers_z[1]),
            7: lambda: (a.at[flip(p.z, 3), p.y, p.x], self.rz.at[2], p.peers_z[2]),
        }[lane]()
        return remote(source, target, self.send.at[lane], self.recv.at[lane], rank)

    def mine(self):
        return pltpu.make_async_copy(self.parts.at[:, :, :, self.place.c, self.cut], self.acc, self.local)

    def add(self, where, other):
        total = self.acc[where].astype(jnp.float32) + other.astype(jnp.float32)
        self.acc[where] = total.astype(jnp.bfloat16)

    def start(self):
        self.copies(0).start()
        self.mine().start()

    def cores(self):
        self.mine().wait()
        self.copies(0).wait_recv()

        def body(zz, carry):
            for yy in range(2):
                for xx in range(2):
                    self.add((zz, yy, xx), self.rc[zz, yy, xx])
            return carry

        lax.fori_loop(0, 4, body, 0)
        self.copies(1).start()
        self.copies(2).start()

    def sides(self):
        p = self.place
        self.copies(1).wait_recv()
        self.copies(2).wait_recv()
        for zz in range(2):
            for other in range(2):
                self.add((zz, other, p.x), self.r1x[zz, other])
                self.add((2 + zz, p.y, other), self.r1y[zz, other])
        self.copies(3).start()
        self.copies(4).start()

    def corners(self):
        p = self.place
        self.copies(3).wait_recv()
        self.copies(4).wait_recv()
        for zz in range(2):
            self.add((zz, p.y, p.x), self.r2y[zz])
            self.add((2 + zz, p.y, p.x), self.r2x[zz])
        for lane in (5, 6, 7):
            self.copies(lane).start()

    def finish(self):
        p = self.place
        total = self.acc[p.z, p.y, p.x].astype(jnp.float32)
        for lane in (5, 6, 7):
            self.copies(lane).wait_recv()
            total += self.rz[lane - 5].astype(jnp.float32)
        return total

    def drain(self):
        for lane in range(8):
            self.copies(lane).wait_send()


class Swap:
    def __init__(self, place, scratch):
        self.place = place
        self.own, self.got, self.send, self.recv = scratch

    @staticmethod
    def scratch(shape):
        return [
            pltpu.VMEM((4,) + shape, jnp.float32),
            pltpu.VMEM((6,) + shape, jnp.float32),
            pltpu.SemaphoreType.DMA((6,)),
            pltpu.SemaphoreType.DMA((6,)),
        ]

    def copies(self, lane):
        p = self.place
        rank = ([p.mate, p.peer_x, p.peer_y] + p.peers_z)[lane]
        return remote(
            self.own.at[min(lane, 3)], self.got.at[lane], self.send.at[lane], self.recv.at[lane], rank
        )

    def hop(self, lane):
        self.copies(lane).wait_recv()
        self.own[lane + 1] = self.own[lane] + self.got[lane]
        if lane < 2:
            self.copies(lane + 1).start()
        else:
            for last in (3, 4, 5):
                self.copies(last).start()

    def finish(self):
        for lane in (3, 4, 5):
            self.copies(lane).wait_recv()
        return (self.own[3] + self.got[3]) + (self.got[4] + self.got[5])

    def drain(self):
        for lane in range(6):
            self.copies(lane).wait_send()


HALVES = 2
HALF = 64 // HALVES
CELLS = (2 * WIN - 1) ** 2
KEYS, QUERIES = 56, 64


def seventh(v):
    return (v * 37) >> 8


def offset_onehot():
    lane = lax.broadcasted_iota(jnp.int32, (1, KEYS * QUERIES), 1)
    key, query = lane >> 6, lane & 63
    key_y, query_y = seventh(key), seventh(query)
    key_x, query_x = key - WIN * key_y, query - WIN * query_y
    cell = (query_y - key_y + WIN - 1) * (2 * WIN - 1) + query_x - key_x + WIN - 1
    offset = lax.broadcasted_iota(jnp.int32, (CELLS, KEYS * QUERIES), 0)
    return jnp.where(offset == cell, 1.0, 0.0).astype(jnp.bfloat16)


def reorder(value):
    row = lax.broadcasted_iota(jnp.int32, (HEADS, HEADS), 0)
    col = lax.broadcasted_iota(jnp.int32, (HEADS, HEADS), 1)
    moved = ((row >> 2) & 1) * 8 + (row >> 3) * 4 + (row & 3)
    order = jnp.where(moved == col, 1.0, 0.0).astype(jnp.bfloat16)
    return sum(dot_nn(order, piece) for piece in pieces_of(value))


def pieces_of(value):
    high = value.astype(jnp.bfloat16)
    rest = value - high.astype(jnp.float32)
    middle = rest.astype(jnp.bfloat16)
    return high, middle, (rest - middle.astype(jnp.float32)).astype(jnp.bfloat16)


def swap_halves(first, second):
    low = lax.broadcasted_iota(jnp.int32, first.shape, 1) < QUERIES
    return (
        jnp.where(low, first, pltpu.roll(second, QUERIES, 1)),
        jnp.where(low, pltpu.roll(first, QUERIES, 1), second),
    )


def table_sums(pairs, heads):
    for tile in range(KEYS // 2):
        upper, lower = swap_halves(
            pairs[pl.ds(2 * tile, 8, stride=KEYS), :], pairs[pl.ds(2 * tile + 1, 8, stride=KEYS), :]
        )
        heads[0:8, tile * 128 : (tile + 1) * 128] = upper
        heads[8:16, tile * 128 : (tile + 1) * 128] = lower
    sums = dot_nt(jnp.concatenate(pieces_of(heads[...]), axis=0), offset_onehot())
    return sums[0:16] + sums[16:32] + sums[32:48]


def reduce_near_kernel(
    parts, near_vec, far_vec, pairs_ref,
    gj_ref, go_ref, table_out, jb_ref, eb_ref, *rest,
):
    owns, rest = rest[:6], rest[6:]
    bias_scratch, spread, heads, rest = rest[0], rest[1], rest[2], rest[3:]
    bigs, rest = [rest[i * 10 : i * 10 + 10] for i in range(HALVES)], rest[10 * HALVES :]
    place = Place()
    place.greet()
    bigs = [Reduce(place, parts, scratch, i * HALF) for i, scratch in enumerate(bigs)]
    vec = Swap(place, rest[0:4])
    tab = Swap(place, rest[4:8])
    vec.own[0, 0:8] = near_vec[...]
    vec.own[0, 8:16] = far_vec[...]
    vec.copies(0).start()
    for big in bigs:
        big.start()
    tab.own[0] = table_sums(pairs_ref, heads)
    tab.copies(0).start()
    vec.hop(0)
    for big in bigs:
        big.cores()
    tab.hop(0)
    vec.hop(1)
    for big in bigs:
        big.sides()
    tab.hop(1)
    vec.hop(2)
    for big in bigs:
        big.corners()
    tab.hop(2)
    for i, big in enumerate(bigs):
        total = big.finish()
        for block in range(HALF // 16):
            b = i * (HALF // 16) + block
            rows = total[block * 16 : (block + 1) * 16]
            if b < 3:
                gj_ref[:, b * C : (b + 1) * C] = rows
            else:
                go_ref[...] = rows
    sums = vec.finish()
    table_out[...] = reorder(tab.finish())
    for tile in range(4):
        spread[tile] = sums[:, tile * 128 : (tile + 1) * 128]
    me = place.me
    turn = lax.rem(128 - 16 * lax.rem(me, 8), 128)
    mine = pltpu.roll(spread[me // 8], turn, 1)[:, 0:16]
    jb_ref[...] = mine[1:3]
    for own, row in zip(owns, (0, 3, 4, 8, 9, 10)):
        own[...] = mine[row : row + 1]
    wide = pltpu.roll(spread[lax.rem(me, 8) // 2], 64 * lax.rem(me, 2), 1)[:, 0:64]
    bias_scratch[...] = wide[8:16]
    eb_ref[...] = bias_scratch[pl.ds(3 + me // 8, 1), :]
    for big in bigs:
        big.drain()
    vec.drain()
    tab.drain()


def reduce_near(parts, near_vec, far_vec, pairs):
    one = jax.ShapeDtypeStruct((1, 16), jnp.float32)
    scratch = [pltpu.VMEM((8, 64), jnp.float32), pltpu.VMEM((4, 16, 128), jnp.float32)]
    scratch += [pltpu.VMEM((HEADS, KEYS * QUERIES), jnp.float32)]
    for _ in range(HALVES):
        scratch += Reduce.scratch(HALF)
    out_shape = [
        jax.ShapeDtypeStruct((16, 3 * C), jnp.float32),
        jax.ShapeDtypeStruct((16, C), jnp.float32),
        jax.ShapeDtypeStruct((HEADS, CELLS), jnp.float32),
        jax.ShapeDtypeStruct((2, 16), jnp.float32),
        jax.ShapeDtypeStruct((1, 64), jnp.float32),
    ] + [one] * 6
    return pl.pallas_call(
        reduce_near_kernel,
        out_shape=out_shape,
        grid=(1,),
        in_specs=[pl.BlockSpec(memory_space=pl.ANY)] + [fixed(v.shape) for v in (near_vec, far_vec, pairs)],
        out_specs=[fixed(v.shape) for v in out_shape],
        scratch_shapes=scratch + Swap.scratch((16, C)) + Swap.scratch((HEADS, CELLS)),
        compiler_params=pltpu.CompilerParams(
            collective_id=2, has_side_effects=True, vmem_limit_bytes=62 << 20
        ),
        name="reduce_near",
    )(parts.reshape(4, 2, 2, 2, 64, C), near_vec, far_vec, pairs)


def fixed(shape):
    return pl.BlockSpec(shape, lambda i: (0,) * len(shape), pipeline_mode=pl.Buffered(1))


def settle_kernel(count, quarters, *refs):
    sources, targets, rest = refs[:count], refs[count : 2 * count], refs[2 * count :]
    held, come, go = rest[:count], rest[count], rest[count + 1]
    cuts = [slice(None)] * (count - 1) + [pl.ds(2 * i, 2) for i in range(quarters)]
    index = list(range(1, count)) + [0] * quarters
    inward = [
        pltpu.make_async_copy(sources[n].at[cut], held[n].at[cut], come.at[i])
        for i, (n, cut) in enumerate(zip(index, cuts))
    ]
    outward = [
        pltpu.make_async_copy(held[n].at[cut], targets[n].at[cut], go.at[i])
        for i, (n, cut) in enumerate(zip(index, cuts))
    ]
    for copy in inward:
        copy.start()
    for first, then in zip(inward, outward):
        first.wait()
        then.start()
    for copy in outward:
        copy.wait()


def settle(dx, others):
    anywhere = pl.BlockSpec(memory_space=pl.ANY)
    arrays = (dx, *others)
    count, quarters = len(arrays), dx.shape[0] // 2
    moves = count - 1 + quarters
    return pl.pallas_call(
        functools.partial(settle_kernel, count, quarters),
        in_specs=[anywhere] * count,
        out_specs=[anywhere] * count,
        out_shape=[jax.ShapeDtypeStruct(v.shape, v.dtype) for v in arrays],
        scratch_shapes=[pltpu.VMEM(v.shape, v.dtype) for v in arrays]
        + [pltpu.SemaphoreType.DMA((moves,)), pltpu.SemaphoreType.DMA((moves,))],
        compiler_params=pltpu.CompilerParams(vmem_limit_bytes=62 << 20),
        name="settle",
    )(*arrays)

ERFC_SLOPE = 0.4
ERFC_TERMS = (
    0.23192538182549352,
    0.16180412136440986,
    0.4683198256010739,
    -0.3709611648908394,
    0.7091781371622337,
    -0.20026632849062864,
)


def gelu_pair(v):
    bell = jnp.exp2(v * v * -0.7213475204444817)
    t = 1.0 / (1.0 + jnp.abs(v) * (ERFC_SLOPE * 0.5**0.5))
    tail = ERFC_TERMS[5] * 0.5
    for term in ERFC_TERMS[4::-1]:
        tail = tail * t + term * 0.5
    tail = tail * t * bell
    below = jnp.where(v < 0, tail, 1.0 - tail)
    return v * below, below + v * (bell * 0.3989422804014327)


def norm_parts(v):
    center = jnp.mean(v, axis=-1, keepdims=True)
    centred = v - center
    spread = jnp.mean(centred * centred, axis=-1, keepdims=True)
    rate = lax.rsqrt(spread + epsilon)
    return centred * rate, rate


def norm_pull(grad, gain, xhat, rate):
    scaled = grad * gain
    first = jnp.mean(scaled, axis=-1, keepdims=True)
    second = jnp.mean(scaled * xhat, axis=-1, keepdims=True)
    return rate * (scaled - first - xhat * second)


def dot_nn(a, b):
    return lax.dot_general(a, b, (((1,), (0,)), ((), ())), preferred_element_type=jnp.float32)


def dot_nt(a, b):
    return lax.dot_general(a, b, (((1,), (1,)), ((), ())), preferred_element_type=jnp.float32)


def dot_tn(a, b):
    return lax.dot_general(a, b, (((0,), (0,)), ((), ())), preferred_element_type=jnp.float32)


def column_sum(v):
    return jnp.sum(v, axis=0, keepdims=True)


def mlp_kernel(
    res_ref, cot_ref, live_ref, far_ref, bias_ref, ebias_ref,
    out_ref, rgrad_ref, part_ref, vec_ref, we_acc, wr_acc, act, hg,
):
    step = pl.program_id(0)
    rows = res_ref.shape[0]

    @pl.when(step == 0)
    def _():
        we_acc[...] = jnp.zeros_like(we_acc)
        wr_acc[...] = jnp.zeros_like(wr_acc)
        vec_ref[...] = jnp.zeros_like(vec_ref)

    res = res_ref[...]
    gain = bias_ref[5:6]
    xhat, rate = norm_parts(res)
    second = (xhat * gain + bias_ref[6:7]).astype(jnp.bfloat16)
    slot = lax.broadcasted_iota(jnp.int32, (16, 1), 0)
    live = jnp.zeros((16, 1), jnp.float32)
    for i in range(16):
        live = jnp.where(slot == i, live_ref[i].astype(jnp.float32), live)
    upstream = (
        cot_ref[...].astype(jnp.float32).reshape(rows // 16, 16, C) * live[None]
    ).reshape(rows, C)
    low = upstream.astype(jnp.bfloat16)
    second_t = second.T
    low_t = low.T
    we_of = lambda b: far_ref[:, b * 16 : (b + 1) * 16, :].reshape(C, C)

    def weight_grads(b):
        cut = slice(b * C, (b + 1) * C)
        wr_acc[b] += dot_nn(low_t, act[:, cut])
        we_acc[b] += dot_nn(second_t, hg[:, cut])
        vec_ref[3 + b : 4 + b] += column_sum(hg[:, cut].astype(jnp.float32))

    for b in range(8):
        cut = slice(b * 256, (b + 1) * 256)
        we = we_of(b // 2)[:, (b % 2) * 256 : (b % 2 + 1) * 256]
        wr = far_ref[b * 4 : (b + 1) * 4, 64:128, :].reshape(256, C)
        hidden = dot_nn(second, we) + ebias_ref[:, cut]
        active, slope = gelu_pair(hidden)
        act[:, cut] = active.astype(jnp.bfloat16)
        hg[:, cut] = (dot_nt(low, wr) * slope).astype(jnp.bfloat16)
        if b % 2 and b > 1:
            weight_grads(b // 2 - 1)
    weight_grads(3)
    reduced = dot_nn(act[...], far_ref[:, 64:128, :].reshape(EXPAND, C))
    pulled = dot_nt(hg[...], jnp.concatenate([we_of(b) for b in range(4)], axis=1))
    out_ref[...] = (res + reduced + bias_ref[7:8]).astype(jnp.bfloat16)
    rgrad_ref[...] = upstream + norm_pull(pulled, gain, xhat, rate)
    vec_ref[0:1] += column_sum(pulled * xhat)
    vec_ref[1:2] += column_sum(pulled)
    vec_ref[2:3] += column_sum(low.astype(jnp.float32))

    @pl.when(step == pl.num_programs(0) - 1)
    def _():
        for b in range(4):
            part_ref[:, b * 16 : (b + 1) * 16, :] = we_acc[b].reshape(RANKS, 16, C).astype(jnp.bfloat16)
            part_ref[b * 8 : (b + 1) * 8, 64:128, :] = (
                wr_acc[b].T.reshape(8, 64, C).astype(jnp.bfloat16)
            )


def mlp_block(res, cot, live, far, vectors, ebias, rows=448):
    tokens = res.shape[0]
    moving = pl.BlockSpec((rows, C), lambda i: (i, 0))
    return pl.pallas_call(
        mlp_kernel,
        grid=(tokens // rows,),
        in_specs=[moving, moving, pl.BlockSpec(memory_space=pltpu.SMEM), fixed((RANKS, FAR, C)), fixed((8, C)), fixed((1, EXPAND))],
        out_specs=[moving, moving, fixed((RANKS, FAR, C)), fixed((8, C))],
        out_shape=[
            jax.ShapeDtypeStruct((tokens, C), jnp.bfloat16),
            jax.ShapeDtypeStruct((tokens, C), jnp.float32),
            jax.ShapeDtypeStruct((RANKS, 128, C), jnp.bfloat16),
            jax.ShapeDtypeStruct((8, C), jnp.float32),
        ],
        scratch_shapes=[pltpu.VMEM((4, C, C), jnp.float32), pltpu.VMEM((4, C, C), jnp.float32), pltpu.VMEM((rows, EXPAND), jnp.bfloat16), pltpu.VMEM((rows, EXPAND), jnp.bfloat16)],
        compiler_params=pltpu.CompilerParams(vmem_limit_bytes=60 << 20, dimension_semantics=("arbitrary",)),
        name="mlp_block",
    )(res, cot, live, far, vectors, ebias)

SPOTS = WIN * WIN
ROWS = SPOTS * 16
QUERY_ROWS = 64
KEY_ROWS = 56
QUAD = 4 * HEAD_DIM
PAIR_SHAPE = (4 * KEY_ROWS, 2 * QUERY_ROWS)
SCALE = HEAD_DIM**-0.5


def spot_of(pane, spot):
    y = lax.rem((pane // 2) * WIN + spot // WIN + SHIFT, SIDE)
    x = lax.rem((pane % 2) * WIN + spot % WIN + SHIFT, SIDE)
    return y, x


def take_pane(pane, source, target):
    for spot in range(SPOTS):
        y, x = spot_of(pane, spot)
        target[spot * 16 : (spot + 1) * 16, :] = source[y, x]


def give_pane(pane, value, target):
    for spot in range(SPOTS):
        y, x = spot_of(pane, spot)
        target[y, x] = value[spot * 16 : (spot + 1) * 16, :]


def put_tiles(target, first, value):
    for tile in range(4):
        target[first + tile, 0:ROWS, :] = value[:, tile * QUAD : (tile + 1) * QUAD]


def get_tiles(source, first):
    return jnp.concatenate([source[first + tile, 0:ROWS, :] for tile in range(4)], axis=1)


def heads_mask(rows):
    return lax.rem(lax.broadcasted_iota(jnp.int32, (rows, 2 * QUAD), 1), QUAD) // HEAD_DIM


def load_pair(source, first, rows):
    return jnp.concatenate([source[first, rows, :], source[first + 1, rows, :]], axis=1)


def spread_heads(pair):
    lanes = heads_mask(KEY_ROWS)
    zero = jnp.zeros_like(pair)
    return jnp.concatenate([jnp.where(lanes == h, pair, zero) for h in range(4)], axis=0).astype(jnp.bfloat16)


def merge_heads(value):
    lanes = heads_mask(KEY_ROWS)
    parts = [value[h * KEY_ROWS : (h + 1) * KEY_ROWS] for h in range(4)]
    return jnp.where(
        lanes < 2, jnp.where(lanes == 0, parts[0], parts[1]), jnp.where(lanes == 2, parts[2], parts[3])
    )


def two_blocks(source, first, rows):
    upper = source[first, rows, :].astype(jnp.bfloat16)
    lower = source[first + 1, rows, :].astype(jnp.bfloat16)
    zero = jnp.zeros_like(upper)
    return jnp.concatenate(
        [jnp.concatenate([upper, zero], axis=1), jnp.concatenate([zero, lower], axis=1)], axis=0
    )


def over_keys(op, value):
    parts = value.reshape(4, KEY_ROWS, 2 * QUERY_ROWS)
    return jnp.broadcast_to(op(parts, axis=1, keepdims=True), parts.shape).reshape(value.shape)


def build_bias(table_ref, pair_bias):
    heads = dot_nn(table_ref[...], offset_onehot())
    heads = reorder(heads)
    for tile in range(KEY_ROWS // 2):
        part = heads[:, tile * 128 : (tile + 1) * 128]
        for key, value in enumerate(swap_halves(part[0:8], part[8:16]), 2 * tile):
            if key >= SPOTS:
                value = jnp.full(value.shape, -1e30, jnp.float32)
            pair_bias[pl.ds(key, 8, stride=KEY_ROWS), :] = value


def place_in(pane, spot):
    down = seventh(spot)
    y = (pane // 2) * WIN + down + SHIFT
    x = lax.rem(pane, 2) * WIN + spot - WIN * down + SHIFT
    return jnp.where(y >= SIDE, y - SIDE, y), jnp.where(x >= SIDE, x - SIDE, x)


def pane_mask(pane, regions_ref):
    labels = regions_ref[...].astype(jnp.float32).astype(jnp.bfloat16)
    row = lax.broadcasted_iota(jnp.int32, (PAIR_SHAPE[0], SIDE), 0)
    key = row - KEY_ROWS * ((row * 1171) >> 16)
    y, x = place_in(pane, key)
    col = lax.broadcasted_iota(jnp.int32, row.shape, 1)
    lines = dot_nn(jnp.where(col == y, 1.0, 0.0).astype(jnp.bfloat16), labels)
    keys = jnp.sum(jnp.where(col == x, lines, 0.0), axis=1, keepdims=True)
    query = lax.broadcasted_iota(jnp.int32, (SIDE, PAIR_SHAPE[1]), 1) & (QUERY_ROWS - 1)
    y, x = place_in(pane, query)
    row = lax.broadcasted_iota(jnp.int32, query.shape, 0)
    lines = dot_nn(labels, jnp.where(row == x, 1.0, 0.0).astype(jnp.bfloat16))
    queries = jnp.sum(jnp.where(row == y, lines, 0.0), axis=0, keepdims=True)
    return jnp.where(keys == queries, 0.0, -100.0)


def bias_rows(rows, vec_ref, ebias_ref):
    values = rows[...].astype(jnp.float32)

    def taken(lhs, width):
        source = lax.broadcasted_iota(jnp.int32, (128, RANKS * width), 0)
        target = lax.broadcasted_iota(jnp.int32, (128, RANKS * width), 1)
        onehot = jnp.where(source == lax.rem(target, width), 1.0, 0.0).astype(jnp.bfloat16)
        spread = dot_nn(lhs.reshape(-1, 128).astype(jnp.bfloat16), onehot).reshape(RANKS, -1, RANKS * width)
        shard = lax.broadcasted_iota(jnp.int32, spread.shape, 0)
        place = lax.broadcasted_iota(jnp.int32, spread.shape, 2) // width
        return jnp.sum(jnp.where(shard == place, spread, 0.0), axis=0)

    vec_ref[...] = taken(values[:, 0:8], 16)
    ebias_ref[...] = taken(values[:, 8:16], 64)[0:1]


def attend_kernel(linked, *refs):
    x_ref, table_ref, regions_ref, *refs = refs
    if linked:
        shards, refs = refs[:5], refs[5:]
    else:
        near, output, rows, *refs = refs
    joint_ref, probs_ref, mixed_ref, res_ref, vec_ref, ebias_ref, *refs = refs
    if linked:
        near_out, output_out, far_out, *refs = refs
    window, wide, blend, both, score_a, score_b, probs_a, probs_b, pair_bias, *refs = refs
    pane = pl.program_id(0)
    last = pl.num_programs(0) - 1
    if linked:
        near, rows, output, far_own, local, *sems = refs
        place = Place()
        joint_w, output_w, expand_w, reduce_w, row_w = shards
        blocks = [joint_w.at[:, b * C : (b + 1) * C] for b in range(3)]
        close = [
            Gather(place, blocks[b], near, *sems[2 * b : 2 * b + 2], 16 * b, 16) for b in range(3)
        ]
        little = Gather(place, row_w, rows, *sems[6:8])
        middle = Gather(place, output_w, output, *sems[8:10])
        distant = Gather(place, far_own, far_out, *sems[10:12])
        pieces = [(blocks[b], close[b].at(place.me)) for b in range(3)]
        pieces += [(row_w, rows.at[place.me]), (output_w, output.at[place.me])]
        pieces += [
            (expand_w.at[:, b * C : (b + 1) * C], far_own.at[b * 16 : (b + 1) * 16]) for b in range(4)
        ]
        pieces += [(reduce_w, far_own.at[64:128])]
        pieces = [pltpu.make_async_copy(a, b, local.at[i]) for i, (a, b) in enumerate(pieces)]
        keep = [(near, near_out), (output, output_out), (far_own, far_out.at[place.me])]
        keep = [pltpu.make_async_copy(a, b, local.at[10 + i]) for i, (a, b) in enumerate(keep)]

    @pl.when(pane == 0)
    def _():
        if linked:
            for piece in pieces:
                piece.start()
            place.greet()
            little.start()
            for group in close:
                group.start()
        build_bias(table_ref, pair_bias)
        wide[:, ROWS:, :] = jnp.zeros((12, QUERY_ROWS * 16 - ROWS, QUAD), jnp.float32)
        probs_b[...] = jnp.zeros_like(probs_b)
        if linked:
            little.relay_columns()
            for group in close:
                group.relay_columns()
            middle.start()
            little.relay_sides()
            for group in close:
                group.relay_sides()
            little.relay_corners()
            for piece in pieces:
                piece.wait()
            little.finish()
        bias_rows(rows, vec_ref, ebias_ref)
        if linked:
            for group in close:
                group.relay_corners()
            middle.relay_columns()
            distant.start()
            keep[2].start()

    if linked:
        @pl.when(pane == 1)
        def _():
            keep[1].start()
            distant.relay_columns()

        @pl.when(pane == 2)
        def _():
            distant.relay_sides()

        @pl.when(pane == 3)
        def _():
            distant.relay_corners()

    take_pane(pane, x_ref, window)
    source = window[...].astype(jnp.float32)
    xhat, _ = norm_parts(source)
    normed = (xhat * vec_ref[0:1] + vec_ref[1:2]).astype(jnp.bfloat16)
    for b in range(3):
        if linked:
            @pl.when(pane == 0)
            def _():
                close[b].finish()
                if b == 2:
                    keep[0].start()
                    middle.relay_sides()

        weight = near[:, b * 16 : (b + 1) * 16, :].reshape(C, C)
        block = dot_nn(normed, weight)
        if b != 1:
            block += vec_ref[2 + b // 2 : 3 + b // 2]
        block = block.astype(jnp.bfloat16)
        joint_ref[0, :, b * C : (b + 1) * C] = block
        put_tiles(wide, b * 4, block.astype(jnp.float32))
    mask = pane_mask(pane, regions_ref)
    for pair in range(2):
        both[pair] = pair_bias[pair * PAIR_SHAPE[0] : (pair + 1) * PAIR_SHAPE[0]] + mask

    def rows_of(m):
        return pl.ds(m, QUERY_ROWS, stride=16), pl.ds(m, KEY_ROWS, stride=16)

    def score(m, target):
        few, many = rows_of(m)
        for pair in range(2):
            k = spread_heads(load_pair(wide, 4 + 2 * pair, many))
            target[pair] = dot_nt(k, two_blocks(wide, 2 * pair, few))

    def soften(m, source, target):
        for pair in range(2):
            scores = source[pair] * SCALE + both[pair]
            powers = jnp.exp(scores - over_keys(jnp.max, scores))
            probs = (powers * (1.0 / over_keys(jnp.sum, powers))).astype(jnp.bfloat16)
            target[pair] = probs
            probs_ref[0, m, pair] = probs

    def mix(m, source):
        few, many = rows_of(m)
        for pair in range(2):
            v = spread_heads(load_pair(wide, 8 + 2 * pair, many))
            blended = dot_tn(source[pair], v)
            blend[2 * pair, many, :] = blended[0:KEY_ROWS, 0:QUAD]
            blend[2 * pair + 1, many, :] = blended[QUERY_ROWS : QUERY_ROWS + KEY_ROWS, QUAD:]

    def two_images(step, carry):
        m = 2 * step
        if linked:
            @pl.when((pane == 0) & (step == 2))
            def _():
                middle.relay_corners()

        mix(jnp.maximum(m - 1, 0), probs_b)
        soften(m, score_a, probs_a)
        score(m + 1, score_b)
        mix(m, probs_a)
        soften(m + 1, score_b, probs_b)
        score(jnp.minimum(m + 2, 15), score_a)
        return carry

    score(0, score_a)
    lax.fori_loop(0, 8, two_images, 0)
    mix(15, probs_b)
    if linked:
        @pl.when(pane == 0)
        def _():
            middle.finish()

    mixed = get_tiles(blend, 0).astype(jnp.bfloat16)
    mixed_ref[0] = mixed
    projected = dot_nn(mixed, output[...].reshape(C, C)) + vec_ref[4:5]
    give_pane(pane, window[...].astype(jnp.float32) + projected, res_ref)

    if linked:
        @pl.when(pane == last)
        def _():
            distant.finish()
            for group in (*close, little, middle, distant):
                group.drain()
            for kept in keep:
                kept.wait()


def fixed(shape):
    return pl.BlockSpec(shape, lambda i: (0,) * len(shape), pipeline_mode=pl.Buffered(1))


def stepped(shape):
    return pl.BlockSpec((1,) + shape, lambda i: (i,) + (0,) * len(shape))


def attend(x, table, regions, weights, linked):
    anywhere = pl.BlockSpec(memory_space=pl.ANY)
    out_specs = [stepped((ROWS, 3 * C)), stepped((16, 2) + PAIR_SHAPE), stepped((ROWS, C)),
                 fixed((SIDE, SIDE, 16, C)), fixed((8, C)), fixed((1, EXPAND))]
    out_shape = [
        jax.ShapeDtypeStruct((PANES, ROWS, 3 * C), jnp.bfloat16),
        jax.ShapeDtypeStruct((PANES, 16, 2) + PAIR_SHAPE, jnp.bfloat16),
        jax.ShapeDtypeStruct((PANES, ROWS, C), jnp.bfloat16),
        jax.ShapeDtypeStruct((SIDE, SIDE, 16, C), jnp.float32),
        jax.ShapeDtypeStruct((8, C), jnp.float32),
        jax.ShapeDtypeStruct((1, EXPAND), jnp.float32),
    ]
    scratch = [
        pltpu.VMEM((ROWS, C), jnp.bfloat16),
        pltpu.VMEM((12, QUERY_ROWS * 16, QUAD), jnp.float32),
        pltpu.VMEM((4, QUERY_ROWS * 16, QUAD), jnp.float32),
        pltpu.VMEM((2,) + PAIR_SHAPE, jnp.float32),
        pltpu.VMEM((2,) + PAIR_SHAPE, jnp.float32),
        pltpu.VMEM((2,) + PAIR_SHAPE, jnp.float32),
        pltpu.VMEM((2,) + PAIR_SHAPE, jnp.bfloat16),
        pltpu.VMEM((2,) + PAIR_SHAPE, jnp.bfloat16),
        pltpu.VMEM((2 * PAIR_SHAPE[0], PAIR_SHAPE[1]), jnp.float32),
    ]
    in_specs = [fixed((SIDE, SIDE, 16, C)), fixed(table.shape), fixed(regions.shape)]
    if linked:
        in_specs += [anywhere] * 5
        out_specs += [anywhere] * 3
        out_shape += [
            jax.ShapeDtypeStruct((RANKS, NEAR, C), jnp.bfloat16),
            jax.ShapeDtypeStruct((RANKS, 16, C), jnp.bfloat16),
            jax.ShapeDtypeStruct((RANKS, FAR, C), jnp.bfloat16),
        ]
        scratch += [
            pltpu.VMEM((RANKS, NEAR, C), jnp.bfloat16),
            pltpu.VMEM((RANKS, 16, 128), jnp.bfloat16),
            pltpu.VMEM((RANKS, 16, C), jnp.bfloat16),
            pltpu.VMEM((FAR, C), jnp.bfloat16),
            pltpu.SemaphoreType.DMA((13,)),
        ] + [pltpu.SemaphoreType.DMA((31,))] * 12
        extra = dict(collective_id=0, has_side_effects=True)
    else:
        in_specs += [fixed((RANKS, NEAR, C)), fixed((RANKS, 16, C)), fixed((RANKS, 16, 128))]
        extra = {}
    return pl.pallas_call(
        functools.partial(attend_kernel, linked),
        grid=(PANES,),
        in_specs=in_specs,
        out_specs=out_specs,
        out_shape=out_shape,
        scratch_shapes=scratch,
        compiler_params=pltpu.CompilerParams(
            vmem_limit_bytes=62 << 20, dimension_semantics=("arbitrary",), **extra
        ),
        name="attend",
    )(x, table, regions, *weights)


def attend_back_kernel(linked, *refs):
    x_ref, near_ref, output_ref, joint_ref, probs_ref, mixed_ref, rgrad_ref, bias_ref, *refs = refs
    if linked:
        far_parts, *refs = refs
    dx_ref, part_ref, vec_ref, pairs_ref, *refs = refs
    if linked:
        ge_ref, gr_ref, *refs = refs
    window, rwindow, wide, blend, turned, wj_acc, wo_acc, pgrad_a, pgrad_b, sgrad_a, sgrad_b, *refs = refs
    pane = pl.program_id(0)
    if linked:
        place = Place()
        distant = Reduce(place, far_parts, refs)

    @pl.when(pane == 0)
    def _():
        if linked:
            place.greet()
            distant.start()
        pads = QUERY_ROWS * 16 - ROWS
        wide[:, ROWS:, :] = jnp.zeros((12, pads, QUAD), jnp.float32)
        blend[:, ROWS:, :] = jnp.zeros((4, pads, QUAD), jnp.float32)
        sgrad_b[...] = jnp.zeros_like(sgrad_b)
        wj_acc[...] = jnp.zeros_like(wj_acc)
        wo_acc[...] = jnp.zeros_like(wo_acc)
        vec_ref[...] = jnp.zeros_like(vec_ref)
        pairs_ref[...] = jnp.zeros_like(pairs_ref)

    if linked:
        @pl.when(pane == 1)
        def _():
            distant.cores()

        @pl.when(pane == 2)
        def _():
            distant.sides()

        @pl.when(pane == 3)
        def _():
            distant.corners()

    take_pane(pane, x_ref, window)
    take_pane(pane, rgrad_ref, rwindow)
    pulled = rwindow[...].astype(jnp.bfloat16)
    wo = output_ref[...].reshape(C, C)
    wo_acc[...] += dot_tn(mixed_ref[0], pulled)
    vec_ref[0:1] += column_sum(pulled.astype(jnp.float32))
    put_tiles(blend, 0, dot_nt(pulled, wo).astype(jnp.bfloat16).astype(jnp.float32))
    for b in range(3):
        put_tiles(wide, b * 4, joint_ref[0, :, b * C : (b + 1) * C].astype(jnp.float32))

    def rows_of(m):
        return pl.ds(m, QUERY_ROWS, stride=16), pl.ds(m, KEY_ROWS, stride=16)

    def pull_probs(m, target):
        few, many = rows_of(m)
        for pair in range(2):
            v = spread_heads(load_pair(wide, 8 + 2 * pair, many))
            target[pair] = dot_nt(v, two_blocks(blend, 2 * pair, few))

    def pull_scores(m, source, target):
        for pair in range(2):
            probs = probs_ref[0, m, pair].astype(jnp.float32)
            weighted = source[pair] * probs
            sgrad = (weighted - probs * over_keys(jnp.sum, weighted)).astype(jnp.bfloat16)
            target[pair] = sgrad
            pairs_ref[pair] += sgrad.astype(jnp.float32)

    def pull_rest(m, source):
        few, many = rows_of(m)
        for pair in range(2):
            sgrad = source[pair]
            k = spread_heads(load_pair(wide, 4 + 2 * pair, many))
            qgrad = dot_tn(sgrad, k) * SCALE
            turned[2 * pair, many, :] = qgrad[0:KEY_ROWS, 0:QUAD]
            turned[2 * pair + 1, many, :] = qgrad[QUERY_ROWS : QUERY_ROWS + KEY_ROWS, QUAD:]
            kgrad = merge_heads(dot_nn(sgrad, two_blocks(wide, 2 * pair, few))) * SCALE
            turned[4 + 2 * pair, many, :] = kgrad[:, 0:QUAD]
            turned[5 + 2 * pair, many, :] = kgrad[:, QUAD:]
            vgrad = merge_heads(dot_nn(probs_ref[0, m, pair], two_blocks(blend, 2 * pair, few)))
            turned[8 + 2 * pair, many, :] = vgrad[:, 0:QUAD]
            turned[9 + 2 * pair, many, :] = vgrad[:, QUAD:]

    def two_images(step, carry):
        m = 2 * step
        pull_rest(jnp.maximum(m - 1, 0), sgrad_b)
        pull_scores(m, pgrad_a, sgrad_a)
        pull_probs(m + 1, pgrad_b)
        pull_rest(m, sgrad_a)
        pull_scores(m + 1, pgrad_b, sgrad_b)
        pull_probs(jnp.minimum(m + 2, 15), pgrad_a)
        return carry

    pull_probs(0, pgrad_a)
    lax.fori_loop(0, 8, two_images, 0)
    pull_rest(15, sgrad_b)
    gain = bias_ref[0:1]
    xhat, rate = norm_parts(window[...].astype(jnp.float32))
    normed = (xhat * gain + bias_ref[1:2]).astype(jnp.bfloat16)
    normed_t = normed.T
    total = jnp.zeros((ROWS, C), jnp.float32)
    for b in range(3):
        weight = near_ref[:, b * 16 : (b + 1) * 16, :].reshape(C, C)
        block = get_tiles(turned, b * 4).astype(jnp.bfloat16)
        wj_acc[b] += dot_nn(normed_t, block)
        total += dot_nt(block, weight)
        if b != 1:
            vec_ref[1 + b // 2 : 2 + b // 2] += column_sum(block.astype(jnp.float32))
    vec_ref[3:4] += column_sum(total * xhat)
    vec_ref[4:5] += column_sum(total)
    dx = rwindow[...] + norm_pull(total, gain, xhat, rate)
    give_pane(pane, dx.astype(jnp.bfloat16), dx_ref)

    @pl.when(pane == PANES - 1)
    def _():
        for b in range(3):
            part_ref[:, b * 16 : (b + 1) * 16, :] = wj_acc[b].reshape(RANKS, 16, C).astype(jnp.bfloat16)
        part_ref[:, 48:64, :] = wo_acc[...].reshape(RANKS, 16, C).astype(jnp.bfloat16)
        if linked:
            total = distant.finish()
            for b in range(4):
                ge_ref[:, b * C : (b + 1) * C] = total[b * 16 : (b + 1) * 16]
            gr_ref[...] = total[64:128]
            distant.drain()


def attend_back(x, near, output, joint, probs, mixed, rgrad, vectors, far_parts, linked):
    in_specs = [fixed((SIDE, SIDE, 16, C)), fixed((RANKS, NEAR, C)), fixed((RANKS, 16, C)), stepped((ROWS, 3 * C)),
                stepped((16, 2) + PAIR_SHAPE), stepped((ROWS, C)), fixed((SIDE, SIDE, 16, C)), fixed((8, C))]
    out_specs = [fixed((SIDE, SIDE, 16, C)), fixed((RANKS, 64, C)), fixed((8, C)), fixed((2,) + PAIR_SHAPE)]
    out_shape = [
        jax.ShapeDtypeStruct((SIDE, SIDE, 16, C), jnp.bfloat16),
        jax.ShapeDtypeStruct((RANKS, 64, C), jnp.bfloat16),
        jax.ShapeDtypeStruct((8, C), jnp.float32),
        jax.ShapeDtypeStruct((2,) + PAIR_SHAPE, jnp.float32),
    ]
    scratch = [
        pltpu.VMEM((ROWS, C), jnp.bfloat16),
        pltpu.VMEM((ROWS, C), jnp.float32),
        pltpu.VMEM((12, QUERY_ROWS * 16, QUAD), jnp.float32),
        pltpu.VMEM((4, QUERY_ROWS * 16, QUAD), jnp.float32),
        pltpu.VMEM((12, QUERY_ROWS * 16, QUAD), jnp.float32),
        pltpu.VMEM((3, C, C), jnp.float32),
        pltpu.VMEM((C, C), jnp.float32),
        pltpu.VMEM((2,) + PAIR_SHAPE, jnp.float32),
        pltpu.VMEM((2,) + PAIR_SHAPE, jnp.float32),
        pltpu.VMEM((2,) + PAIR_SHAPE, jnp.bfloat16),
        pltpu.VMEM((2,) + PAIR_SHAPE, jnp.bfloat16),
    ]
    operands = [x, near, output, joint, probs, mixed, rgrad, vectors]
    extra = {}
    if linked:
        in_specs.append(pl.BlockSpec(memory_space=pl.ANY))
        out_specs += [fixed((16, EXPAND)), fixed((64, C))]
        out_shape += [
            jax.ShapeDtypeStruct((16, EXPAND), jnp.float32),
            jax.ShapeDtypeStruct((64, C), jnp.float32),
        ]
        scratch += Reduce.scratch(FAR)
        operands.append(far_parts.reshape(4, 2, 2, 2, FAR, C))
        extra = dict(collective_id=1, has_side_effects=True)
    return pl.pallas_call(
        functools.partial(attend_back_kernel, linked),
        grid=(PANES,),
        in_specs=in_specs,
        out_specs=out_specs,
        out_shape=out_shape,
        scratch_shapes=scratch,
        compiler_params=pltpu.CompilerParams(
            vmem_limit_bytes=(1 << 26) - (64 << 10), dimension_semantics=("arbitrary",), **extra
        ),
        name="attend_back",
    )(*operands)

def regroup(packed, blocks, rows):
    count = packed.shape[0] // RANKS
    return (
        packed.reshape(RANKS, count, blocks, rows, C)
        .transpose(0, 2, 1, 3, 4)
        .reshape(RANKS, blocks * rows * count, C)
    )


def ungroup(parts, blocks, ranks):
    rows = parts.shape[1] // blocks
    flat = parts.reshape(RANKS, blocks, rows, C).transpose(1, 0, 2, 3).reshape(blocks, RANKS * rows, C)
    return flat.reshape(blocks, ranks, RANKS * rows // ranks, C).transpose(1, 0, 2, 3)


def on_device(
    images,
    first_gain,
    first_shift,
    joint_weight,
    joint_bias,
    output_weight,
    output_bias,
    second_gain,
    second_shift,
    expand_weight,
    expand_bias,
    reduce_weight,
    reduce_bias,
    bias_table,
    regions,
    live_slots,
    cotangent,
):
    ranks = lax.axis_size("dp")
    count = images.shape[0]
    linked = ranks == RANKS
    small = (
        first_gain,
        first_shift,
        joint_bias[0],
        joint_bias[1],
        output_bias,
        second_gain,
        second_shift,
        reduce_bias,
        expand_bias,
    )
    x = images.transpose(1, 2, 0, 3)
    cot = cotangent.transpose(1, 2, 0, 3).reshape(-1, C)
    if linked:
        row = jnp.zeros((16, 128), jnp.bfloat16)
        for first, vector in (
            (0, first_gain), (1, first_shift), (2, joint_bias), (4, output_bias), (5, second_gain),
            (6, second_shift), (7, reduce_bias), (8, expand_bias),
        ):
            vector = jnp.atleast_2d(vector)
            height, width = vector.shape
            row += jnp.pad(vector, ((first, 16 - first - height), (0, 128 - width)))
        weights = (joint_weight, output_weight, expand_weight, reduce_weight, row)
        joint, probs, mixed, res, vectors, ebias, near, output, far = attend(x, bias_table.T, regions, weights, True)
    else:
        rows = C // ranks
        wide = lambda w: lax.all_gather(w, "dp", axis=0)
        near = jnp.concatenate([wide(joint_weight[:, i * C : (i + 1) * C]) for i in range(3)], axis=1)
        near, output = regroup(near, 3, rows), regroup(wide(output_weight), 1, rows)
        pieces = [
            lax.all_gather(v, "dp", axis=0, tiled=True).reshape(RANKS, 1, -1) for v in small
        ]
        row = jnp.concatenate([jnp.pad(v, ((0, 0), (0, 0), (0, 128 - v.shape[2]))) for v in pieces], axis=1)
        row = jnp.pad(row, ((0, 0), (0, 7), (0, 0)))
        far = jnp.concatenate([wide(expand_weight[:, i * C : (i + 1) * C]) for i in range(4)], axis=1)
        far = jnp.concatenate([regroup(far, 4, rows), wide(reduce_weight).reshape(RANKS, 64, C)], axis=1)
        joint, probs, mixed, res, vectors, ebias = attend(x, bias_table.T, regions, (near, output, row), False)
    out, rgrad, far_part, far_vec = mlp_block(
        res.reshape(-1, C), cot, live_slots, far, vectors, ebias
    )
    rgrad = rgrad.reshape(SIDE, SIDE, count, C)
    dx, near_part, near_vec, pairs, *far_grads = attend_back(
        x, near, output, joint, probs, mixed, rgrad, vectors, far_part, linked
    )
    pairs = pairs.reshape(-1, pairs.shape[-1])
    if linked:
        ge, gr = far_grads
        reduced = reduce_near(near_part, near_vec, far_vec, pairs)
        dx, ge, gr, gj, go, table, jb, eb, *own = settle(dx, (ge, gr, *reduced))
        own = [v.reshape(-1) for v in own]
        ob, gain1, shift1, gain2, shift2, rb = own
        eb = eb.reshape(-1)
    else:
        scatter = lambda g: lax.psum_scatter(g.astype(jnp.float32), "dp", scatter_dimension=0, tiled=True)
        cut = lambda part, blocks: scatter(
            ungroup(part, blocks, ranks).transpose(0, 2, 1, 3).reshape(C, blocks * C)
        )
        gj, go = cut(near_part[:, :48], 3), cut(near_part[:, 48:], 1)
        ge, gr = cut(far_part[:, :64], 4), scatter(far_part[:, 64:].reshape(EXPAND, C))
        ob, qb, vb, gain1, shift1 = [scatter(near_vec[i]) for i in range(5)]
        gain2, shift2, rb = [scatter(far_vec[i]) for i in range(3)]
        eb, jb = scatter(far_vec[3:7].reshape(-1)), jnp.stack([qb, vb])
        heads = pairs.reshape(2, 4, KEY_ROWS, 2, QUERY_ROWS).transpose(0, 3, 1, 2, 4).reshape(HEADS, -1)
        table = lax.dot_general(
            heads, offset_onehot().astype(jnp.float32), (((1,), (1,)), ((), ())),
            precision=exact_mode, preferred_element_type=jnp.float32,
        )
        table = lax.psum(table, "dp")
    image_order = lambda v: v.reshape(SIDE, SIDE, count, C).transpose(2, 0, 1, 3)
    return (
        image_order(out),
        image_order(dx),
        gain1,
        shift1,
        gj,
        jb,
        go,
        ob,
        gain2,
        shift2,
        ge,
        eb,
        gr,
        rb,
        table.T,
    )


def solution(mesh):
    in_specs = (
        P("dp", None, None, None),
        P("dp"),
        P("dp"),
        P("dp", None),
        P(None, "dp"),
        P("dp", None),
        P("dp"),
        P("dp"),
        P("dp"),
        P("dp", None),
        P("dp"),
        P("dp", None),
        P("dp"),
        P(),
        P(),
        P("dp"),
        P("dp", None, None, None),
    )
    out_specs = (
        P("dp", None, None, None),
        P("dp", None, None, None),
        P("dp"),
        P("dp"),
        P("dp", None),
        P(None, "dp"),
        P("dp", None),
        P("dp"),
        P("dp"),
        P("dp"),
        P("dp", None),
        P("dp"),
        P("dp", None),
        P("dp"),
        P(),
    )
    return jax.shard_map(
        on_device, mesh=mesh, in_specs=in_specs, out_specs=out_specs, check_vma=False
    )
```
